32 devices in a mesh: blk: 16 (over z, x, core), cuts: 2 (over y).
Axes of the slice: x: 2, y: 2, z: 4, core: 2. Of those that a mesh axis runs over, the one named last changes fastest.
Arguments:
- left_env: bfloat16 [2048, 8, 2048], P('blk', 'cuts'), may hold values from -4 to 4
- right_env: bfloat16 [2048, 8, 2048], P('blk', 'cuts'), may hold values from -4 to 4
- left_core: float32 [8, 8, 2, 2], replicated, may hold values from -1.5 to 1.5
- right_core: float32 [8, 8, 2, 2], replicated, may hold values from -1.5 to 1.5
- slot_bond: int32 [8], replicated, may hold values from 0 to 7, each once
- krylov_basis: float32 [8, 2048, 4, 2048], P(None, 'blk', None, 'cuts'), may hold values from -30 to 30
- beta_prev: float32 [], replicated, may hold values from 0.3 to 1.2
Outputs:
- next_vector: float32 [2048, 4, 2048], P('blk', None, 'cuts')
- alpha_values: float32 [1], replicated
- beta_values: float32 [1], replicated
The draws below stay inside these ranges and needn't reach their ends.
Inputs may be any that keep to these rules, and one draw needn't show every extreme that they name: `slot_bond`: a permutation of the 8 bond values.
All inputs are finite; a program needn't handle non-finite values.
Results may differ from the reference program's by a relative error of at most 0.00073.
The reference program's roundings to bfloat16 on the way (of `current` and `mixed_left`) count: a program that leaves them out, or rounds other values in their place, can miss the bound.
Values may be sent and summed in bfloat16 or wider, within the bound.
A program may use at most 192 MiB of HBM per device.

```python
import math
import jax
import jax.numpy as jnp
from jax import lax

D = 2048
PHYS = 2
W = 8
KRY = 8
STEPS = 1


def draw_environment(key):
    key_noise, key_diag = jax.random.split(key, 2)
    noise_part = jnp.clip(jax.random.normal(key_noise, (D, W, D), jnp.float32), -6.0, 6.0) * (0.8 / math.sqrt(D))
    diag_values = jax.random.uniform(key_diag, (D, W), jnp.float32, 0.5, 1.5)
    on_diagonal = jnp.arange(D, dtype=jnp.int32)[:, None, None] == jnp.arange(D, dtype=jnp.int32)[None, None, :]
    return (noise_part + jnp.where(on_diagonal, diag_values[:, :, None], 0.0)).astype(jnp.bfloat16)


def draw_left_env(key, part):
    return draw_environment(jax.random.fold_in(key, 11))


def draw_right_env(key, part):
    return draw_environment(jax.random.fold_in(key, 23))


def draw_krylov_basis(key, part):
    key_common, key_single = jax.random.split(jax.random.fold_in(key, 37), 2)
    one_shape = (D, PHYS * PHYS, D)
    rising_scale = jnp.exp(math.log(3.0) * jnp.arange(D, dtype=jnp.float32) / D)[:, None, None]
    common = jnp.clip(jax.random.normal(key_common, one_shape, jnp.float32), -6.0, 6.0)
    single = jnp.clip(jax.random.normal(key_single, (KRY,) + one_shape, jnp.float32), -6.0, 6.0)
    return rising_scale[None] * (0.6 * common[None] + 0.8 * single)


def bell_draw(own_key, shape, scale, bound, kind=jnp.bfloat16):
    values = scale * jax.random.normal(own_key, shape, jnp.float32)
    return jnp.clip(values, min=-bound, max=bound).astype(kind)


def setup_inputs(seed: int = 0) -> dict:
    streams_of = jax.random.split(jax.random.key(seed), 8)
    left_env = draw_left_env(jax.random.fold_in(streams_of[7], 71), 0)
    right_env = draw_right_env(jax.random.fold_in(streams_of[7], 71), 0)
    left_core = bell_draw(streams_of[2], (W, W, PHYS, PHYS), (W * PHYS) ** -0.5, 1.5, jnp.float32)
    right_core = bell_draw(streams_of[3], (W, W, PHYS, PHYS), (W * PHYS) ** -0.5, 1.5, jnp.float32)
    slot_bond = jax.random.permutation(streams_of[4], W).astype(jnp.int32)
    krylov_basis = draw_krylov_basis(jax.random.fold_in(streams_of[7], 71), 0)
    beta_prev = jnp.clip(jax.random.uniform(streams_of[6], (), jnp.float32, 0.3, 1.2), 0.3, 1.2)
    return dict(left_env=left_env, right_env=right_env, left_core=left_core, right_core=right_core, slot_bond=slot_bond, krylov_basis=krylov_basis, beta_prev=beta_prev)


def build_table(left_core, right_core, slot_bond):
    picked = left_core[slot_bond]
    table = jnp.einsum('kxac,xybd->kyabcd', picked, right_core, precision=lax.Precision.HIGHEST)
    return table.reshape(W, W, PHYS * PHYS, PHYS * PHYS)

def apply_hamiltonian(left_env, right_env, mpo_table, current):
    pair_count = PHYS * PHYS
    block_rows = min(D, 256)
    block_count = D // block_rows
    right_matrix = right_env.reshape(D, W * D).T
    vector_matrix = current.reshape(D, pair_count * D)

    def one_block(block_index):
        start_row = (block_index * block_rows).astype(jnp.int32)
        left_rows = lax.dynamic_slice_in_dim(left_env, start_row, block_rows, 0).reshape(block_rows * W, D)
        projected = jnp.dot(left_rows, vector_matrix, preferred_element_type=jnp.float32)
        projected = projected.reshape(block_rows, W, pair_count, D)
        mixed_left = jnp.einsum('kypq,akqb->apyb', mpo_table, projected, precision=lax.Precision.HIGHEST).astype(jnp.bfloat16)
        image_rows = jnp.dot(mixed_left.reshape(block_rows * pair_count, W * D), right_matrix, preferred_element_type=jnp.float32)
        return image_rows.reshape(block_rows, pair_count, D)
    image_vec = lax.map(one_block, jnp.arange(block_count, dtype=jnp.int32))
    return image_vec.reshape(D, pair_count, D)

def reference(left_env, right_env, left_core, right_core, slot_bond, krylov_basis, beta_prev):
    highest = lax.Precision.HIGHEST
    entries = float(D * PHYS * PHYS * D)
    mpo_table = build_table(left_core, right_core, slot_bond)
    basis_now = krylov_basis
    beta_now = beta_prev
    alpha_list = []
    beta_list = []
    next_vector = krylov_basis[KRY - 1]
    for step_index in range(STEPS):
        current_f = basis_now[KRY - 1]
        previous = basis_now[KRY - 2]
        image_vec = apply_hamiltonian(left_env, right_env, mpo_table, current_f.astype(jnp.bfloat16))
        alpha_now = jnp.sum(current_f * image_vec) / entries
        first_pass = image_vec - alpha_now * current_f - beta_now * previous
        ortho_coeffs = jnp.einsum('japb,apb->j', basis_now, first_pass, precision=highest) / entries
        second_pass = first_pass - jnp.einsum('j,japb->apb', ortho_coeffs, basis_now, precision=highest)
        beta_new = jnp.sqrt(jnp.sum(second_pass * second_pass) / entries + 1e-06)
        next_vector = second_pass / beta_new
        alpha_list.append(alpha_now)
        beta_list.append(beta_new)
        basis_now = jnp.concatenate([basis_now[1:], next_vector[None]], axis=0)
        beta_now = beta_new
    return (next_vector, jnp.stack(alpha_list), jnp.stack(beta_list))
```

```python
import functools

import jax
import jax.numpy as jnp
from jax import lax
from jax.experimental import pallas as pl
from jax.experimental.pallas import tpu as pltpu
from jax.sharding import PartitionSpec as P

VMEM_BYTES = 60 * 1024 * 1024


def params():
    return pltpu.CompilerParams(vmem_limit_bytes=VMEM_BYTES)


def tile_of(size, most):
    return most if size % most == 0 else size


def build_table(left_core, right_core, slot_bond):
    bond_width = left_core.shape[0]
    phys_dim = left_core.shape[2]
    chosen = (slot_bond[:, None] == jnp.arange(bond_width, dtype=jnp.int32)[None, :]).astype(
        jnp.float32
    )
    picked = jnp.einsum("kw,wxac->kxac", chosen, left_core, precision=lax.Precision.HIGHEST)
    table = jnp.einsum("kxac,xybd->kyabcd", picked, right_core, precision=lax.Precision.HIGHEST)
    return table.reshape(bond_width, bond_width, phys_dim * phys_dim, phys_dim * phys_dim)


def mix_kernel(mix_ref, left_ref, cur_ref, out_ref, proj):
    slots, rows, depth = left_ref.shape
    pairs = cur_ref.shape[0]
    bonds = out_ref.shape[0]
    cols = cur_ref.shape[2]

    @pl.loop(0, pairs)
    def _(q):
        proj[q] = jnp.dot(
            left_ref[...].reshape(slots * rows, depth),
            cur_ref[q],
            preferred_element_type=jnp.float32,
        ).reshape(slots, rows, cols)

    @pl.loop(0, rows // 16)
    def _(g):
        mixed = []
        for h in range(2):
            at = pl.ds(pl.multiple_of(g * 16 + h * 8, 8), 8)
            stacked = jnp.concatenate(
                [proj[q, k, at, :] for k in range(slots) for q in range(pairs)], axis=0
            )
            mixed.append(
                jnp.dot(
                    mix_ref[...],
                    stacked,
                    precision=lax.Precision.HIGHEST,
                    preferred_element_type=jnp.float32,
                )
            )
        at = pl.ds(pl.multiple_of(g * 16, 16), 16)
        for y in range(bonds):
            for p in range(pairs):
                i = (y * pairs + p) * 8
                out_ref[y, p, at, :] = jnp.concatenate(
                    [m[i : i + 8] for m in mixed], axis=0
                ).astype(out_ref.dtype)


def mixed_left_of(table, left_k, cur_full):
    slots, rows, depth = left_k.shape
    pairs, _, cols = cur_full.shape
    bonds = table.shape[1]
    tb = tile_of(cols, 256)
    square = table.transpose(1, 2, 0, 3).reshape(bonds * pairs, slots * pairs)
    mix = jnp.kron(square, jnp.eye(8, dtype=jnp.float32))
    return pl.pallas_call(
        mix_kernel,
        grid=(cols // tb,),
        in_specs=[
            pl.BlockSpec(mix.shape, lambda i: (0, 0)),
            pl.BlockSpec((slots, rows, depth), lambda i: (0, 0, 0)),
            pl.BlockSpec((pairs, depth, tb), lambda i: (0, 0, i)),
        ],
        out_specs=pl.BlockSpec((bonds, pairs, rows, tb), lambda i: (0, 0, 0, i)),
        out_shape=jax.ShapeDtypeStruct((bonds, pairs, rows, cols), jnp.bfloat16),
        scratch_shapes=[pltpu.VMEM((pairs, slots, rows, tb), jnp.float32)],
        compiler_params=params(),
        cost_estimate=pl.CostEstimate(
            flops=2 * slots * rows * depth * pairs * cols,
            bytes_accessed=2 * (left_k.size + cur_full.size + bonds * pairs * rows * cols),
            transcendentals=0,
        ),
    )(mix, left_k, cur_full)


def image_kernel(start_ref, mixed_ref, right_ref, out_ref):
    bonds = mixed_ref.shape[0]
    out_ref[...] = jnp.zeros_like(out_ref)

    @pl.loop(0, bonds)
    def _(y):
        out_ref[...] += lax.dot_general(
            mixed_ref[y],
            right_ref[y],
            (((1,), (1,)), ((), ())),
            preferred_element_type=jnp.float32,
        )


def image_part(mixed, right_full, start, count):
    bonds, lines, cols = mixed.shape
    tb = tile_of(count, 256)
    return pl.pallas_call(
        image_kernel,
        grid_spec=pltpu.PrefetchScalarGridSpec(
            num_scalar_prefetch=1,
            grid=(count // tb,),
            in_specs=[
                pl.BlockSpec((bonds, lines, cols), lambda i, s: (0, 0, 0)),
                pl.BlockSpec((bonds, tb, cols), lambda i, s: (0, s[0] + i, 0)),
            ],
            out_specs=pl.BlockSpec((lines, tb), lambda i, s: (0, i)),
        ),
        out_shape=jax.ShapeDtypeStruct((lines, count), jnp.float32),
        compiler_params=params(),
        cost_estimate=pl.CostEstimate(
            flops=2 * bonds * lines * cols * count,
            bytes_accessed=2 * (mixed.size + bonds * count * cols),
            transcendentals=0,
        ),
    )((start // tb).reshape(1).astype(jnp.int32), mixed, right_full)


def gram_kernel(basis_ref, out_ref):
    basis_count, rows, pairs, cols = basis_ref.shape
    chunk = 4
    lanes = cols // 128

    @pl.when(pl.program_id(0) == 0)
    def _():
        out_ref[...] = jnp.zeros_like(out_ref)

    @pl.loop(0, rows // chunk)
    def _(r):
        for c in range(lanes):
            vecs = [
                basis_ref[j, pl.ds(r * chunk, chunk), :, c * 128 : (c + 1) * 128]
                for j in range(basis_count)
            ]
            i = 0
            for j in range(basis_count):
                for k in range(j, basis_count):
                    out_ref[i] += jnp.sum(vecs[j] * vecs[k], axis=0)
                    i += 1


def gram_of(basis):
    basis_count, rows, pairs, cols = basis.shape
    count = basis_count * (basis_count + 1) // 2
    ta = tile_of(rows, 16)
    sums = pl.pallas_call(
        gram_kernel,
        grid=(rows // ta,),
        in_specs=[pl.BlockSpec((basis_count, ta, pairs, cols), lambda i: (0, i, 0, 0))],
        out_specs=pl.BlockSpec((count, pairs, 128), lambda i: (0, 0, 0)),
        out_shape=jax.ShapeDtypeStruct((count, pairs, 128), jnp.float32),
        compiler_params=params(),
        cost_estimate=pl.CostEstimate(
            flops=2 * count * rows * pairs * cols,
            bytes_accessed=4 * basis.size,
            transcendentals=0,
        ),
    )(basis)
    return jnp.sum(sums, axis=(1, 2))


def dots_kernel(basis_ref, image_ref, out_ref):
    basis_count, rows, pairs, cols = basis_ref.shape

    @pl.when(pl.program_id(0) == 0)
    def _():
        out_ref[...] = jnp.zeros_like(out_ref)

    for c in range(cols // 128):
        at = slice(c * 128, (c + 1) * 128)
        image = image_ref[:, :, at]
        for j in range(basis_count):
            out_ref[j] += jnp.sum(basis_ref[j, :, :, at] * image, axis=0)
        out_ref[basis_count] += jnp.sum(image * image, axis=0)


def dots_of(basis, image):
    basis_count, rows, pairs, cols = basis.shape
    ta = tile_of(rows, 16)
    sums = pl.pallas_call(
        dots_kernel,
        grid=(rows // ta,),
        in_specs=[
            pl.BlockSpec((basis_count, ta, pairs, cols), lambda i: (0, i, 0, 0)),
            pl.BlockSpec((ta, pairs, cols), lambda i: (i, 0, 0)),
        ],
        out_specs=pl.BlockSpec((basis_count + 1, pairs, 128), lambda i: (0, 0, 0)),
        out_shape=jax.ShapeDtypeStruct((basis_count + 1, pairs, 128), jnp.float32),
        compiler_params=params(),
    )(basis, image)
    return jnp.sum(sums, axis=(1, 2))


def final_kernel(coef_ref, basis_ref, image_ref, out_ref):
    basis_count = basis_ref.shape[0]
    total = image_ref[...]
    for j in range(basis_count):
        total = total - coef_ref[j] * basis_ref[j]
    out_ref[...] = total * coef_ref[basis_count]


def final_of(coefs, basis, image):
    basis_count, rows, pairs, cols = basis.shape
    ta = tile_of(rows, 16)
    return pl.pallas_call(
        final_kernel,
        grid=(rows // ta,),
        in_specs=[
            pl.BlockSpec(memory_space=pltpu.SMEM),
            pl.BlockSpec((basis_count, ta, pairs, cols), lambda i: (0, i, 0, 0)),
            pl.BlockSpec((ta, pairs, cols), lambda i: (i, 0, 0)),
        ],
        out_specs=pl.BlockSpec((ta, pairs, cols), lambda i: (i, 0, 0)),
        out_shape=jax.ShapeDtypeStruct((rows, pairs, cols), jnp.float32),
        compiler_params=params(),
    )(coefs, basis, image)


MESH = pl.DeviceIdType.MESH


def ring_kernel(
    vec_ref, left_ref, right_ref, mix_ref, basis_ref,
    image_ref, gram_ref,
    vec, left, right, mixed, proj, parts, pair_in, cut_in, gram_buf,
    own_sem, pre_send, pre_recv, vec_send, vec_recv, right_send, right_recv,
    pair_send, pair_recv, cut_send, cut_recv, gram_sem,
):
    chips, pairs, chip_rows, quarter = vec.shape
    slots, _, depth = left.shape
    half_slots, rows, _ = left_ref.shape
    span = right_ref.shape[3]
    last = chips - 1
    polls = 2 * last
    row_tile, col_tile = proj.shape[2], proj.shape[3]
    col_tiles = quarter // col_tile
    mix_units = (chip_rows // row_tile) * col_tiles
    basis_count = basis_ref.shape[0]
    gram_rows = gram_buf.shape[2]
    gram_units = rows // gram_rows
    half = chips // 2

    blk = lax.axis_index("blk")
    cut = lax.axis_index("cuts")
    core = lax.rem(blk, 2)
    chip = blk // 2
    side = lax.rem(chip, 2)
    place = (1 - side) * (chip // 2) + side * (last - chip // 2)

    def chip_at(index):
        index = lax.rem(index + 2 * chips, chips)
        far = index // half
        return (1 - far) * 2 * index + far * (2 * (last - index) + 1)

    after = (2 * chip_at(place + 1) + core, cut)
    before = (2 * chip_at(place - 1) + core, cut)
    onward = (after, before)
    partner = (2 * chip + 1 - core, cut)
    across = (blk, 1 - cut)
    corner = (2 * chip + 1 - core, 1 - cut)

    def remote(src, dst, send, recv, device):
        return pltpu.make_async_remote_copy(
            src_ref=src, dst_ref=dst, send_sem=send, recv_sem=recv,
            device_id=device, device_id_type=MESH,
        )

    def from_place(way, step):
        return chip_at(place - 1 - step) if way == 0 else chip_at(place + 1 + step)

    def vec_copy(way, step, sub, at):
        view = vec.at[at, pl.ds(way * (pairs // 2), pairs // 2), pl.ds(sub * rows, rows), :]
        return remote(
            view, view, vec_send.at[way, step, sub], vec_recv.at[way, step, sub], onward[way]
        )

    def right_copy(way, step, sub, at):
        view = right.at[at, pl.ds(way * rows, rows), pl.ds(sub * span, span)]
        return remote(
            view, view, right_send.at[way, step, sub], right_recv.at[way, step, sub], onward[way]
        )

    def poll(copy_of, index):
        step, sub = index // 2, lax.rem(index, 2)
        for way in range(2):
            at = from_place(way, step)
            copy_of(way, step, sub, at).wait_recv()

            @pl.when(step < last - 1)
            def _():
                copy_of(way, step + 1, sub, at).start()

    def drain(copy_of):
        @pl.loop(0, polls)
        def _(index):
            for way in range(2):
                copy_of(way, index // 2, lax.rem(index, 2), chip).wait_send()

    mine = pl.ds(core * rows, rows)
    vec_own = pltpu.make_async_copy(vec_ref.at[core], vec.at[chip, :, mine, :], own_sem.at[0])
    left_view = left.at[pl.ds(cut * half_slots, half_slots), mine, :]
    left_other = left.at[pl.ds((1 - cut) * half_slots, half_slots), mine, :]
    left_own = pltpu.make_async_copy(left_ref, left_view, own_sem.at[1])
    right_view = right.at[chip, mine, pl.ds(cut * span, span)]
    right_own = pltpu.make_async_copy(right_ref.at[cut, core], right_view, own_sem.at[2])
    vec_own.start()
    left_own.start()
    right_own.start()

    def gram_copy(unit):
        slot = lax.rem(unit, 2)
        return pltpu.make_async_copy(
            basis_ref.at[:, pl.ds(unit * gram_rows, gram_rows), :, :],
            gram_buf.at[slot],
            gram_sem.at[slot],
        )

    barrier = pltpu.get_barrier_semaphore()
    friends = (after, before, partner, across, corner)
    for friend in friends:
        pl.semaphore_signal(barrier, inc=1, device_id=friend, device_id_type=MESH)
    pl.semaphore_wait(barrier, len(friends))

    vec_pre = remote(
        vec_ref.at[1 - core], vec.at[chip, :, mine, :], pre_send.at[0], pre_recv.at[0], partner
    )
    vec_pre.start()
    left_across = remote(left_ref, left_view, pre_send.at[1], pre_recv.at[1], across)
    left_across.start()
    right_pre = (
        remote(right_ref.at[1 - cut, core], right_view, pre_send.at[2], pre_recv.at[2], across),
        remote(
            right_ref.at[1 - cut, 1 - core], right_view, pre_send.at[3], pre_recv.at[3], corner
        ),
        remote(right_ref.at[cut, 1 - core], right_view, pre_send.at[4], pre_recv.at[4], partner),
    )
    for copy in right_pre:
        copy.start()
    left_pair = remote(left_ref, left_view, pre_send.at[5], pre_recv.at[5], partner)
    left_pair.start()
    gram_copy(0).start()
    gram_ref[...] = jnp.zeros_like(gram_ref)

    vec_own.wait()
    vec_pre.wait_recv()
    for sub in range(2):
        for way in range(2):
            vec_copy(way, 0, sub, chip).start()

    def gram_unit(unit):
        slot = lax.rem(unit, 2)
        gram_copy(unit).wait()

        @pl.when(unit + 1 < gram_units)
        def _():
            gram_copy(unit + 1).start()

        chunk = 4

        @pl.loop(0, gram_rows // chunk)
        def _(r):
            for c in range(gram_buf.shape[4] // 128):
                vecs = [
                    gram_buf[slot, j, pl.ds(r * chunk, chunk), :, c * 128 : (c + 1) * 128]
                    for j in range(basis_count)
                ]
                i = 0
                for j in range(basis_count):
                    for k in range(j, basis_count):
                        gram_ref[i] += jnp.sum(vecs[j] * vecs[k], axis=0)
                        i += 1

    @pl.loop(0, polls - 2)
    def _(index):
        poll(vec_copy, index)

        @pl.when(index < gram_units)
        def _():
            gram_unit(index)

    right_own.wait()
    for copy in right_pre:
        copy.wait_recv()
    for sub in range(2):
        for way in range(2):
            right_copy(way, 0, sub, chip).start()

    left_across.wait_recv()
    left_pass = remote(left_other, left_other, pre_send.at[6], pre_recv.at[6], partner)
    left_pass.start()

    @pl.loop(polls - 2, polls)
    def _(index):
        poll(vec_copy, index)

    left_own.wait()
    left_pair.wait_recv()
    left_pass.wait_recv()

    def mix_unit(unit):
        row0 = pl.multiple_of((unit // col_tiles) * row_tile, row_tile)
        col0 = pl.multiple_of(lax.rem(unit, col_tiles) * col_tile, col_tile)

        @pl.loop(0, pairs)
        def _(q):
            proj[q] = jnp.dot(
                left[:, pl.ds(row0, row_tile), :].reshape(slots * row_tile, depth),
                vec[:, q, :, pl.ds(col0, col_tile)].reshape(depth, col_tile),
                preferred_element_type=jnp.float32,
            ).reshape(slots, row_tile, col_tile)

        owner = row0 // rows
        base = owner * (pairs * rows) + row0 - owner * rows

        @pl.loop(0, row_tile // 16)
        def _(g):
            lines = []
            for h in range(2):
                at = pl.ds(pl.multiple_of(g * 16 + h * 8, 8), 8)
                stacked = jnp.concatenate(
                    [proj[q, k, at, :] for k in range(slots) for q in range(pairs)], axis=0
                )
                lines.append(
                    jnp.dot(
                        mix_ref[...],
                        stacked,
                        precision=lax.Precision.HIGHEST,
                        preferred_element_type=jnp.float32,
                    )
                )
            for y in range(slots):
                cols = pl.ds(pl.multiple_of(y * quarter + col0, col_tile), col_tile)
                for p in range(pairs):
                    i = (y * pairs + p) * 8
                    at = pl.ds(pl.multiple_of(base + p * rows + g * 16, 16), 16)
                    mixed[at, cols] = jnp.concatenate(
                        [m[i : i + 8] for m in lines], axis=0
                    ).astype(mixed.dtype)

    lot = pairs * rows

    def pair_copy(unit):
        return remote(
            parts.at[chips + lax.rem(unit, 2)], pair_in.at[unit],
            pair_send.at[unit], pair_recv.at[unit], partner,
        )

    def block_of(unit, way):
        return chip_at(place - unit) if way == 0 else chip_at(place + unit)

    def home_of(unit, way):
        at = block_of(unit, way)
        return at // half, lax.rem(at, half) * 2 + way

    def cut_copy(unit, way):
        _, piece = home_of(unit, way)
        return remote(
            parts.at[unit, way], cut_in.at[piece],
            cut_send.at[unit, way], cut_recv.at[piece], across,
        )

    def image_unit(unit):
        @pl.when(unit >= 2)
        def _():
            pair_copy(unit - 2).wait_send()

        @pl.loop(0, 2)
        def _(k):
            owner = lax.rem(core + 1 + k, 2)
            to = (1 - k) * (chips + lax.rem(unit, 2)) + k * unit
            lines = jnp.concatenate(
                [right[block_of(unit, way), way * rows : (way + 1) * rows, :] for way in range(2)],
                axis=0,
            )
            out = lax.dot_general(
                mixed[pl.ds(pl.multiple_of(owner * lot, lot), lot), :],
                lines,
                (((1,), (1,)), ((), ())),
                preferred_element_type=jnp.float32,
            )
            for way in range(2):
                parts[to, way] = out[:, way * rows : (way + 1) * rows].reshape(pairs, rows, rows)

        pair_copy(unit).start()

    def join_unit(unit):
        pair_copy(unit).wait_recv()
        for way in range(2):
            parts[unit, way] += pair_in[unit, way]
            home, _ = home_of(unit, way)

            @pl.when(home != cut)
            def _():
                cut_copy(unit, way).start()

    @pl.loop(0, mix_units)
    def _(index):
        poll(right_copy, index)
        mix_unit(index)

    def ready(index):
        return jnp.minimum(2 * (index - mix_units + 1), (index + 1) // 2 + 1)

    @pl.loop(mix_units, polls)
    def _(index):
        poll(right_copy, index)

        @pl.loop(ready(index - 1), ready(index))
        def _(unit):
            image_unit(unit)

            @pl.when(unit > 0)
            def _():
                join_unit(unit - 1)

    join_unit(last)

    @pl.loop(0, chips)
    def _(unit):
        for way in range(2):
            home, piece = home_of(unit, way)
            copy = cut_copy(unit, way)

            @pl.when(home == cut)
            def _():
                copy.wait_recv()
                cols = pl.ds(pl.multiple_of(piece * rows, rows), rows)
                image_ref[:, :, cols] = parts[unit, way] + cut_in[piece]

            @pl.when(home != cut)
            def _():
                copy.wait_send()

    drain(vec_copy)
    drain(right_copy)
    for unit in (chips - 2, chips - 1):
        pair_copy(unit).wait_send()
    vec_pre.wait_send()
    left_across.wait_send()
    for copy in right_pre:
        copy.wait_send()
    left_pair.wait_send()
    left_pass.wait_send()


def ring_image(table, left_env, right_env, current, basis):
    rows, half_slots, depth = left_env.shape
    pairs, cols = current.shape[1], current.shape[2]
    slots, chips, quarter = 2 * half_slots, depth // (2 * rows), cols // 2
    basis_count = basis.shape[0]
    count = basis_count * (basis_count + 1) // 2
    square = table.transpose(1, 2, 0, 3).reshape(slots * pairs, slots * pairs)
    mix = jnp.kron(square, jnp.eye(8, dtype=jnp.float32))
    vec = current.reshape(rows, pairs, 2, quarter).transpose(2, 1, 0, 3)
    left = left_env.transpose(1, 0, 2)
    right = right_env.reshape(rows, half_slots, 2, 2, quarter).transpose(2, 3, 0, 1, 4)
    right = right.reshape(2, 2, rows, half_slots * quarter)
    bf16, f32 = jnp.bfloat16, jnp.float32
    sem = pltpu.SemaphoreType.DMA
    steps = chips - 1
    hbm = pl.BlockSpec(memory_space=pltpu.HBM)
    vmem = pl.BlockSpec(memory_space=pltpu.VMEM)
    return pl.pallas_call(
        ring_kernel,
        name="ring",
        in_specs=[hbm, hbm, hbm, vmem, hbm],
        out_specs=[vmem, vmem],
        out_shape=[
            jax.ShapeDtypeStruct((pairs, rows, cols), f32),
            jax.ShapeDtypeStruct((count, pairs, 128), f32),
        ],
        scratch_shapes=[
            pltpu.VMEM((chips, pairs, 2 * rows, quarter), bf16),
            pltpu.VMEM((slots, 2 * rows, depth), bf16),
            pltpu.VMEM((chips, 2 * rows, slots * quarter), bf16),
            pltpu.VMEM((2 * pairs * rows, slots * quarter), bf16),
            pltpu.VMEM((pairs, slots, rows // 2, quarter // 2), f32),
            pltpu.VMEM((chips + 2, 2, pairs, rows, rows), f32),
            pltpu.VMEM((chips, 2, pairs, rows, rows), f32),
            pltpu.VMEM((chips, pairs, rows, rows), f32),
            pltpu.VMEM((2, basis_count, rows // 8, pairs, cols), f32),
            sem((3,)),
            sem((7,)),
            sem((7,)),
            sem((2, steps, 2)),
            sem((2, steps, 2)),
            sem((2, steps, 2)),
            sem((2, steps, 2)),
            sem((chips,)),
            sem((chips,)),
            sem((chips, 2)),
            sem((chips,)),
            sem((2,)),
        ],
        compiler_params=pltpu.CompilerParams(
            vmem_limit_bytes=63 * 1024 * 1024, collective_id=1, has_side_effects=True
        ),
    )(vec, left, right, mix, basis)


def ring_fits(blocks, rows, depth):
    return blocks == 16 and rows * blocks == depth and rows % 128 == 0


def gathered_image(cuts, table, left_env, right_env, current):
    row_count, pair_count, col_count = current.shape
    bond_width = table.shape[0]
    full_width = left_env.shape[2]
    me = lax.axis_index("cuts")
    swap = [(0, 1), (1, 0)]

    current = current.transpose(1, 0, 2)
    left_t = left_env.transpose(1, 0, 2)
    right_t = right_env.transpose(1, 0, 2)
    if cuts == 2:
        half = left_t.shape[0]
        theirs = lax.dynamic_slice_in_dim(right_t, (1 - me) * col_count, col_count, 2)
        mine = lax.dynamic_slice_in_dim(right_t, me * col_count, col_count, 2)
        right_k = jnp.concatenate([mine, lax.ppermute(theirs, "cuts", swap)], axis=0)
        left_k = jnp.concatenate([left_t, lax.ppermute(left_t, "cuts", swap)], axis=0)
        turned = jnp.roll(jnp.roll(table, -half, axis=0), -half, axis=1)
        table = jnp.where(me == 0, table, turned)
    else:
        left_k = lax.all_gather(left_t, "cuts", axis=0, tiled=True)
        right_k = lax.all_to_all(right_t, "cuts", split_axis=2, concat_axis=0, tiled=True)
    cur_full = lax.all_gather(current, "blk", axis=1, tiled=True)
    right_full = lax.all_gather(right_k, "blk", axis=1, tiled=True)

    mixed = mixed_left_of(table, left_k, cur_full)
    mixed = mixed.reshape(bond_width, pair_count * row_count, col_count)
    if cuts == 2:
        away = image_part(mixed, right_full, (1 - me) * col_count, col_count)
        away = lax.ppermute(away, "cuts", swap)
        here = image_part(mixed, right_full, me * col_count, col_count)
        image = here + away
    else:
        image = image_part(mixed, right_full, jnp.int32(0), full_width)
        image = lax.psum_scatter(image, "cuts", scatter_dimension=1, tiled=True)
    return image.reshape(pair_count, row_count, col_count).transpose(1, 0, 2)


def on_device(
    blocks, cuts, left_env, right_env, left_core, right_core, slot_bond, krylov_basis, beta_prev
):
    pair_count = left_core.shape[2] * left_core.shape[2]
    basis_count, row_count, _, _ = krylov_basis.shape
    full_width = left_env.shape[2]
    entries = float(full_width * pair_count * full_width)
    table = build_table(left_core, right_core, slot_bond)
    current = krylov_basis[basis_count - 1].astype(jnp.bfloat16)
    if cuts == 2 and ring_fits(blocks, row_count, full_width):
        image, gram = ring_image(table, left_env, right_env, current, krylov_basis)
        image = image.transpose(1, 0, 2)
        gram = jnp.sum(gram, axis=(1, 2))
    else:
        image = gathered_image(cuts, table, left_env, right_env, current)
        gram = gram_of(krylov_basis)

    sums = lax.psum(jnp.concatenate([gram, dots_of(krylov_basis, image)]), ("blk", "cuts"))
    sums = sums / entries
    count = basis_count * (basis_count + 1) // 2
    where = []
    for j in range(basis_count):
        for k in range(basis_count):
            low, high = min(j, k), max(j, k)
            where.append(low * basis_count - low * (low - 1) // 2 + high - low)
    gram_matrix = sums[jnp.array(where)].reshape(basis_count, basis_count)
    inner_prods = sums[count : count + basis_count]
    image_square = sums[count + basis_count]
    last, prior = basis_count - 1, basis_count - 2
    alpha_now = inner_prods[last]
    ortho_coeffs = (
        inner_prods - alpha_now * gram_matrix[:, last] - beta_prev * gram_matrix[:, prior]
    )
    first_square = (
        image_square
        - 2.0 * alpha_now * inner_prods[last]
        - 2.0 * beta_prev * inner_prods[prior]
        + alpha_now * alpha_now * gram_matrix[last, last]
        + 2.0 * alpha_now * beta_prev * gram_matrix[last, prior]
        + beta_prev * beta_prev * gram_matrix[prior, prior]
    )
    square_mean = (
        first_square
        - 2.0 * jnp.sum(ortho_coeffs * ortho_coeffs)
        + jnp.sum(ortho_coeffs[:, None] * gram_matrix * ortho_coeffs[None, :])
    )
    beta_new = jnp.sqrt(square_mean + 1e-06)
    index = jnp.arange(basis_count)
    coefs = (
        ortho_coeffs
        + jnp.where(index == last, alpha_now, 0.0)
        + jnp.where(index == prior, beta_prev, 0.0)
    )
    coefs = jnp.concatenate([coefs, (1.0 / beta_new)[None]])
    next_vector = final_of(coefs, krylov_basis, image)
    return (next_vector, alpha_now[None], beta_new[None])


def solution(mesh):
    in_specs = (
        P("blk", "cuts", None),
        P("blk", "cuts", None),
        P(),
        P(),
        P(),
        P(None, "blk", None, "cuts"),
        P(),
    )
    out_specs = (P("blk", None, "cuts"), P(), P())
    return jax.shard_map(
        functools.partial(on_device, mesh.shape["blk"], mesh.shape["cuts"]),
        mesh=mesh,
        in_specs=in_specs,
        out_specs=out_specs,
        check_vma=False,
    )
```

```python
import functools

import jax
import jax.numpy as jnp
from jax import lax
from jax.experimental import pallas as pl
from jax.experimental.pallas import tpu as pltpu
from jax.sharding import PartitionSpec as P

VMEM_BYTES = 60 * 1024 * 1024


def params():
    return pltpu.CompilerParams(vmem_limit_bytes=VMEM_BYTES)


def tile_of(size, most):
    return most if size % most == 0 else size


def build_table(left_core, right_core, slot_bond):
    bond_width = left_core.shape[0]
    phys_dim = left_core.shape[2]
    chosen = (slot_bond[:, None] == jnp.arange(bond_width, dtype=jnp.int32)[None, :]).astype(
        jnp.float32
    )
    picked = jnp.einsum("kw,wxac->kxac", chosen, left_core, precision=lax.Precision.HIGHEST)
    table = jnp.einsum("kxac,xybd->kyabcd", picked, right_core, precision=lax.Precision.HIGHEST)
    return table.reshape(bond_width, bond_width, phys_dim * phys_dim, phys_dim * phys_dim)


def mix_kernel(mix_ref, left_ref, cur_ref, out_ref, proj):
    slots, rows, depth = left_ref.shape
    pairs = cur_ref.shape[0]
    bonds = out_ref.shape[0]
    cols = cur_ref.shape[2]

    @pl.loop(0, pairs)
    def _(q):
        proj[q] = jnp.dot(
            left_ref[...].reshape(slots * rows, depth),
            cur_ref[q],
            preferred_element_type=jnp.float32,
        ).reshape(slots, rows, cols)

    @pl.loop(0, rows // 16)
    def _(g):
        mixed = []
        for h in range(2):
            at = pl.ds(pl.multiple_of(g * 16 + h * 8, 8), 8)
            stacked = jnp.concatenate(
                [proj[q, k, at, :] for k in range(slots) for q in range(pairs)], axis=0
            )
            mixed.append(
                jnp.dot(
                    mix_ref[...],
                    stacked,
                    precision=lax.Precision.HIGHEST,
                    preferred_element_type=jnp.float32,
                )
            )
        at = pl.ds(pl.multiple_of(g * 16, 16), 16)
        for y in range(bonds):
            for p in range(pairs):
                i = (y * pairs + p) * 8
                out_ref[y, p, at, :] = jnp.concatenate(
                    [m[i : i + 8] for m in mixed], axis=0
                ).astype(out_ref.dtype)


def mixed_left_of(table, left_k, cur_full):
    slots, rows, depth = left_k.shape
    pairs, _, cols = cur_full.shape
    bonds = table.shape[1]
    tb = tile_of(cols, 256)
    square = table.transpose(1, 2, 0, 3).reshape(bonds * pairs, slots * pairs)
    mix = jnp.kron(square, jnp.eye(8, dtype=jnp.float32))
    return pl.pallas_call(
        mix_kernel,
        grid=(cols // tb,),
        in_specs=[
            pl.BlockSpec(mix.shape, lambda i: (0, 0)),
            pl.BlockSpec((slots, rows, depth), lambda i: (0, 0, 0)),
            pl.BlockSpec((pairs, depth, tb), lambda i: (0, 0, i)),
        ],
        out_specs=pl.BlockSpec((bonds, pairs, rows, tb), lambda i: (0, 0, 0, i)),
        out_shape=jax.ShapeDtypeStruct((bonds, pairs, rows, cols), jnp.bfloat16),
        scratch_shapes=[pltpu.VMEM((pairs, slots, rows, tb), jnp.float32)],
        compiler_params=params(),
        cost_estimate=pl.CostEstimate(
            flops=2 * slots * rows * depth * pairs * cols,
            bytes_accessed=2 * (left_k.size + cur_full.size + bonds * pairs * rows * cols),
            transcendentals=0,
        ),
    )(mix, left_k, cur_full)


def image_kernel(start_ref, mixed_ref, right_ref, out_ref):
    bonds = mixed_ref.shape[0]
    out_ref[...] = jnp.zeros_like(out_ref)

    @pl.loop(0, bonds)
    def _(y):
        out_ref[...] += lax.dot_general(
            mixed_ref[y],
            right_ref[y],
            (((1,), (1,)), ((), ())),
            preferred_element_type=jnp.float32,
        )


def image_part(mixed, right_full, start, count):
    bonds, lines, cols = mixed.shape
    tb = tile_of(count, 256)
    return pl.pallas_call(
        image_kernel,
        grid_spec=pltpu.PrefetchScalarGridSpec(
            num_scalar_prefetch=1,
            grid=(count // tb,),
            in_specs=[
                pl.BlockSpec((bonds, lines, cols), lambda i, s: (0, 0, 0)),
                pl.BlockSpec((bonds, tb, cols), lambda i, s: (0, s[0] + i, 0)),
            ],
            out_specs=pl.BlockSpec((lines, tb), lambda i, s: (0, i)),
        ),
        out_shape=jax.ShapeDtypeStruct((lines, count), jnp.float32),
        compiler_params=params(),
        cost_estimate=pl.CostEstimate(
            flops=2 * bonds * lines * cols * count,
            bytes_accessed=2 * (mixed.size + bonds * count * cols),
            transcendentals=0,
        ),
    )((start // tb).reshape(1).astype(jnp.int32), mixed, right_full)


def gram_kernel(basis_ref, out_ref):
    basis_count, rows, pairs, cols = basis_ref.shape
    chunk = 4
    lanes = cols // 128

    @pl.when(pl.program_id(0) == 0)
    def _():
        out_ref[...] = jnp.zeros_like(out_ref)

    @pl.loop(0, rows // chunk)
    def _(r):
        for c in range(lanes):
            vecs = [
                basis_ref[j, pl.ds(r * chunk, chunk), :, c * 128 : (c + 1) * 128]
                for j in range(basis_count)
            ]
            i = 0
            for j in range(basis_count):
                for k in range(j, basis_count):
                    out_ref[i] += jnp.sum(vecs[j] * vecs[k], axis=0)
                    i += 1


def gram_of(basis):
    basis_count, rows, pairs, cols = basis.shape
    count = basis_count * (basis_count + 1) // 2
    ta = tile_of(rows, 16)
    sums = pl.pallas_call(
        gram_kernel,
        grid=(rows // ta,),
        in_specs=[pl.BlockSpec((basis_count, ta, pairs, cols), lambda i: (0, i, 0, 0))],
        out_specs=pl.BlockSpec((count, pairs, 128), lambda i: (0, 0, 0)),
        out_shape=jax.ShapeDtypeStruct((count, pairs, 128), jnp.float32),
        compiler_params=params(),
        cost_estimate=pl.CostEstimate(
            flops=2 * count * rows * pairs * cols,
            bytes_accessed=4 * basis.size,
            transcendentals=0,
        ),
    )(basis)
    return jnp.sum(sums, axis=(1, 2))


def dots_kernel(basis_ref, image_ref, out_ref):
    basis_count, rows, pairs, cols = basis_ref.shape

    @pl.when(pl.program_id(0) == 0)
    def _():
        out_ref[...] = jnp.zeros_like(out_ref)

    for c in range(cols // 128):
        at = slice(c * 128, (c + 1) * 128)
        image = image_ref[:, :, at]
        for j in range(basis_count):
            out_ref[j] += jnp.sum(basis_ref[j, :, :, at] * image, axis=0)
        out_ref[basis_count] += jnp.sum(image * image, axis=0)


def dots_of(basis, image):
    basis_count, rows, pairs, cols = basis.shape
    ta = tile_of(rows, 16)
    sums = pl.pallas_call(
        dots_kernel,
        grid=(rows // ta,),
        in_specs=[
            pl.BlockSpec((basis_count, ta, pairs, cols), lambda i: (0, i, 0, 0)),
            pl.BlockSpec((ta, pairs, cols), lambda i: (i, 0, 0)),
        ],
        out_specs=pl.BlockSpec((basis_count + 1, pairs, 128), lambda i: (0, 0, 0)),
        out_shape=jax.ShapeDtypeStruct((basis_count + 1, pairs, 128), jnp.float32),
        compiler_params=params(),
    )(basis, image)
    return jnp.sum(sums, axis=(1, 2))


def final_kernel(coef_ref, basis_ref, image_ref, out_ref):
    basis_count = basis_ref.shape[0]
    total = image_ref[...]
    for j in range(basis_count):
        total = total - coef_ref[j] * basis_ref[j]
    out_ref[...] = total * coef_ref[basis_count]


def final_of(coefs, basis, image):
    basis_count, rows, pairs, cols = basis.shape
    ta = tile_of(rows, 16)
    return pl.pallas_call(
        final_kernel,
        grid=(rows // ta,),
        in_specs=[
            pl.BlockSpec(memory_space=pltpu.SMEM),
            pl.BlockSpec((basis_count, ta, pairs, cols), lambda i: (0, i, 0, 0)),
            pl.BlockSpec((ta, pairs, cols), lambda i: (i, 0, 0)),
        ],
        out_specs=pl.BlockSpec((ta, pairs, cols), lambda i: (i, 0, 0)),
        out_shape=jax.ShapeDtypeStruct((rows, pairs, cols), jnp.float32),
        compiler_params=params(),
    )(coefs, basis, image)


MESH = pl.DeviceIdType.MESH


def ring_kernel(
    vec_ref, left_ref, right_ref, mix_ref, basis_ref,
    image_ref, gram_ref,
    vec, left, right, mixed, proj, parts, pair_in, cut_in, gram_buf,
    own_sem, pre_send, pre_recv, vec_send, vec_recv, right_send, right_recv,
    pair_send, pair_recv, cut_send, cut_recv, gram_sem,
):
    chips, pairs, chip_rows, quarter = vec.shape
    slots, _, depth = left.shape
    half_slots, rows, _ = left_ref.shape
    span = right_ref.shape[3]
    last = chips - 1
    polls = 2 * last
    row_tile, col_tile = proj.shape[2], proj.shape[3]
    col_tiles = quarter // col_tile
    mix_units = (chip_rows // row_tile) * col_tiles
    basis_count = basis_ref.shape[0]
    gram_rows = gram_buf.shape[2]
    gram_units = rows // gram_rows
    half = chips // 2

    blk = lax.axis_index("blk")
    cut = lax.axis_index("cuts")
    core = lax.rem(blk, 2)
    chip = blk // 2
    side = lax.rem(chip, 2)
    place = (1 - side) * (chip // 2) + side * (last - chip // 2)

    def chip_at(index):
        index = lax.rem(index + 2 * chips, chips)
        far = index // half
        return (1 - far) * 2 * index + far * (2 * (last - index) + 1)

    after = (2 * chip_at(place + 1) + core, cut)
    before = (2 * chip_at(place - 1) + core, cut)
    onward = (after, before)
    partner = (2 * chip + 1 - core, cut)
    across = (blk, 1 - cut)
    corner = (2 * chip + 1 - core, 1 - cut)

    def remote(src, dst, send, recv, device):
        return pltpu.make_async_remote_copy(
            src_ref=src, dst_ref=dst, send_sem=send, recv_sem=recv,
            device_id=device, device_id_type=MESH,
        )

    def from_place(way, step):
        return chip_at(place - 1 - step) if way == 0 else chip_at(place + 1 + step)

    def vec_copy(way, step, sub, at):
        view = vec.at[at, pl.ds(way * (pairs // 2), pairs // 2), pl.ds(sub * rows, rows), :]
        return remote(
            view, view, vec_send.at[way, step, sub], vec_recv.at[way, step, sub], onward[way]
        )

    def right_copy(way, step, sub, at):
        view = right.at[at, pl.ds(way * rows, rows), pl.ds(sub * span, span)]
        return remote(
            view, view, right_send.at[way, step, sub], right_recv.at[way, step, sub], onward[way]
        )

    def poll(copy_of, index):
        step, sub = index // 2, lax.rem(index, 2)
        for way in range(2):
            at = from_place(way, step)
            copy_of(way, step, sub, at).wait_recv()

            @pl.when(step < last - 1)
            def _():
                copy_of(way, step + 1, sub, at).start()

    def drain(copy_of):
        @pl.loop(0, polls)
        def _(index):
            for way in range(2):
                copy_of(way, index // 2, lax.rem(index, 2), chip).wait_send()

    mine = pl.ds(core * rows, rows)
    vec_own = pltpu.make_async_copy(vec_ref.at[core], vec.at[chip, :, mine, :], own_sem.at[0])
    left_view = left.at[pl.ds(cut * half_slots, half_slots), mine, :]
    left_other = left.at[pl.ds((1 - cut) * half_slots, half_slots), mine, :]
    left_own = pltpu.make_async_copy(left_ref, left_view, own_sem.at[1])
    right_view = right.at[chip, mine, pl.ds(cut * span, span)]
    right_own = pltpu.make_async_copy(right_ref.at[cut, core], right_view, own_sem.at[2])
    vec_own.start()
    left_own.start()
    right_own.start()

    def gram_copy(unit):
        slot = lax.rem(unit, 2)
        return pltpu.make_async_copy(
            basis_ref.at[:, pl.ds(unit * gram_rows, gram_rows), :, :],
            gram_buf.at[slot],
            gram_sem.at[slot],
        )

    barrier = pltpu.get_barrier_semaphore()
    friends = (after, before, partner, across, corner)
    for friend in friends:
        pl.semaphore_signal(barrier, inc=1, device_id=friend, device_id_type=MESH)
    pl.semaphore_wait(barrier, len(friends))

    vec_pre = remote(
        vec_ref.at[1 - core], vec.at[chip, :, mine, :], pre_send.at[0], pre_recv.at[0], partner
    )
    vec_pre.start()
    left_across = remote(left_ref, left_view, pre_send.at[1], pre_recv.at[1], across)
    left_across.start()
    right_pre = (
        remote(right_ref.at[1 - cut, core], right_view, pre_send.at[2], pre_recv.at[2], across),
        remote(
            right_ref.at[1 - cut, 1 - core], right_view, pre_send.at[3], pre_recv.at[3], corner
        ),
        remote(right_ref.at[cut, 1 - core], right_view, pre_send.at[4], pre_recv.at[4], partner),
    )
    for copy in right_pre:
        copy.start()
    left_pair = remote(left_ref, left_view, pre_send.at[5], pre_recv.at[5], partner)
    left_pair.start()
    gram_copy(0).start()
    gram_ref[...] = jnp.zeros_like(gram_ref)

    vec_own.wait()
    vec_pre.wait_recv()
    for sub in range(2):
        for way in range(2):
            vec_copy(way, 0, sub, chip).start()

    def gram_unit(unit):
        slot = lax.rem(unit, 2)
        gram_copy(unit).wait()

        @pl.when(unit + 1 < gram_units)
        def _():
            gram_copy(unit + 1).start()

        chunk = 4

        @pl.loop(0, gram_rows // chunk)
        def _(r):
            for c in range(gram_buf.shape[4] // 128):
                vecs = [
                    gram_buf[slot, j, pl.ds(r * chunk, chunk), :, c * 128 : (c + 1) * 128]
                    for j in range(basis_count)
                ]
                i = 0
                for j in range(basis_count):
                    for k in range(j, basis_count):
                        gram_ref[i] += jnp.sum(vecs[j] * vecs[k], axis=0)
                        i += 1

    @pl.loop(0, polls - 2)
    def _(index):
        poll(vec_copy, index)

        @pl.when(index < gram_units)
        def _():
            gram_unit(index)

    right_own.wait()
    for copy in right_pre:
        copy.wait_recv()
    for sub in range(2):
        for way in range(2):
            right_copy(way, 0, sub, chip).start()

    left_across.wait_recv()
    left_pass = remote(left_other, left_other, pre_send.at[6], pre_recv.at[6], partner)
    left_pass.start()

    @pl.loop(polls - 2, polls)
    def _(index):
        poll(vec_copy, index)

    left_own.wait()
    left_pair.wait_recv()
    left_pass.wait_recv()

    def mix_unit(unit):
        row0 = pl.multiple_of((unit // col_tiles) * row_tile, row_tile)
        col0 = pl.multiple_of(lax.rem(unit, col_tiles) * col_tile, col_tile)

        @pl.loop(0, pairs)
        def _(q):
            proj[q] = jnp.dot(
                left[:, pl.ds(row0, row_tile), :].reshape(slots * row_tile, depth),
                vec[:, q, :, pl.ds(col0, col_tile)].reshape(depth, col_tile),
                preferred_element_type=jnp.float32,
            ).reshape(slots, row_tile, col_tile)

        owner = row0 // rows
        base = owner * (pairs * rows) + row0 - owner * rows

        @pl.loop(0, row_tile // 16)
        def _(g):
            lines = []
            for h in range(2):
                at = pl.ds(pl.multiple_of(g * 16 + h * 8, 8), 8)
                stacked = jnp.concatenate(
                    [proj[q, k, at, :] for k in range(slots) for q in range(pairs)], axis=0
                )
                lines.append(
                    jnp.dot(
                        mix_ref[...],
                        stacked,
                        precision=lax.Precision.HIGHEST,
                        preferred_element_type=jnp.float32,
                    )
                )
            for y in range(slots):
                cols = pl.ds(pl.multiple_of(y * quarter + col0, col_tile), col_tile)
                for p in range(pairs):
                    i = (y * pairs + p) * 8
                    at = pl.ds(pl.multiple_of(base + p * rows + g * 16, 16), 16)
                    mixed[at, cols] = jnp.concatenate(
                        [m[i : i + 8] for m in lines], axis=0
                    ).astype(mixed.dtype)

    lot = pairs * rows

    def pair_copy(unit):
        return remote(
            parts.at[chips + lax.rem(unit, 2)], pair_in.at[unit],
            pair_send.at[unit], pair_recv.at[unit], partner,
        )

    def block_of(unit, way):
        return chip_at(place - unit) if way == 0 else chip_at(place + unit)

    def home_of(unit, way):
        at = block_of(unit, way)
        return at // half, lax.rem(at, half) * 2 + way

    def cut_copy(unit, way):
        _, piece = home_of(unit, way)
        return remote(
            parts.at[unit, way], cut_in.at[piece],
            cut_send.at[unit, way], cut_recv.at[piece], across,
        )

    def image_unit(unit):
        @pl.when(unit >= 2)
        def _():
            pair_copy(unit - 2).wait_send()

        @pl.loop(0, 2)
        def _(k):
            owner = lax.rem(core + 1 + k, 2)
            to = (1 - k) * (chips + lax.rem(unit, 2)) + k * unit
            lines = jnp.concatenate(
                [right[block_of(unit, way), way * rows : (way + 1) * rows, :] for way in range(2)],
                axis=0,
            )
            out = lax.dot_general(
                mixed[pl.ds(pl.multiple_of(owner * lot, lot), lot), :],
                lines,
                (((1,), (1,)), ((), ())),
                preferred_element_type=jnp.float32,
            )
            for way in range(2):
                parts[to, way] = out[:, way * rows : (way + 1) * rows].reshape(pairs, rows, rows)

        pair_copy(unit).start()

    def join_unit(unit):
        pair_copy(unit).wait_recv()
        for way in range(2):
            parts[unit, way] += pair_in[unit, way]
            home, _ = home_of(unit, way)

            @pl.when(home != cut)
            def _():
                cut_copy(unit, way).start()

    @pl.loop(0, mix_units)
    def _(index):
        poll(right_copy, index)
        mix_unit(index)

    def ready(index):
        return jnp.minimum(2 * (index - mix_units + 1), (index + 1) // 2 + 1)

    @pl.loop(mix_units, polls)
    def _(index):
        poll(right_copy, index)

        @pl.loop(ready(index - 1), ready(index))
        def _(unit):
            image_unit(unit)

            @pl.when(unit > 0)
            def _():
                join_unit(unit - 1)

    join_unit(last)

    @pl.loop(0, chips)
    def _(unit):
        for way in range(2):
            home, piece = home_of(unit, way)
            copy = cut_copy(unit, way)

            @pl.when(home == cut)
            def _():
                copy.wait_recv()
                cols = pl.ds(pl.multiple_of(piece * rows, rows), rows)
                whole = parts[unit, way] + cut_in[piece]
                for p in range(pairs):
                    image_ref[:, p, cols] = whole[p]

            @pl.when(home != cut)
            def _():
                copy.wait_send()

    drain(vec_copy)
    drain(right_copy)
    for unit in (chips - 2, chips - 1):
        pair_copy(unit).wait_send()
    vec_pre.wait_send()
    left_across.wait_send()
    for copy in right_pre:
        copy.wait_send()
    left_pair.wait_send()
    left_pass.wait_send()


def ring_image(table, left_env, right_env, current, basis):
    rows, half_slots, depth = left_env.shape
    pairs, cols = current.shape[1], current.shape[2]
    slots, chips, quarter = 2 * half_slots, depth // (2 * rows), cols // 2
    basis_count = basis.shape[0]
    count = basis_count * (basis_count + 1) // 2
    square = table.transpose(1, 2, 0, 3).reshape(slots * pairs, slots * pairs)
    mix = jnp.kron(square, jnp.eye(8, dtype=jnp.float32))
    vec = current.reshape(rows, pairs, 2, quarter).transpose(2, 1, 0, 3)
    left = left_env.transpose(1, 0, 2)
    right = right_env.reshape(rows, half_slots, 2, 2, quarter).transpose(2, 3, 0, 1, 4)
    right = right.reshape(2, 2, rows, half_slots * quarter)
    bf16, f32 = jnp.bfloat16, jnp.float32
    sem = pltpu.SemaphoreType.DMA
    steps = chips - 1
    hbm = pl.BlockSpec(memory_space=pltpu.HBM)
    vmem = pl.BlockSpec(memory_space=pltpu.VMEM)
    return pl.pallas_call(
        ring_kernel,
        name="ring",
        in_specs=[hbm, hbm, hbm, vmem, hbm],
        out_specs=[vmem, vmem],
        out_shape=[
            jax.ShapeDtypeStruct((rows, pairs, cols), f32),
            jax.ShapeDtypeStruct((count, pairs, 128), f32),
        ],
        scratch_shapes=[
            pltpu.VMEM((chips, pairs, 2 * rows, quarter), bf16),
            pltpu.VMEM((slots, 2 * rows, depth), bf16),
            pltpu.VMEM((chips, 2 * rows, slots * quarter), bf16),
            pltpu.VMEM((2 * pairs * rows, slots * quarter), bf16),
            pltpu.VMEM((pairs, slots, rows // 2, quarter // 2), f32),
            pltpu.VMEM((chips + 2, 2, pairs, rows, rows), f32),
            pltpu.VMEM((chips, 2, pairs, rows, rows), f32),
            pltpu.VMEM((chips, pairs, rows, rows), f32),
            pltpu.VMEM((2, basis_count, rows // 8, pairs, cols), f32),
            sem((3,)),
            sem((7,)),
            sem((7,)),
            sem((2, steps, 2)),
            sem((2, steps, 2)),
            sem((2, steps, 2)),
            sem((2, steps, 2)),
            sem((chips,)),
            sem((chips,)),
            sem((chips, 2)),
            sem((chips,)),
            sem((2,)),
        ],
        compiler_params=pltpu.CompilerParams(
            vmem_limit_bytes=63 * 1024 * 1024, collective_id=1, has_side_effects=True
        ),
    )(vec, left, right, mix, basis)


def finish_kernel(
    blocks, cuts, entries,
    beta_ref, gram_ref, image_ref, basis_ref,
    next_ref, values_ref,
    basis, tile, inbox, load_sem, send_sem, recv_sem,
):
    basis_count, rows, pairs, cols = basis.shape
    chunks = load_sem.shape[0]
    chunk = rows // chunks
    lanes = cols // 128
    devices = blocks * cuts
    me = lax.axis_index("blk") * cuts + lax.axis_index("cuts")

    def load(unit):
        at = pl.ds(unit * chunk, chunk)
        return pltpu.make_async_copy(
            basis_ref.at[:, at, :, :], basis.at[:, at, :, :], load_sem.at[unit]
        )

    for unit in range(chunks):
        load(unit).start()

    def place(offset):
        device = lax.rem(me + offset, devices)
        return (device // cuts, lax.rem(device, cuts))

    barrier = pltpu.get_barrier_semaphore()
    for offset in range(1, devices):
        pl.semaphore_signal(barrier, inc=1, device_id=place(offset), device_id_type=MESH)

    row = lax.broadcasted_iota(jnp.int32, tile.shape, 0)
    lane = lax.broadcasted_iota(jnp.int32, tile.shape, 1)

    def total_of(x):
        return jnp.sum(jnp.sum(x, axis=0, keepdims=True), axis=1, keepdims=True)

    found = jnp.zeros(tile.shape, jnp.float32)
    i = 0
    for j in range(basis_count):
        for k in range(j, basis_count):
            here = ((row == j) & (lane == k)) | ((row == k) & (lane == j))
            found = jnp.where(here, total_of(gram_ref[i]), found)
            i += 1
    tile[...] = found

    def dots(unit, sums):
        load(unit).wait()
        for c in range(lanes):
            at = slice(c * 128, (c + 1) * 128)
            for step in range(chunk // 8):
                r = pl.ds(unit * chunk + step * 8, 8)
                image = image_ref[r, :, at]
                sums = tuple(
                    sums[j] + jnp.sum(basis[j, r, :, at] * image, axis=0)
                    for j in range(basis_count)
                ) + (sums[basis_count] + jnp.sum(image * image, axis=0),)
        return sums

    zero = jnp.zeros((pairs, 128), jnp.float32)
    sums = lax.fori_loop(0, chunks, dots, (zero,) * (basis_count + 1))
    found = tile[...]
    for j in range(basis_count + 1):
        here = ((row == j) & (lane == basis_count)) | ((row == basis_count) & (lane == j))
        found = jnp.where(here, total_of(sums[j]), found)
    tile[...] = found
    inbox[me] = found

    pl.semaphore_wait(barrier, devices - 1)

    def send(offset):
        return pltpu.make_async_remote_copy(
            src_ref=tile, dst_ref=inbox.at[me],
            send_sem=send_sem.at[offset], recv_sem=recv_sem.at[offset],
            device_id=place(offset), device_id_type=MESH,
        )

    for offset in range(1, devices):
        send(offset).start()
    for offset in range(1, devices):
        send(offset).wait_recv()

    sums = inbox[0]
    for d in range(1, devices):
        sums = sums + inbox[d]
    sums = sums / entries
    n, last, prior = basis_count, basis_count - 1, basis_count - 2
    gram = sums[0:n, 0:n]
    down, along = sums[0:n, n : n + 1], sums[n : n + 1, 0:n]
    square = sums[n : n + 1, n : n + 1]
    alpha = down[last : last + 1]
    beta = jnp.full((1, 1), beta_ref[0], jnp.float32)
    ortho = down - alpha * gram[:, last : last + 1] - beta * gram[:, prior : prior + 1]
    ortho_row = along - alpha * gram[last : last + 1, :] - beta * gram[prior : prior + 1, :]
    first = (
        square
        - 2.0 * alpha * alpha
        - 2.0 * beta * down[prior : prior + 1]
        + alpha * alpha * gram[last : last + 1, last : last + 1]
        + 2.0 * alpha * beta * gram[last : last + 1, prior : prior + 1]
        + beta * beta * gram[prior : prior + 1, prior : prior + 1]
    )
    bent = jnp.sum(ortho * gram, axis=0, keepdims=True) * ortho_row
    mean = (
        first
        - 2.0 * jnp.sum(ortho * ortho, axis=0, keepdims=True)
        + jnp.sum(bent, axis=1, keepdims=True)
    )
    beta_new = jnp.sqrt(mean + 1e-06)
    values_ref[...] = jnp.where(
        (row == 0) & (lane == 0), alpha, jnp.where((row == 0) & (lane == 1), beta_new, 0.0)
    )
    index = lax.broadcasted_iota(jnp.int32, ortho.shape, 0)
    coefs = (
        ortho + jnp.where(index == last, alpha, 0.0) + jnp.where(index == prior, beta, 0.0)
    )
    spread = [jnp.broadcast_to(coefs[j : j + 1], (pairs, 128)) for j in range(n)]
    scale = jnp.broadcast_to(1.0 / beta_new, (pairs, 128))

    @pl.loop(0, rows // 8)
    def _(step):
        r = pl.ds(step * 8, 8)
        for c in range(lanes):
            at = slice(c * 128, (c + 1) * 128)
            value = image_ref[r, :, at]
            for j in range(n):
                value = value - spread[j][None] * basis[j, r, :, at]
            next_ref[r, :, at] = value * scale[None]

    for offset in range(1, devices):
        send(offset).wait_send()


def finish(blocks, cuts, entries, beta_prev, gram, image, basis):
    basis_count, rows, pairs, cols = basis.shape
    tile = (16, 128)
    devices = blocks * cuts
    sem = pltpu.SemaphoreType.DMA
    vmem = pl.BlockSpec(memory_space=pltpu.VMEM)
    next_vector, values = pl.pallas_call(
        functools.partial(finish_kernel, blocks, cuts, entries),
        name="finish",
        in_specs=[
            pl.BlockSpec(memory_space=pltpu.SMEM),
            vmem,
            vmem,
            pl.BlockSpec(memory_space=pltpu.HBM),
        ],
        out_specs=[vmem, vmem],
        out_shape=[
            jax.ShapeDtypeStruct((rows, pairs, cols), jnp.float32),
            jax.ShapeDtypeStruct(tile, jnp.float32),
        ],
        scratch_shapes=[
            pltpu.VMEM(basis.shape, jnp.float32),
            pltpu.VMEM(tile, jnp.float32),
            pltpu.VMEM((devices,) + tile, jnp.float32),
            sem((rows // 16,)),
            sem((devices,)),
            sem((devices,)),
        ],
        compiler_params=pltpu.CompilerParams(
            vmem_limit_bytes=40 * 1024 * 1024, collective_id=2, has_side_effects=True
        ),
    )(beta_prev.reshape(1), gram, image, basis)
    return next_vector, values[0, 0:1], values[0, 1:2]


def ring_fits(blocks, rows, depth):
    return blocks == 16 and rows * blocks == depth and rows % 128 == 0


def gathered_image(cuts, table, left_env, right_env, current):
    row_count, pair_count, col_count = current.shape
    bond_width = table.shape[0]
    full_width = left_env.shape[2]
    me = lax.axis_index("cuts")
    swap = [(0, 1), (1, 0)]

    current = current.transpose(1, 0, 2)
    left_t = left_env.transpose(1, 0, 2)
    right_t = right_env.transpose(1, 0, 2)
    if cuts == 2:
        half = left_t.shape[0]
        theirs = lax.dynamic_slice_in_dim(right_t, (1 - me) * col_count, col_count, 2)
        mine = lax.dynamic_slice_in_dim(right_t, me * col_count, col_count, 2)
        right_k = jnp.concatenate([mine, lax.ppermute(theirs, "cuts", swap)], axis=0)
        left_k = jnp.concatenate([left_t, lax.ppermute(left_t, "cuts", swap)], axis=0)
        turned = jnp.roll(jnp.roll(table, -half, axis=0), -half, axis=1)
        table = jnp.where(me == 0, table, turned)
    else:
        left_k = lax.all_gather(left_t, "cuts", axis=0, tiled=True)
        right_k = lax.all_to_all(right_t, "cuts", split_axis=2, concat_axis=0, tiled=True)
    cur_full = lax.all_gather(current, "blk", axis=1, tiled=True)
    right_full = lax.all_gather(right_k, "blk", axis=1, tiled=True)

    mixed = mixed_left_of(table, left_k, cur_full)
    mixed = mixed.reshape(bond_width, pair_count * row_count, col_count)
    if cuts == 2:
        away = image_part(mixed, right_full, (1 - me) * col_count, col_count)
        away = lax.ppermute(away, "cuts", swap)
        here = image_part(mixed, right_full, me * col_count, col_count)
        image = here + away
    else:
        image = image_part(mixed, right_full, jnp.int32(0), full_width)
        image = lax.psum_scatter(image, "cuts", scatter_dimension=1, tiled=True)
    return image.reshape(pair_count, row_count, col_count).transpose(1, 0, 2)


def on_device(
    blocks, cuts, left_env, right_env, left_core, right_core, slot_bond, krylov_basis, beta_prev
):
    pair_count = left_core.shape[2] * left_core.shape[2]
    basis_count, row_count, _, _ = krylov_basis.shape
    full_width = left_env.shape[2]
    entries = float(full_width * pair_count * full_width)
    table = build_table(left_core, right_core, slot_bond)
    current = krylov_basis[basis_count - 1].astype(jnp.bfloat16)
    if cuts == 2 and ring_fits(blocks, row_count, full_width):
        image, gram = ring_image(table, left_env, right_env, current, krylov_basis)
        return finish(blocks, cuts, entries, beta_prev, gram, image, krylov_basis)
    image = gathered_image(cuts, table, left_env, right_env, current)
    gram = gram_of(krylov_basis)

    sums = lax.psum(jnp.concatenate([gram, dots_of(krylov_basis, image)]), ("blk", "cuts"))
    sums = sums / entries
    count = basis_count * (basis_count + 1) // 2
    where = []
    for j in range(basis_count):
        for k in range(basis_count):
            low, high = min(j, k), max(j, k)
            where.append(low * basis_count - low * (low - 1) // 2 + high - low)
    gram_matrix = sums[jnp.array(where)].reshape(basis_count, basis_count)
    inner_prods = sums[count : count + basis_count]
    image_square = sums[count + basis_count]
    last, prior = basis_count - 1, basis_count - 2
    alpha_now = inner_prods[last]
    ortho_coeffs = (
        inner_prods - alpha_now * gram_matrix[:, last] - beta_prev * gram_matrix[:, prior]
    )
    first_square = (
        image_square
        - 2.0 * alpha_now * inner_prods[last]
        - 2.0 * beta_prev * inner_prods[prior]
        + alpha_now * alpha_now * gram_matrix[last, last]
        + 2.0 * alpha_now * beta_prev * gram_matrix[last, prior]
        + beta_prev * beta_prev * gram_matrix[prior, prior]
    )
    square_mean = (
        first_square
        - 2.0 * jnp.sum(ortho_coeffs * ortho_coeffs)
        + jnp.sum(ortho_coeffs[:, None] * gram_matrix * ortho_coeffs[None, :])
    )
    beta_new = jnp.sqrt(square_mean + 1e-06)
    index = jnp.arange(basis_count)
    coefs = (
        ortho_coeffs
        + jnp.where(index == last, alpha_now, 0.0)
        + jnp.where(index == prior, beta_prev, 0.0)
    )
    coefs = jnp.concatenate([coefs, (1.0 / beta_new)[None]])
    next_vector = final_of(coefs, krylov_basis, image)
    return (next_vector, alpha_now[None], beta_new[None])


def solution(mesh):
    in_specs = (
        P("blk", "cuts", None),
        P("blk", "cuts", None),
        P(),
        P(),
        P(),
        P(None, "blk", None, "cuts"),
        P(),
    )
    out_specs = (P("blk", None, "cuts"), P(), P())
    return jax.shard_map(
        functools.partial(on_device, mesh.shape["blk"], mesh.shape["cuts"]),
        mesh=mesh,
        in_specs=in_specs,
        out_specs=out_specs,
        check_vma=False,
    )
```

```python
import functools

import jax
import jax.numpy as jnp
from jax import lax
from jax.experimental import pallas as pl
from jax.experimental.pallas import tpu as pltpu
from jax.sharding import PartitionSpec as P

VMEM_BYTES = 60 * 1024 * 1024


def params():
    return pltpu.CompilerParams(vmem_limit_bytes=VMEM_BYTES)


def tile_of(size, most):
    return most if size % most == 0 else size


def build_table(left_core, right_core, slot_bond):
    bond_width = left_core.shape[0]
    phys_dim = left_core.shape[2]
    chosen = (slot_bond[:, None] == jnp.arange(bond_width, dtype=jnp.int32)[None, :]).astype(
        jnp.float32
    )
    picked = jnp.einsum("kw,wxac->kxac", chosen, left_core, precision=lax.Precision.HIGHEST)
    table = jnp.einsum("kxac,xybd->kyabcd", picked, right_core, precision=lax.Precision.HIGHEST)
    return table.reshape(bond_width, bond_width, phys_dim * phys_dim, phys_dim * phys_dim)


def mix_kernel(mix_ref, left_ref, cur_ref, out_ref, proj):
    slots, rows, depth = left_ref.shape
    pairs = cur_ref.shape[0]
    bonds = out_ref.shape[0]
    cols = cur_ref.shape[2]

    @pl.loop(0, pairs)
    def _(q):
        proj[q] = jnp.dot(
            left_ref[...].reshape(slots * rows, depth),
            cur_ref[q],
            preferred_element_type=jnp.float32,
        ).reshape(slots, rows, cols)

    @pl.loop(0, rows // 16)
    def _(g):
        mixed = []
        for h in range(2):
            at = pl.ds(pl.multiple_of(g * 16 + h * 8, 8), 8)
            stacked = jnp.concatenate(
                [proj[q, k, at, :] for k in range(slots) for q in range(pairs)], axis=0
            )
            mixed.append(
                jnp.dot(
                    mix_ref[...],
                    stacked,
                    precision=lax.Precision.HIGHEST,
                    preferred_element_type=jnp.float32,
                )
            )
        at = pl.ds(pl.multiple_of(g * 16, 16), 16)
        for y in range(bonds):
            for p in range(pairs):
                i = (y * pairs + p) * 8
                out_ref[y, p, at, :] = jnp.concatenate(
                    [m[i : i + 8] for m in mixed], axis=0
                ).astype(out_ref.dtype)


def mixed_left_of(table, left_k, cur_full):
    slots, rows, depth = left_k.shape
    pairs, _, cols = cur_full.shape
    bonds = table.shape[1]
    tb = tile_of(cols, 256)
    square = table.transpose(1, 2, 0, 3).reshape(bonds * pairs, slots * pairs)
    mix = jnp.kron(square, jnp.eye(8, dtype=jnp.float32))
    return pl.pallas_call(
        mix_kernel,
        grid=(cols // tb,),
        in_specs=[
            pl.BlockSpec(mix.shape, lambda i: (0, 0)),
            pl.BlockSpec((slots, rows, depth), lambda i: (0, 0, 0)),
            pl.BlockSpec((pairs, depth, tb), lambda i: (0, 0, i)),
        ],
        out_specs=pl.BlockSpec((bonds, pairs, rows, tb), lambda i: (0, 0, 0, i)),
        out_shape=jax.ShapeDtypeStruct((bonds, pairs, rows, cols), jnp.bfloat16),
        scratch_shapes=[pltpu.VMEM((pairs, slots, rows, tb), jnp.float32)],
        compiler_params=params(),
        cost_estimate=pl.CostEstimate(
            flops=2 * slots * rows * depth * pairs * cols,
            bytes_accessed=2 * (left_k.size + cur_full.size + bonds * pairs * rows * cols),
            transcendentals=0,
        ),
    )(mix, left_k, cur_full)


def image_kernel(start_ref, mixed_ref, right_ref, out_ref):
    bonds = mixed_ref.shape[0]
    out_ref[...] = jnp.zeros_like(out_ref)

    @pl.loop(0, bonds)
    def _(y):
        out_ref[...] += lax.dot_general(
            mixed_ref[y],
            right_ref[y],
            (((1,), (1,)), ((), ())),
            preferred_element_type=jnp.float32,
        )


def image_part(mixed, right_full, start, count):
    bonds, lines, cols = mixed.shape
    tb = tile_of(count, 256)
    return pl.pallas_call(
        image_kernel,
        grid_spec=pltpu.PrefetchScalarGridSpec(
            num_scalar_prefetch=1,
            grid=(count // tb,),
            in_specs=[
                pl.BlockSpec((bonds, lines, cols), lambda i, s: (0, 0, 0)),
                pl.BlockSpec((bonds, tb, cols), lambda i, s: (0, s[0] + i, 0)),
            ],
            out_specs=pl.BlockSpec((lines, tb), lambda i, s: (0, i)),
        ),
        out_shape=jax.ShapeDtypeStruct((lines, count), jnp.float32),
        compiler_params=params(),
        cost_estimate=pl.CostEstimate(
            flops=2 * bonds * lines * cols * count,
            bytes_accessed=2 * (mixed.size + bonds * count * cols),
            transcendentals=0,
        ),
    )((start // tb).reshape(1).astype(jnp.int32), mixed, right_full)


def gram_kernel(basis_ref, out_ref):
    basis_count, rows, pairs, cols = basis_ref.shape
    chunk = 4
    lanes = cols // 128

    @pl.when(pl.program_id(0) == 0)
    def _():
        out_ref[...] = jnp.zeros_like(out_ref)

    @pl.loop(0, rows // chunk)
    def _(r):
        for c in range(lanes):
            vecs = [
                basis_ref[j, pl.ds(r * chunk, chunk), :, c * 128 : (c + 1) * 128]
                for j in range(basis_count)
            ]
            i = 0
            for j in range(basis_count):
                for k in range(j, basis_count):
                    out_ref[i] += jnp.sum(vecs[j] * vecs[k], axis=0)
                    i += 1


def gram_of(basis):
    basis_count, rows, pairs, cols = basis.shape
    count = basis_count * (basis_count + 1) // 2
    ta = tile_of(rows, 16)
    sums = pl.pallas_call(
        gram_kernel,
        grid=(rows // ta,),
        in_specs=[pl.BlockSpec((basis_count, ta, pairs, cols), lambda i: (0, i, 0, 0))],
        out_specs=pl.BlockSpec((count, pairs, 128), lambda i: (0, 0, 0)),
        out_shape=jax.ShapeDtypeStruct((count, pairs, 128), jnp.float32),
        compiler_params=params(),
        cost_estimate=pl.CostEstimate(
            flops=2 * count * rows * pairs * cols,
            bytes_accessed=4 * basis.size,
            transcendentals=0,
        ),
    )(basis)
    return jnp.sum(sums, axis=(1, 2))


def dots_kernel(basis_ref, image_ref, out_ref):
    basis_count, rows, pairs, cols = basis_ref.shape

    @pl.when(pl.program_id(0) == 0)
    def _():
        out_ref[...] = jnp.zeros_like(out_ref)

    for c in range(cols // 128):
        at = slice(c * 128, (c + 1) * 128)
        image = image_ref[:, :, at]
        for j in range(basis_count):
            out_ref[j] += jnp.sum(basis_ref[j, :, :, at] * image, axis=0)
        out_ref[basis_count] += jnp.sum(image * image, axis=0)


def dots_of(basis, image):
    basis_count, rows, pairs, cols = basis.shape
    ta = tile_of(rows, 16)
    sums = pl.pallas_call(
        dots_kernel,
        grid=(rows // ta,),
        in_specs=[
            pl.BlockSpec((basis_count, ta, pairs, cols), lambda i: (0, i, 0, 0)),
            pl.BlockSpec((ta, pairs, cols), lambda i: (i, 0, 0)),
        ],
        out_specs=pl.BlockSpec((basis_count + 1, pairs, 128), lambda i: (0, 0, 0)),
        out_shape=jax.ShapeDtypeStruct((basis_count + 1, pairs, 128), jnp.float32),
        compiler_params=params(),
    )(basis, image)
    return jnp.sum(sums, axis=(1, 2))


def final_kernel(coef_ref, basis_ref, image_ref, out_ref):
    basis_count = basis_ref.shape[0]
    total = image_ref[...]
    for j in range(basis_count):
        total = total - coef_ref[j] * basis_ref[j]
    out_ref[...] = total * coef_ref[basis_count]


def final_of(coefs, basis, image):
    basis_count, rows, pairs, cols = basis.shape
    ta = tile_of(rows, 16)
    return pl.pallas_call(
        final_kernel,
        grid=(rows // ta,),
        in_specs=[
            pl.BlockSpec(memory_space=pltpu.SMEM),
            pl.BlockSpec((basis_count, ta, pairs, cols), lambda i: (0, i, 0, 0)),
            pl.BlockSpec((ta, pairs, cols), lambda i: (i, 0, 0)),
        ],
        out_specs=pl.BlockSpec((ta, pairs, cols), lambda i: (i, 0, 0)),
        out_shape=jax.ShapeDtypeStruct((rows, pairs, cols), jnp.float32),
        compiler_params=params(),
    )(coefs, basis, image)


MESH = pl.DeviceIdType.MESH


def ring_kernel(
    vec_ref, left_ref, right_ref, square_ref, basis_ref,
    image_ref, gram_ref,
    vec, left, right, mixed, mix_ref, proj, parts, pair_in, cut_in, gram_buf,
    own_sem, pre_send, pre_recv, vec_send, vec_recv, right_send, right_recv,
    pair_send, pair_recv, cut_send, cut_recv, gram_sem,
):
    chips, pairs, chip_rows, quarter = vec.shape
    slots, _, depth = left.shape
    half_slots, rows, _ = left_ref.shape
    span = half_slots * quarter
    last = chips - 1
    polls = 2 * last
    row_tile, col_tile = proj.shape[2], proj.shape[3]
    col_tiles = quarter // col_tile
    mix_units = (chip_rows // row_tile) * col_tiles
    basis_count = basis_ref.shape[0]
    gram_rows = gram_buf.shape[2]
    gram_units = rows // gram_rows
    half = chips // 2

    blk = lax.axis_index("blk")
    cut = lax.axis_index("cuts")
    core = lax.rem(blk, 2)
    chip = blk // 2
    side = lax.rem(chip, 2)
    place = (1 - side) * (chip // 2) + side * (last - chip // 2)

    def chip_at(index):
        index = lax.rem(index + 2 * chips, chips)
        far = index // half
        return (1 - far) * 2 * index + far * (2 * (last - index) + 1)

    after = (2 * chip_at(place + 1) + core, cut)
    before = (2 * chip_at(place - 1) + core, cut)
    onward = (after, before)
    partner = (2 * chip + 1 - core, cut)
    across = (blk, 1 - cut)
    corner = (2 * chip + 1 - core, 1 - cut)

    def remote(src, dst, send, recv, device):
        return pltpu.make_async_remote_copy(
            src_ref=src, dst_ref=dst, send_sem=send, recv_sem=recv,
            device_id=device, device_id_type=MESH,
        )

    def from_place(way, step):
        return chip_at(place - 1 - step) if way == 0 else chip_at(place + 1 + step)

    def vec_copy(way, step, sub, at):
        view = vec.at[at, pl.ds(way * (pairs // 2), pairs // 2), pl.ds(sub * rows, rows), :]
        return remote(
            view, view, vec_send.at[way, step, sub], vec_recv.at[way, step, sub], onward[way]
        )

    def right_copy(way, step, sub, at):
        view = right.at[at, pl.ds(way * rows, rows), pl.ds(sub * span, span)]
        return remote(
            view, view, right_send.at[way, step, sub], right_recv.at[way, step, sub], onward[way]
        )

    def poll(copy_of, index):
        step, sub = index // 2, lax.rem(index + core, 2)
        for way in range(2):
            at = from_place(way, step)
            copy_of(way, step, sub, at).wait_recv()

            @pl.when(step < last - 1)
            def _():
                copy_of(way, step + 1, sub, at).start()

    def drain(copy_of):
        @pl.loop(0, polls)
        def _(index):
            for way in range(2):
                copy_of(way, index // 2, lax.rem(index, 2), chip).wait_send()

    mine = pl.ds(core * rows, rows)
    vec_own = pltpu.make_async_copy(vec_ref.at[:, :, pl.ds(core * quarter, quarter)], vec.at[chip, :, mine, :], own_sem.at[0])
    left_view = left.at[pl.ds(cut * half_slots, half_slots), mine, :]
    left_other = left.at[pl.ds((1 - cut) * half_slots, half_slots), mine, :]
    left_own = pltpu.make_async_copy(left_ref, left_view, own_sem.at[1])

    def slot_view(slot):
        return right.at[chip, mine, pl.ds(cut * span + slot * quarter, quarter)]

    def slot_part(slot, to_cut, to_core):
        return right_ref.at[slot, :, pl.ds((2 * to_cut + to_core) * quarter, quarter)]

    def vec_part(to_core):
        return vec_ref.at[:, :, pl.ds(to_core * quarter, quarter)]

    right_own = [
        pltpu.make_async_copy(slot_part(slot, cut, core), slot_view(slot), own_sem.at[2 + slot])
        for slot in range(half_slots)
    ]
    vec_own.start()
    left_own.start()
    for copy in right_own:
        copy.start()

    def gram_copy(unit):
        slot = lax.rem(unit, 2)
        return pltpu.make_async_copy(
            basis_ref.at[:, pl.ds(unit * gram_rows, gram_rows), :, :],
            gram_buf.at[slot],
            gram_sem.at[slot],
        )

    barrier = pltpu.get_barrier_semaphore()
    friends = (after, before, partner, across, corner)
    for friend in friends:
        pl.semaphore_signal(barrier, inc=1, device_id=friend, device_id_type=MESH)
    pl.semaphore_wait(barrier, len(friends))

    vec_pre = remote(
        vec_part(1 - core), vec.at[chip, :, mine, :], pre_send.at[0], pre_recv.at[0], partner
    )
    vec_pre.start()
    right_pre = []
    for way, (to_cut, to_core, device) in enumerate((
        (1 - cut, core, across), (1 - cut, 1 - core, corner), (cut, 1 - core, partner)
    )):
        for slot in range(half_slots):
            index = 4 + way * half_slots + slot
            right_pre.append(remote(
                slot_part(slot, to_cut, to_core), slot_view(slot),
                pre_send.at[index], pre_recv.at[index], device,
            ))
    for copy in right_pre:
        copy.start()
    left_across = remote(left_ref, left_view, pre_send.at[1], pre_recv.at[1], across)
    left_across.start()
    left_pair = remote(left_ref, left_view, pre_send.at[2], pre_recv.at[2], partner)
    left_pair.start()
    gram_copy(0).start()
    gram_ref[...] = jnp.zeros_like(gram_ref)

    vec_own.wait()
    for way in range(2):
        vec_copy(way, 0, core, chip).start()
    vec_pre.wait_recv()
    for way in range(2):
        vec_copy(way, 0, 1 - core, chip).start()

    wide = lax.broadcasted_iota(jnp.int32, (mix_ref.shape[0], slots * pairs), 0)
    thin = lax.broadcasted_iota(jnp.int32, (mix_ref.shape[0], slots * pairs), 1)
    stretch = (wide // 8 == thin).astype(jnp.float32)
    tall = jnp.dot(
        stretch, square_ref[...],
        precision=lax.Precision.HIGHEST, preferred_element_type=jnp.float32,
    )
    full = lax.dot_general(
        tall, stretch, (((1,), (1,)), ((), ())),
        precision=lax.Precision.HIGHEST, preferred_element_type=jnp.float32,
    )
    row = lax.broadcasted_iota(jnp.int32, mix_ref.shape, 0)
    lane = lax.broadcasted_iota(jnp.int32, mix_ref.shape, 1)
    mix_ref[...] = jnp.where(lax.rem(row, 8) == lax.rem(lane, 8), full, 0.0)

    def gram_unit(unit):
        slot = lax.rem(unit, 2)
        gram_copy(unit).wait()

        @pl.when(unit + 1 < gram_units)
        def _():
            gram_copy(unit + 1).start()

        chunk = 4

        @pl.loop(0, gram_rows // chunk)
        def _(r):
            for c in range(gram_buf.shape[4] // 128):
                vecs = [
                    gram_buf[slot, j, pl.ds(r * chunk, chunk), :, c * 128 : (c + 1) * 128]
                    for j in range(basis_count)
                ]
                i = 0
                for j in range(basis_count):
                    for k in range(j, basis_count):
                        gram_ref[i] += jnp.sum(vecs[j] * vecs[k], axis=0)
                        i += 1

    @pl.loop(0, polls - 2)
    def _(index):
        poll(vec_copy, index)

        @pl.when(index < gram_units)
        def _():
            gram_unit(index)

    for copy in right_own:
        copy.wait()
    for copy in right_pre:
        copy.wait_recv()
    for sub in range(2):
        for way in range(2):
            right_copy(way, 0, lax.rem(sub + core, 2), chip).start()

    left_across.wait_recv()
    left_pass = remote(left_other, left_other, pre_send.at[3], pre_recv.at[3], partner)
    left_pass.start()

    @pl.loop(polls - 2, polls)
    def _(index):
        poll(vec_copy, index)

    left_own.wait()
    left_pair.wait_recv()
    left_pass.wait_recv()

    def mix_unit(unit):
        row0 = pl.multiple_of((unit // col_tiles) * row_tile, row_tile)
        col0 = pl.multiple_of(lax.rem(unit, col_tiles) * col_tile, col_tile)

        @pl.loop(0, pairs)
        def _(q):
            proj[q] = jnp.dot(
                left[:, pl.ds(row0, row_tile), :].reshape(slots * row_tile, depth),
                vec[:, q, :, pl.ds(col0, col_tile)].reshape(depth, col_tile),
                preferred_element_type=jnp.float32,
            ).reshape(slots, row_tile, col_tile)

        owner = row0 // rows
        base = owner * (pairs * rows) + row0 - owner * rows

        @pl.loop(0, row_tile // 16)
        def _(g):
            lines = []
            for h in range(2):
                at = pl.ds(pl.multiple_of(g * 16 + h * 8, 8), 8)
                stacked = jnp.concatenate(
                    [proj[q, k, at, :] for k in range(slots) for q in range(pairs)], axis=0
                )
                lines.append(
                    jnp.dot(
                        mix_ref[...],
                        stacked,
                        precision=lax.Precision.HIGHEST,
                        preferred_element_type=jnp.float32,
                    )
                )
            for y in range(slots):
                cols = pl.ds(pl.multiple_of(y * quarter + col0, col_tile), col_tile)
                for p in range(pairs):
                    i = (y * pairs + p) * 8
                    at = pl.ds(pl.multiple_of(base + p * rows + g * 16, 16), 16)
                    mixed[at, cols] = jnp.concatenate(
                        [m[i : i + 8] for m in lines], axis=0
                    ).astype(mixed.dtype)

    lot = pairs * rows

    def pair_copy(unit):
        return remote(
            parts.at[chips + lax.rem(unit, 2)], pair_in.at[unit],
            pair_send.at[unit], pair_recv.at[unit], partner,
        )

    def block_of(unit, way):
        return chip_at(place - unit) if way == 0 else chip_at(place + unit)

    def home_of(unit, way):
        at = block_of(unit, way)
        return at // half, lax.rem(at, half) * 2 + way

    def cut_copy(unit, way):
        _, piece = home_of(unit, way)
        return remote(
            parts.at[unit, way], cut_in.at[piece],
            cut_send.at[unit, way], cut_recv.at[piece], across,
        )

    def image_half(unit, sub):
        @pl.when((unit >= 2) & (sub == 0))
        def _():
            pair_copy(unit - 2).wait_send()

        at = lax.rem(sub + core, 2)
        cols = pl.ds(pl.multiple_of(at * span, span), span)

        @pl.loop(0, 2)
        def _(k):
            owner = lax.rem(core + 1 + k, 2)
            to = (1 - k) * (chips + lax.rem(unit, 2)) + k * unit
            lines = jnp.concatenate(
                [
                    right[block_of(unit, way), way * rows : (way + 1) * rows, cols]
                    for way in range(2)
                ],
                axis=0,
            )
            out = lax.dot_general(
                mixed[pl.ds(pl.multiple_of(owner * lot, lot), lot), cols],
                lines,
                (((1,), (1,)), ((), ())),
                preferred_element_type=jnp.float32,
            )

            @pl.when(sub == 0)
            def _():
                for way in range(2):
                    piece = out[:, way * rows : (way + 1) * rows]
                    parts[to, way] = piece.reshape(pairs, rows, rows)

            @pl.when(sub == 1)
            def _():
                for way in range(2):
                    piece = out[:, way * rows : (way + 1) * rows]
                    parts[to, way] += piece.reshape(pairs, rows, rows)

        @pl.when(sub == 1)
        def _():
            pair_copy(unit).start()

    def join_unit(unit):
        pair_copy(unit).wait_recv()
        for way in range(2):
            parts[unit, way] += pair_in[unit, way]
            home, _ = home_of(unit, way)

            @pl.when(home != cut)
            def _():
                cut_copy(unit, way).start()

    @pl.loop(0, mix_units)
    def _(index):
        poll(right_copy, index)
        mix_unit(index)

    def ready(index):
        return jnp.minimum(4 * (index - mix_units + 1), index + 3)

    @pl.loop(mix_units, polls)
    def _(index):
        poll(right_copy, index)

        @pl.loop(ready(index - 1), ready(index))
        def _(piece):
            unit, sub = piece // 2, lax.rem(piece, 2)
            image_half(unit, sub)

            @pl.when((unit > 0) & (sub == 1))
            def _():
                join_unit(unit - 1)

    join_unit(last)

    @pl.loop(0, chips)
    def _(unit):
        for way in range(2):
            home, piece = home_of(unit, way)
            copy = cut_copy(unit, way)

            @pl.when(home == cut)
            def _():
                copy.wait_recv()
                cols = pl.ds(pl.multiple_of(piece * rows, rows), rows)
                whole = parts[unit, way] + cut_in[piece]
                for p in range(pairs):
                    image_ref[:, p, cols] = whole[p]

            @pl.when(home != cut)
            def _():
                copy.wait_send()

    drain(vec_copy)
    drain(right_copy)
    for unit in (chips - 2, chips - 1):
        pair_copy(unit).wait_send()
    vec_pre.wait_send()
    left_across.wait_send()
    for copy in right_pre:
        copy.wait_send()
    left_pair.wait_send()
    left_pass.wait_send()


def ring_image(table, left_env, right_env, current, basis):
    rows, half_slots, depth = left_env.shape
    pairs, cols = current.shape[1], current.shape[2]
    slots, chips, quarter = 2 * half_slots, depth // (2 * rows), cols // 2
    basis_count = basis.shape[0]
    count = basis_count * (basis_count + 1) // 2
    square = table.transpose(1, 2, 0, 3).reshape(slots * pairs, slots * pairs)
    vec = current.transpose(1, 0, 2)
    left = left_env.transpose(1, 0, 2)
    right = right_env.transpose(1, 0, 2)
    bf16, f32 = jnp.bfloat16, jnp.float32
    sem = pltpu.SemaphoreType.DMA
    steps = chips - 1
    hbm = pl.BlockSpec(memory_space=pltpu.HBM)
    vmem = pl.BlockSpec(memory_space=pltpu.VMEM)
    return pl.pallas_call(
        ring_kernel,
        name="ring",
        in_specs=[hbm, hbm, hbm, vmem, hbm],
        out_specs=[vmem, vmem],
        out_shape=[
            jax.ShapeDtypeStruct((rows, pairs, cols), f32),
            jax.ShapeDtypeStruct((count, pairs, 128), f32),
        ],
        scratch_shapes=[
            pltpu.VMEM((chips, pairs, 2 * rows, quarter), bf16),
            pltpu.VMEM((slots, 2 * rows, depth), bf16),
            pltpu.VMEM((chips, 2 * rows, slots * quarter), bf16),
            pltpu.VMEM((2 * pairs * rows, slots * quarter), bf16),
            pltpu.VMEM((slots * pairs * 8, slots * pairs * 8), f32),
            pltpu.VMEM((pairs, slots, rows // 2, quarter // 2), f32),
            pltpu.VMEM((chips + 2, 2, pairs, rows, rows), f32),
            pltpu.VMEM((chips, 2, pairs, rows, rows), f32),
            pltpu.VMEM((chips, pairs, rows, rows), f32),
            pltpu.VMEM((2, basis_count, rows // 8, pairs, cols), f32),
            sem((2 + half_slots,)),
            sem((4 + 3 * half_slots,)),
            sem((4 + 3 * half_slots,)),
            sem((2, steps, 2)),
            sem((2, steps, 2)),
            sem((2, steps, 2)),
            sem((2, steps, 2)),
            sem((chips,)),
            sem((chips,)),
            sem((chips, 2)),
            sem((chips,)),
            sem((2,)),
        ],
        compiler_params=pltpu.CompilerParams(
            vmem_limit_bytes=63 * 1024 * 1024, collective_id=1, has_side_effects=True
        ),
    )(vec, left, right, square, basis)


def finish_kernel(
    blocks, cuts, entries,
    beta_ref, gram_ref, image_ref, basis_ref,
    next_ref, values_ref,
    basis, tile, inbox, load_sem, send_sem, recv_sem,
):
    basis_count, rows, pairs, cols = basis.shape
    chunks = load_sem.shape[0]
    chunk = rows // chunks
    lanes = cols // 128
    devices = blocks * cuts
    me = lax.axis_index("blk") * cuts + lax.axis_index("cuts")

    def load(unit):
        at = pl.ds(unit * chunk, chunk)
        return pltpu.make_async_copy(
            basis_ref.at[:, at, :, :], basis.at[:, at, :, :], load_sem.at[unit]
        )

    for unit in range(chunks):
        load(unit).start()

    def place(offset):
        device = lax.rem(me + offset, devices)
        return (device // cuts, lax.rem(device, cuts))

    barrier = pltpu.get_barrier_semaphore()
    for offset in range(1, devices):
        pl.semaphore_signal(barrier, inc=1, device_id=place(offset), device_id_type=MESH)

    row = lax.broadcasted_iota(jnp.int32, tile.shape, 0)
    lane = lax.broadcasted_iota(jnp.int32, tile.shape, 1)

    def total_of(x):
        return jnp.sum(jnp.sum(x, axis=0, keepdims=True), axis=1, keepdims=True)

    found = jnp.zeros(tile.shape, jnp.float32)
    i = 0
    for j in range(basis_count):
        for k in range(j, basis_count):
            here = ((row == j) & (lane == k)) | ((row == k) & (lane == j))
            found = jnp.where(here, total_of(gram_ref[i]), found)
            i += 1
    tile[...] = found

    def dots(unit, sums):
        load(unit).wait()
        for c in range(lanes):
            at = slice(c * 128, (c + 1) * 128)
            for step in range(chunk // 8):
                r = pl.ds(unit * chunk + step * 8, 8)
                image = image_ref[r, :, at]
                sums = tuple(
                    sums[j] + jnp.sum(basis[j, r, :, at] * image, axis=0)
                    for j in range(basis_count)
                ) + (sums[basis_count] + jnp.sum(image * image, axis=0),)
        return sums

    zero = jnp.zeros((pairs, 128), jnp.float32)
    sums = lax.fori_loop(0, chunks, dots, (zero,) * (basis_count + 1))
    found = tile[...]
    for j in range(basis_count + 1):
        here = ((row == j) & (lane == basis_count)) | ((row == basis_count) & (lane == j))
        found = jnp.where(here, total_of(sums[j]), found)
    tile[...] = found
    inbox[me] = found

    pl.semaphore_wait(barrier, devices - 1)

    def send(offset):
        return pltpu.make_async_remote_copy(
            src_ref=tile, dst_ref=inbox.at[me],
            send_sem=send_sem.at[offset], recv_sem=recv_sem.at[offset],
            device_id=place(offset), device_id_type=MESH,
        )

    for offset in range(1, devices):
        send(offset).start()
    for offset in range(1, devices):
        send(offset).wait_recv()

    sums = inbox[0]
    for d in range(1, devices):
        sums = sums + inbox[d]
    sums = sums / entries
    n, last, prior = basis_count, basis_count - 1, basis_count - 2
    gram = sums[0:n, 0:n]
    down, along = sums[0:n, n : n + 1], sums[n : n + 1, 0:n]
    square = sums[n : n + 1, n : n + 1]
    alpha = down[last : last + 1]
    beta = jnp.full((1, 1), beta_ref[0], jnp.float32)
    ortho = down - alpha * gram[:, last : last + 1] - beta * gram[:, prior : prior + 1]
    ortho_row = along - alpha * gram[last : last + 1, :] - beta * gram[prior : prior + 1, :]
    first = (
        square
        - 2.0 * alpha * alpha
        - 2.0 * beta * down[prior : prior + 1]
        + alpha * alpha * gram[last : last + 1, last : last + 1]
        + 2.0 * alpha * beta * gram[last : last + 1, prior : prior + 1]
        + beta * beta * gram[prior : prior + 1, prior : prior + 1]
    )
    bent = jnp.sum(ortho * gram, axis=0, keepdims=True) * ortho_row
    mean = (
        first
        - 2.0 * jnp.sum(ortho * ortho, axis=0, keepdims=True)
        + jnp.sum(bent, axis=1, keepdims=True)
    )
    beta_new = jnp.sqrt(mean + 1e-06)
    values_ref[...] = jnp.where(
        (row == 0) & (lane == 0), alpha, jnp.where((row == 0) & (lane == 1), beta_new, 0.0)
    )
    index = lax.broadcasted_iota(jnp.int32, ortho.shape, 0)
    coefs = (
        ortho + jnp.where(index == last, alpha, 0.0) + jnp.where(index == prior, beta, 0.0)
    )
    spread = [jnp.broadcast_to(coefs[j : j + 1], (pairs, 128)) for j in range(n)]
    scale = jnp.broadcast_to(1.0 / beta_new, (pairs, 128))

    @pl.loop(0, rows // 8)
    def _(step):
        r = pl.ds(step * 8, 8)
        for c in range(lanes):
            at = slice(c * 128, (c + 1) * 128)
            value = image_ref[r, :, at]
            for j in range(n):
                value = value - spread[j][None] * basis[j, r, :, at]
            next_ref[r, :, at] = value * scale[None]

    for offset in range(1, devices):
        send(offset).wait_send()


def finish(blocks, cuts, entries, beta_prev, gram, image, basis):
    basis_count, rows, pairs, cols = basis.shape
    tile = (16, 128)
    devices = blocks * cuts
    sem = pltpu.SemaphoreType.DMA
    vmem = pl.BlockSpec(memory_space=pltpu.VMEM)
    next_vector, values = pl.pallas_call(
        functools.partial(finish_kernel, blocks, cuts, entries),
        name="finish",
        in_specs=[
            pl.BlockSpec(memory_space=pltpu.SMEM),
            vmem,
            vmem,
            pl.BlockSpec(memory_space=pltpu.HBM),
        ],
        out_specs=[vmem, vmem],
        out_shape=[
            jax.ShapeDtypeStruct((rows, pairs, cols), jnp.float32),
            jax.ShapeDtypeStruct(tile, jnp.float32),
        ],
        scratch_shapes=[
            pltpu.VMEM(basis.shape, jnp.float32),
            pltpu.VMEM(tile, jnp.float32),
            pltpu.VMEM((devices,) + tile, jnp.float32),
            sem((rows // 16,)),
            sem((devices,)),
            sem((devices,)),
        ],
        compiler_params=pltpu.CompilerParams(
            vmem_limit_bytes=40 * 1024 * 1024, collective_id=2, has_side_effects=True
        ),
    )(beta_prev.reshape(1), gram, image, basis)
    return next_vector, values[0, 0:1], values[0, 1:2]


def ring_fits(blocks, rows, depth):
    return blocks == 16 and rows * blocks == depth and rows % 128 == 0


def gathered_image(cuts, table, left_env, right_env, current):
    row_count, pair_count, col_count = current.shape
    bond_width = table.shape[0]
    full_width = left_env.shape[2]
    me = lax.axis_index("cuts")
    swap = [(0, 1), (1, 0)]

    current = current.transpose(1, 0, 2)
    left_t = left_env.transpose(1, 0, 2)
    right_t = right_env.transpose(1, 0, 2)
    if cuts == 2:
        half = left_t.shape[0]
        theirs = lax.dynamic_slice_in_dim(right_t, (1 - me) * col_count, col_count, 2)
        mine = lax.dynamic_slice_in_dim(right_t, me * col_count, col_count, 2)
        right_k = jnp.concatenate([mine, lax.ppermute(theirs, "cuts", swap)], axis=0)
        left_k = jnp.concatenate([left_t, lax.ppermute(left_t, "cuts", swap)], axis=0)
        turned = jnp.roll(jnp.roll(table, -half, axis=0), -half, axis=1)
        table = jnp.where(me == 0, table, turned)
    else:
        left_k = lax.all_gather(left_t, "cuts", axis=0, tiled=True)
        right_k = lax.all_to_all(right_t, "cuts", split_axis=2, concat_axis=0, tiled=True)
    cur_full = lax.all_gather(current, "blk", axis=1, tiled=True)
    right_full = lax.all_gather(right_k, "blk", axis=1, tiled=True)

    mixed = mixed_left_of(table, left_k, cur_full)
    mixed = mixed.reshape(bond_width, pair_count * row_count, col_count)
    if cuts == 2:
        away = image_part(mixed, right_full, (1 - me) * col_count, col_count)
        away = lax.ppermute(away, "cuts", swap)
        here = image_part(mixed, right_full, me * col_count, col_count)
        image = here + away
    else:
        image = image_part(mixed, right_full, jnp.int32(0), full_width)
        image = lax.psum_scatter(image, "cuts", scatter_dimension=1, tiled=True)
    return image.reshape(pair_count, row_count, col_count).transpose(1, 0, 2)


def on_device(
    blocks, cuts, left_env, right_env, left_core, right_core, slot_bond, krylov_basis, beta_prev
):
    pair_count = left_core.shape[2] * left_core.shape[2]
    basis_count, row_count, _, _ = krylov_basis.shape
    full_width = left_env.shape[2]
    entries = float(full_width * pair_count * full_width)
    table = build_table(left_core, right_core, slot_bond)
    current = krylov_basis[basis_count - 1].astype(jnp.bfloat16)
    if cuts == 2 and ring_fits(blocks, row_count, full_width):
        image, gram = ring_image(table, left_env, right_env, current, krylov_basis)
        return finish(blocks, cuts, entries, beta_prev, gram, image, krylov_basis)
    image = gathered_image(cuts, table, left_env, right_env, current)
    gram = gram_of(krylov_basis)

    sums = lax.psum(jnp.concatenate([gram, dots_of(krylov_basis, image)]), ("blk", "cuts"))
    sums = sums / entries
    count = basis_count * (basis_count + 1) // 2
    where = []
    for j in range(basis_count):
        for k in range(basis_count):
            low, high = min(j, k), max(j, k)
            where.append(low * basis_count - low * (low - 1) // 2 + high - low)
    gram_matrix = sums[jnp.array(where)].reshape(basis_count, basis_count)
    inner_prods = sums[count : count + basis_count]
    image_square = sums[count + basis_count]
    last, prior = basis_count - 1, basis_count - 2
    alpha_now = inner_prods[last]
    ortho_coeffs = (
        inner_prods - alpha_now * gram_matrix[:, last] - beta_prev * gram_matrix[:, prior]
    )
    first_square = (
        image_square
        - 2.0 * alpha_now * inner_prods[last]
        - 2.0 * beta_prev * inner_prods[prior]
        + alpha_now * alpha_now * gram_matrix[last, last]
        + 2.0 * alpha_now * beta_prev * gram_matrix[last, prior]
        + beta_prev * beta_prev * gram_matrix[prior, prior]
    )
    square_mean = (
        first_square
        - 2.0 * jnp.sum(ortho_coeffs * ortho_coeffs)
        + jnp.sum(ortho_coeffs[:, None] * gram_matrix * ortho_coeffs[None, :])
    )
    beta_new = jnp.sqrt(square_mean + 1e-06)
    index = jnp.arange(basis_count)
    coefs = (
        ortho_coeffs
        + jnp.where(index == last, alpha_now, 0.0)
        + jnp.where(index == prior, beta_prev, 0.0)
    )
    coefs = jnp.concatenate([coefs, (1.0 / beta_new)[None]])
    next_vector = final_of(coefs, krylov_basis, image)
    return (next_vector, alpha_now[None], beta_new[None])


def solution(mesh):
    in_specs = (
        P("blk", "cuts", None),
        P("blk", "cuts", None),
        P(),
        P(),
        P(),
        P(None, "blk", None, "cuts"),
        P(),
    )
    out_specs = (P("blk", None, "cuts"), P(), P())
    return jax.shard_map(
        functools.partial(on_device, mesh.shape["blk"], mesh.shape["cuts"]),
        mesh=mesh,
        in_specs=in_specs,
        out_specs=out_specs,
        check_vma=False,
    )
```

```python
import functools

import jax
import jax.numpy as jnp
from jax import lax
from jax.experimental import pallas as pl
from jax.experimental.pallas import tpu as pltpu
from jax.sharding import PartitionSpec as P

VMEM_BYTES = 60 * 1024 * 1024


def params():
    return pltpu.CompilerParams(vmem_limit_bytes=VMEM_BYTES)


def tile_of(size, most):
    return most if size % most == 0 else size


def build_table(left_core, right_core, slot_bond):
    bond_width = left_core.shape[0]
    phys_dim = left_core.shape[2]
    chosen = (slot_bond[:, None] == jnp.arange(bond_width, dtype=jnp.int32)[None, :]).astype(
        jnp.float32
    )
    picked = jnp.einsum("kw,wxac->kxac", chosen, left_core, precision=lax.Precision.HIGHEST)
    table = jnp.einsum("kxac,xybd->kyabcd", picked, right_core, precision=lax.Precision.HIGHEST)
    return table.reshape(bond_width, bond_width, phys_dim * phys_dim, phys_dim * phys_dim)


def mix_kernel(mix_ref, left_ref, cur_ref, out_ref, proj):
    slots, rows, depth = left_ref.shape
    pairs = cur_ref.shape[0]
    bonds = out_ref.shape[0]
    cols = cur_ref.shape[2]

    @pl.loop(0, pairs)
    def _(q):
        proj[q] = jnp.dot(
            left_ref[...].reshape(slots * rows, depth),
            cur_ref[q],
            preferred_element_type=jnp.float32,
        ).reshape(slots, rows, cols)

    @pl.loop(0, rows // 16)
    def _(g):
        mixed = []
        for h in range(2):
            at = pl.ds(pl.multiple_of(g * 16 + h * 8, 8), 8)
            stacked = jnp.concatenate(
                [proj[q, k, at, :] for k in range(slots) for q in range(pairs)], axis=0
            )
            mixed.append(
                jnp.dot(
                    mix_ref[...],
                    stacked,
                    precision=lax.Precision.HIGHEST,
                    preferred_element_type=jnp.float32,
                )
            )
        at = pl.ds(pl.multiple_of(g * 16, 16), 16)
        for y in range(bonds):
            for p in range(pairs):
                i = (y * pairs + p) * 8
                out_ref[y, p, at, :] = jnp.concatenate(
                    [m[i : i + 8] for m in mixed], axis=0
                ).astype(out_ref.dtype)


def mixed_left_of(table, left_k, cur_full):
    slots, rows, depth = left_k.shape
    pairs, _, cols = cur_full.shape
    bonds = table.shape[1]
    tb = tile_of(cols, 256)
    square = table.transpose(1, 2, 0, 3).reshape(bonds * pairs, slots * pairs)
    mix = jnp.kron(square, jnp.eye(8, dtype=jnp.float32))
    return pl.pallas_call(
        mix_kernel,
        grid=(cols // tb,),
        in_specs=[
            pl.BlockSpec(mix.shape, lambda i: (0, 0)),
            pl.BlockSpec((slots, rows, depth), lambda i: (0, 0, 0)),
            pl.BlockSpec((pairs, depth, tb), lambda i: (0, 0, i)),
        ],
        out_specs=pl.BlockSpec((bonds, pairs, rows, tb), lambda i: (0, 0, 0, i)),
        out_shape=jax.ShapeDtypeStruct((bonds, pairs, rows, cols), jnp.bfloat16),
        scratch_shapes=[pltpu.VMEM((pairs, slots, rows, tb), jnp.float32)],
        compiler_params=params(),
        cost_estimate=pl.CostEstimate(
            flops=2 * slots * rows * depth * pairs * cols,
            bytes_accessed=2 * (left_k.size + cur_full.size + bonds * pairs * rows * cols),
            transcendentals=0,
        ),
    )(mix, left_k, cur_full)


def image_kernel(start_ref, mixed_ref, right_ref, out_ref):
    bonds = mixed_ref.shape[0]
    out_ref[...] = jnp.zeros_like(out_ref)

    @pl.loop(0, bonds)
    def _(y):
        out_ref[...] += lax.dot_general(
            mixed_ref[y],
            right_ref[y],
            (((1,), (1,)), ((), ())),
            preferred_element_type=jnp.float32,
        )


def image_part(mixed, right_full, start, count):
    bonds, lines, cols = mixed.shape
    tb = tile_of(count, 256)
    return pl.pallas_call(
        image_kernel,
        grid_spec=pltpu.PrefetchScalarGridSpec(
            num_scalar_prefetch=1,
            grid=(count // tb,),
            in_specs=[
                pl.BlockSpec((bonds, lines, cols), lambda i, s: (0, 0, 0)),
                pl.BlockSpec((bonds, tb, cols), lambda i, s: (0, s[0] + i, 0)),
            ],
            out_specs=pl.BlockSpec((lines, tb), lambda i, s: (0, i)),
        ),
        out_shape=jax.ShapeDtypeStruct((lines, count), jnp.float32),
        compiler_params=params(),
        cost_estimate=pl.CostEstimate(
            flops=2 * bonds * lines * cols * count,
            bytes_accessed=2 * (mixed.size + bonds * count * cols),
            transcendentals=0,
        ),
    )((start // tb).reshape(1).astype(jnp.int32), mixed, right_full)


def gram_kernel(basis_ref, out_ref):
    basis_count, rows, pairs, cols = basis_ref.shape
    chunk = 4
    lanes = cols // 128

    @pl.when(pl.program_id(0) == 0)
    def _():
        out_ref[...] = jnp.zeros_like(out_ref)

    @pl.loop(0, rows // chunk)
    def _(r):
        for c in range(lanes):
            vecs = [
                basis_ref[j, pl.ds(r * chunk, chunk), :, c * 128 : (c + 1) * 128]
                for j in range(basis_count)
            ]
            i = 0
            for j in range(basis_count):
                for k in range(j, basis_count):
                    out_ref[i] += jnp.sum(vecs[j] * vecs[k], axis=0)
                    i += 1


def gram_of(basis):
    basis_count, rows, pairs, cols = basis.shape
    count = basis_count * (basis_count + 1) // 2
    ta = tile_of(rows, 16)
    sums = pl.pallas_call(
        gram_kernel,
        grid=(rows // ta,),
        in_specs=[pl.BlockSpec((basis_count, ta, pairs, cols), lambda i: (0, i, 0, 0))],
        out_specs=pl.BlockSpec((count, pairs, 128), lambda i: (0, 0, 0)),
        out_shape=jax.ShapeDtypeStruct((count, pairs, 128), jnp.float32),
        compiler_params=params(),
        cost_estimate=pl.CostEstimate(
            flops=2 * count * rows * pairs * cols,
            bytes_accessed=4 * basis.size,
            transcendentals=0,
        ),
    )(basis)
    return jnp.sum(sums, axis=(1, 2))


def dots_kernel(basis_ref, image_ref, out_ref):
    basis_count, rows, pairs, cols = basis_ref.shape

    @pl.when(pl.program_id(0) == 0)
    def _():
        out_ref[...] = jnp.zeros_like(out_ref)

    for c in range(cols // 128):
        at = slice(c * 128, (c + 1) * 128)
        image = image_ref[:, :, at]
        for j in range(basis_count):
            out_ref[j] += jnp.sum(basis_ref[j, :, :, at] * image, axis=0)
        out_ref[basis_count] += jnp.sum(image * image, axis=0)


def dots_of(basis, image):
    basis_count, rows, pairs, cols = basis.shape
    ta = tile_of(rows, 16)
    sums = pl.pallas_call(
        dots_kernel,
        grid=(rows // ta,),
        in_specs=[
            pl.BlockSpec((basis_count, ta, pairs, cols), lambda i: (0, i, 0, 0)),
            pl.BlockSpec((ta, pairs, cols), lambda i: (i, 0, 0)),
        ],
        out_specs=pl.BlockSpec((basis_count + 1, pairs, 128), lambda i: (0, 0, 0)),
        out_shape=jax.ShapeDtypeStruct((basis_count + 1, pairs, 128), jnp.float32),
        compiler_params=params(),
    )(basis, image)
    return jnp.sum(sums, axis=(1, 2))


def final_kernel(coef_ref, basis_ref, image_ref, out_ref):
    basis_count = basis_ref.shape[0]
    total = image_ref[...]
    for j in range(basis_count):
        total = total - coef_ref[j] * basis_ref[j]
    out_ref[...] = total * coef_ref[basis_count]


def final_of(coefs, basis, image):
    basis_count, rows, pairs, cols = basis.shape
    ta = tile_of(rows, 16)
    return pl.pallas_call(
        final_kernel,
        grid=(rows // ta,),
        in_specs=[
            pl.BlockSpec(memory_space=pltpu.SMEM),
            pl.BlockSpec((basis_count, ta, pairs, cols), lambda i: (0, i, 0, 0)),
            pl.BlockSpec((ta, pairs, cols), lambda i: (i, 0, 0)),
        ],
        out_specs=pl.BlockSpec((ta, pairs, cols), lambda i: (i, 0, 0)),
        out_shape=jax.ShapeDtypeStruct((rows, pairs, cols), jnp.float32),
        compiler_params=params(),
    )(coefs, basis, image)


MESH = pl.DeviceIdType.MESH


def ring_kernel(
    blocks, cuts, entries,
    beta_ref, vec_ref, left_ref, right_ref, square_ref, basis_ref,
    next_ref, values_ref,
    vec, left, right, mixed, mix_ref, proj, parts, pair_in, cut_in, stream,
    gram_ref, dots_ref, gram_tile, gram_inbox, dots_tile, dots_inbox,
    gram_send, gram_recv, dots_send, dots_recv,
    own_sem, pre_send, pre_recv, vec_send, vec_recv, right_send, right_recv,
    pair_send, pair_recv, cut_send, cut_recv, stream_sem,
):
    chips, pairs, chip_rows, quarter = vec.shape
    slots, _, depth = left.shape
    half_slots, rows, _ = left_ref.shape
    span = half_slots * quarter
    last = chips - 1
    polls = 2 * last
    row_tile, col_tile = proj.shape[2], proj.shape[3]
    col_tiles = quarter // col_tile
    mix_units = (chip_rows // row_tile) * col_tiles
    basis_count = basis_ref.shape[0]
    lanes = stream.shape[4]
    pieces = basis_ref.shape[3] // lanes
    half = chips // 2

    blk = lax.axis_index("blk")
    cut = lax.axis_index("cuts")
    core = lax.rem(blk, 2)
    chip = blk // 2
    side = lax.rem(chip, 2)
    place = (1 - side) * (chip // 2) + side * (last - chip // 2)

    def chip_at(index):
        index = lax.rem(index + 2 * chips, chips)
        far = index // half
        return (1 - far) * 2 * index + far * (2 * (last - index) + 1)

    after = (2 * chip_at(place + 1) + core, cut)
    before = (2 * chip_at(place - 1) + core, cut)
    onward = (after, before)
    partner = (2 * chip + 1 - core, cut)
    across = (blk, 1 - cut)
    corner = (2 * chip + 1 - core, 1 - cut)

    def remote(src, dst, send, recv, device):
        return pltpu.make_async_remote_copy(
            src_ref=src, dst_ref=dst, send_sem=send, recv_sem=recv,
            device_id=device, device_id_type=MESH,
        )

    def from_place(way, step):
        return chip_at(place - 1 - step) if way == 0 else chip_at(place + 1 + step)

    def vec_copy(way, step, sub, at):
        view = vec.at[at, pl.ds(way * (pairs // 2), pairs // 2), pl.ds(sub * rows, rows), :]
        return remote(
            view, view, vec_send.at[way, step, sub], vec_recv.at[way, step, sub], onward[way]
        )

    def right_copy(way, step, sub, at):
        view = right.at[at, pl.ds(way * rows, rows), pl.ds(sub * span, span)]
        return remote(
            view, view, right_send.at[way, step, sub], right_recv.at[way, step, sub], onward[way]
        )

    def poll(copy_of, index):
        step, sub = index // 2, lax.rem(index + core, 2)
        for way in range(2):
            at = from_place(way, step)
            copy_of(way, step, sub, at).wait_recv()

            @pl.when(step < last - 1)
            def _():
                copy_of(way, step + 1, sub, at).start()

    def drain(copy_of):
        @pl.loop(0, polls)
        def _(index):
            for way in range(2):
                copy_of(way, index // 2, lax.rem(index, 2), chip).wait_send()

    mine = pl.ds(core * rows, rows)
    vec_own = pltpu.make_async_copy(vec_ref.at[:, :, pl.ds(core * quarter, quarter)], vec.at[chip, :, mine, :], own_sem.at[0])
    left_view = left.at[pl.ds(cut * half_slots, half_slots), mine, :]
    left_other = left.at[pl.ds((1 - cut) * half_slots, half_slots), mine, :]
    left_own = pltpu.make_async_copy(left_ref, left_view, own_sem.at[1])

    def slot_view(slot):
        return right.at[chip, mine, pl.ds(cut * span + slot * quarter, quarter)]

    def slot_part(slot, to_cut, to_core):
        return right_ref.at[slot, :, pl.ds((2 * to_cut + to_core) * quarter, quarter)]

    def vec_part(to_core):
        return vec_ref.at[:, :, pl.ds(to_core * quarter, quarter)]

    right_own = [
        pltpu.make_async_copy(slot_part(slot, cut, core), slot_view(slot), own_sem.at[2 + slot])
        for slot in range(half_slots)
    ]
    vec_own.start()
    left_own.start()
    for copy in right_own:
        copy.start()

    def stream_copy(piece, slot):
        return pltpu.make_async_copy(
            basis_ref.at[:, :, :, pl.ds(pl.multiple_of(piece * lanes, lanes), lanes)],
            stream.at[slot],
            stream_sem.at[slot],
        )

    devices = blocks * cuts
    me = blk * cuts + cut

    def place_of(offset):
        device = lax.rem(me + offset, devices)
        return (device // cuts, lax.rem(device, cuts))

    barrier = pltpu.get_barrier_semaphore()
    for offset in range(1, devices):
        pl.semaphore_signal(barrier, inc=1, device_id=place_of(offset), device_id_type=MESH)
    pl.semaphore_wait(barrier, devices - 1)

    vec_pre = remote(
        vec_part(1 - core), vec.at[chip, :, mine, :], pre_send.at[0], pre_recv.at[0], partner
    )
    vec_pre.start()
    right_pre = []
    for way, (to_cut, to_core, device) in enumerate((
        (1 - cut, core, across), (1 - cut, 1 - core, corner), (cut, 1 - core, partner)
    )):
        for slot in range(half_slots):
            index = 4 + way * half_slots + slot
            right_pre.append(remote(
                slot_part(slot, to_cut, to_core), slot_view(slot),
                pre_send.at[index], pre_recv.at[index], device,
            ))
    for copy in right_pre:
        copy.start()
    left_across = remote(left_ref, left_view, pre_send.at[1], pre_recv.at[1], across)
    left_across.start()
    left_pair = remote(left_ref, left_view, pre_send.at[2], pre_recv.at[2], partner)
    left_pair.start()
    stream_copy(0, 0).start()
    gram_ref[...] = jnp.zeros_like(gram_ref)
    dots_ref[...] = jnp.zeros_like(dots_ref)

    vec_own.wait()
    for way in range(2):
        vec_copy(way, 0, core, chip).start()
    vec_pre.wait_recv()
    for way in range(2):
        vec_copy(way, 0, 1 - core, chip).start()

    wide = lax.broadcasted_iota(jnp.int32, (mix_ref.shape[0], slots * pairs), 0)
    thin = lax.broadcasted_iota(jnp.int32, (mix_ref.shape[0], slots * pairs), 1)
    stretch = (wide // 8 == thin).astype(jnp.float32)
    tall = jnp.dot(
        stretch, square_ref[...],
        precision=lax.Precision.HIGHEST, preferred_element_type=jnp.float32,
    )
    full = lax.dot_general(
        tall, stretch, (((1,), (1,)), ((), ())),
        precision=lax.Precision.HIGHEST, preferred_element_type=jnp.float32,
    )
    row = lax.broadcasted_iota(jnp.int32, mix_ref.shape, 0)
    lane = lax.broadcasted_iota(jnp.int32, mix_ref.shape, 1)
    mix_ref[...] = jnp.where(lax.rem(row, 8) == lax.rem(lane, 8), full, 0.0)

    def gram_unit(unit):
        slot = lax.rem(unit, 2)
        stream_copy(unit, slot).wait()

        @pl.when(unit + 1 < pieces)
        def _():
            stream_copy(unit + 1, 1 - slot).start()

        chunk = 4

        @pl.loop(0, rows // chunk)
        def _(r):
            vecs = [stream[slot, j, pl.ds(r * chunk, chunk), :, :] for j in range(basis_count)]
            i = 0
            for j in range(basis_count):
                for k in range(j, basis_count):
                    gram_ref[i] += jnp.sum(vecs[j] * vecs[k], axis=0)
                    i += 1

    @pl.loop(0, polls - 2)
    def _(index):
        poll(vec_copy, index)

        @pl.when(index < pieces)
        def _():
            gram_unit(index)

    for copy in right_own:
        copy.wait()
    for copy in right_pre:
        copy.wait_recv()
    for sub in range(2):
        for way in range(2):
            right_copy(way, 0, lax.rem(sub + core, 2), chip).start()

    left_across.wait_recv()
    left_pass = remote(left_other, left_other, pre_send.at[3], pre_recv.at[3], partner)
    left_pass.start()

    def total_of(x):
        return jnp.sum(jnp.sum(x, axis=0, keepdims=True), axis=1, keepdims=True)

    row = lax.broadcasted_iota(jnp.int32, gram_tile.shape, 0)
    lane = lax.broadcasted_iota(jnp.int32, gram_tile.shape, 1)
    found = jnp.zeros(gram_tile.shape, jnp.float32)
    i = 0
    for j in range(basis_count):
        for k in range(j, basis_count):
            here = ((row == j) & (lane == k)) | ((row == k) & (lane == j))
            found = jnp.where(here, total_of(gram_ref[i]), found)
            i += 1
    gram_tile[...] = found
    gram_inbox[me] = found

    def gram_copy(offset):
        return remote(
            gram_tile, gram_inbox.at[me],
            gram_send.at[offset], gram_recv.at[offset], place_of(offset),
        )

    def dots_copy(offset):
        return remote(
            dots_tile, dots_inbox.at[me],
            dots_send.at[offset], dots_recv.at[offset], place_of(offset),
        )

    for offset in range(1, devices):
        gram_copy(offset).start()

    @pl.loop(polls - 2, polls)
    def _(index):
        poll(vec_copy, index)

    left_own.wait()
    left_pair.wait_recv()
    left_pass.wait_recv()

    def mix_unit(unit):
        row0 = pl.multiple_of((unit // col_tiles) * row_tile, row_tile)
        col0 = pl.multiple_of(lax.rem(unit, col_tiles) * col_tile, col_tile)

        @pl.loop(0, pairs)
        def _(q):
            proj[q] = jnp.dot(
                left[:, pl.ds(row0, row_tile), :].reshape(slots * row_tile, depth),
                vec[:, q, :, pl.ds(col0, col_tile)].reshape(depth, col_tile),
                preferred_element_type=jnp.float32,
            ).reshape(slots, row_tile, col_tile)

        owner = row0 // rows
        base = owner * (pairs * rows) + row0 - owner * rows

        @pl.loop(0, row_tile // 16)
        def _(g):
            lines = []
            for h in range(2):
                at = pl.ds(pl.multiple_of(g * 16 + h * 8, 8), 8)
                stacked = jnp.concatenate(
                    [proj[q, k, at, :] for k in range(slots) for q in range(pairs)], axis=0
                )
                lines.append(
                    jnp.dot(
                        mix_ref[...],
                        stacked,
                        precision=lax.Precision.HIGHEST,
                        preferred_element_type=jnp.float32,
                    )
                )
            for y in range(slots):
                cols = pl.ds(pl.multiple_of(y * quarter + col0, col_tile), col_tile)
                for p in range(pairs):
                    i = (y * pairs + p) * 8
                    at = pl.ds(pl.multiple_of(base + p * rows + g * 16, 16), 16)
                    mixed[at, cols] = jnp.concatenate(
                        [m[i : i + 8] for m in lines], axis=0
                    ).astype(mixed.dtype)

    lot = pairs * rows

    def pair_copy(unit):
        return remote(
            parts.at[chips + lax.rem(unit, 2)], pair_in.at[unit],
            pair_send.at[unit], pair_recv.at[unit], partner,
        )

    def block_of(unit, way):
        return chip_at(place - unit) if way == 0 else chip_at(place + unit)

    def home_of(unit, way):
        at = block_of(unit, way)
        return at // half, lax.rem(at, half) * 2 + way

    def cut_copy(unit, way):
        _, piece = home_of(unit, way)
        return remote(
            parts.at[unit, way], cut_in.at[piece],
            cut_send.at[unit, way], cut_recv.at[piece], across,
        )

    def image_half(unit, sub):
        @pl.when((unit >= 2) & (sub == 0))
        def _():
            pair_copy(unit - 2).wait_send()

        at = lax.rem(sub + core, 2)
        cols = pl.ds(pl.multiple_of(at * span, span), span)

        @pl.loop(0, 2)
        def _(k):
            owner = lax.rem(core + 1 + k, 2)
            to = (1 - k) * (chips + lax.rem(unit, 2)) + k * unit
            lines = jnp.concatenate(
                [
                    right[block_of(unit, way), way * rows : (way + 1) * rows, cols]
                    for way in range(2)
                ],
                axis=0,
            )
            out = lax.dot_general(
                mixed[pl.ds(pl.multiple_of(owner * lot, lot), lot), cols],
                lines,
                (((1,), (1,)), ((), ())),
                preferred_element_type=jnp.float32,
            )

            @pl.when(sub == 0)
            def _():
                for way in range(2):
                    piece = out[:, way * rows : (way + 1) * rows]
                    parts[to, way] = piece.reshape(pairs, rows, rows)

            @pl.when(sub == 1)
            def _():
                for way in range(2):
                    piece = out[:, way * rows : (way + 1) * rows]
                    parts[to, way] += piece.reshape(pairs, rows, rows)

            @pl.when((sub == 1) & (k == 0))
            def _():
                pair_copy(unit).start()

    def join_unit(unit):
        pair_copy(unit).wait_recv()
        for way in range(2):
            parts[unit, way] += pair_in[unit, way]
            home, piece = home_of(unit, way)

            @pl.when(home != cut)
            def _():
                cut_copy(unit, way).start()

    def fetch_unit(unit):
        for way in range(2):
            home, piece = home_of(unit, way)

            @pl.when(home == cut)
            def _():
                stream_copy(piece, way).start()

    def settle_unit(unit):
        for way in range(2):
            home, piece = home_of(unit, way)

            @pl.when(home == cut)
            def _():
                cut_copy(unit, way).wait_recv()
                cols = pl.ds(pl.multiple_of(piece * rows, rows), rows)
                whole = parts[unit, way] + cut_in[piece]
                for p in range(pairs):
                    next_ref[:, p, cols] = whole[p]
                stream_copy(piece, way).wait()

                def add(step, sums):
                    sums = list(sums)
                    for line in range(16):
                        at = step * 16 + line
                        image = next_ref[at, :, cols]
                        for j in range(basis_count):
                            sums[j] += stream[way, j, at, :, :] * image
                        sums[basis_count] += image * image
                    return tuple(sums)

                sums = lax.fori_loop(
                    0, rows // 16, add, tuple(dots_ref[j] for j in range(basis_count + 1))
                )
                for j in range(basis_count + 1):
                    dots_ref[j] = sums[j]

    first = polls - chips

    @pl.loop(0, first)
    def _(index):
        poll(right_copy, index)

        @pl.loop((mix_units * index) // first, (mix_units * (index + 1)) // first)
        def _(unit):
            mix_unit(unit)

    def ready(index):
        return jnp.minimum(2 * (index - first) + 3, index + 3)

    @pl.loop(first, polls)
    def _(index):
        poll(right_copy, index)

        @pl.loop(jnp.where(index == first, 0, ready(index - 1)), ready(index))
        def _(piece):
            unit, sub = piece // 2, lax.rem(piece, 2)
            image_half(unit, sub)

            @pl.when(sub == 1)
            def _():
                join_unit(unit)

            @pl.when((sub == 1) & (unit == 1))
            def _():
                fetch_unit(0)

            @pl.when((sub == 1) & (unit > 1) & (unit < last))
            def _():
                settle_unit(unit - 2)
                fetch_unit(unit - 1)

    slots_held = stream.shape[0]
    stream_copy(0, slots_held - 1).start()
    settle_unit(last - 2)
    fetch_unit(last - 1)
    settle_unit(last - 1)
    fetch_unit(last)
    for offset in range(1, devices):
        gram_copy(offset).wait_recv()
    gram = gram_inbox[0]
    for d in range(1, devices):
        gram = gram + gram_inbox[d]
    gram = gram / entries
    settle_unit(last)
    for piece in range(1, slots_held):
        stream_copy(piece, piece - 1).start()

    spot = lax.broadcasted_iota(jnp.int32, dots_tile.shape, 1)
    found = jnp.zeros(dots_tile.shape, jnp.float32)
    for j in range(basis_count + 1):
        found = jnp.where(spot == j, total_of(dots_ref[j]), found)
    dots_tile[...] = found
    dots_inbox[me] = found
    for offset in range(1, devices):
        dots_copy(offset).start()
    for offset in range(1, devices):
        dots_copy(offset).wait_recv()
    along = dots_inbox[0]
    for d in range(1, devices):
        along = along + dots_inbox[d]
    along = along / entries

    n, end, prior = basis_count, basis_count - 1, basis_count - 2
    spread = jnp.broadcast_to(along, gram_tile.shape)
    down = jnp.sum(jnp.where(row == lane, spread, 0.0), axis=1, keepdims=True)[0:n]
    square = along[:, n : n + 1]
    along = along[:, 0:n]
    gram = gram[0:n, 0:n]
    alpha = down[end : end + 1]
    beta = jnp.full((1, 1), beta_ref[0], jnp.float32)
    ortho = down - alpha * gram[:, end : end + 1] - beta * gram[:, prior : prior + 1]
    ortho_row = along - alpha * gram[end : end + 1, :] - beta * gram[prior : prior + 1, :]
    first = (
        square
        - 2.0 * alpha * alpha
        - 2.0 * beta * down[prior : prior + 1]
        + alpha * alpha * gram[end : end + 1, end : end + 1]
        + 2.0 * alpha * beta * gram[end : end + 1, prior : prior + 1]
        + beta * beta * gram[prior : prior + 1, prior : prior + 1]
    )
    bent = jnp.sum(ortho * gram, axis=0, keepdims=True) * ortho_row
    mean = (
        first
        - 2.0 * jnp.sum(ortho * ortho, axis=0, keepdims=True)
        + jnp.sum(bent, axis=1, keepdims=True)
    )
    beta_new = jnp.sqrt(mean + 1e-06)
    values_ref[...] = jnp.where(
        (row == 0) & (lane == 0), alpha, jnp.where((row == 0) & (lane == 1), beta_new, 0.0)
    )
    index = lax.broadcasted_iota(jnp.int32, ortho.shape, 0)
    coefs = ortho + jnp.where(index == end, alpha, 0.0) + jnp.where(index == prior, beta, 0.0)
    coefs = [jnp.broadcast_to(coefs[j : j + 1], (pairs, lanes)) for j in range(n)]
    scale = jnp.broadcast_to(1.0 / beta_new, (pairs, lanes))

    @pl.loop(0, pieces)
    def _(piece):
        slot = lax.rem(piece + slots_held - 1, slots_held)
        stream_copy(piece, slot).wait()
        cols = pl.ds(pl.multiple_of(piece * lanes, lanes), lanes)

        @pl.loop(0, rows // 32)
        def _(step):
            for line in range(32):
                at = step * 32 + line
                value = next_ref[at, :, cols]
                for j in range(n):
                    value = value - coefs[j] * stream[slot, j, at, :, :]
                next_ref[at, :, cols] = value * scale

        @pl.when(piece + slots_held < pieces)
        def _():
            stream_copy(piece + slots_held, slot).start()

    @pl.loop(0, chips)
    def _(unit):
        for way in range(2):
            home, _ = home_of(unit, way)

            @pl.when(home != cut)
            def _():
                cut_copy(unit, way).wait_send()

    drain(vec_copy)
    drain(right_copy)
    for unit in (chips - 2, chips - 1):
        pair_copy(unit).wait_send()
    vec_pre.wait_send()
    left_across.wait_send()
    for copy in right_pre:
        copy.wait_send()
    left_pair.wait_send()
    left_pass.wait_send()
    for offset in range(1, devices):
        gram_copy(offset).wait_send()
        dots_copy(offset).wait_send()


def ring_step(blocks, cuts, entries, table, left_env, right_env, current, basis, beta_prev):
    rows, half_slots, depth = left_env.shape
    pairs, cols = current.shape[1], current.shape[2]
    slots, chips, quarter = 2 * half_slots, depth // (2 * rows), cols // 2
    basis_count = basis.shape[0]
    count = basis_count * (basis_count + 1) // 2
    square = table.transpose(1, 2, 0, 3).reshape(slots * pairs, slots * pairs)
    vec = current.transpose(1, 0, 2)
    left = left_env.transpose(1, 0, 2)
    right = right_env.transpose(1, 0, 2)
    bf16, f32 = jnp.bfloat16, jnp.float32
    sem = pltpu.SemaphoreType.DMA
    steps = chips - 1
    hbm = pl.BlockSpec(memory_space=pltpu.HBM)
    vmem = pl.BlockSpec(memory_space=pltpu.VMEM)
    devices = blocks * cuts
    smem = pl.BlockSpec(memory_space=pltpu.SMEM)
    next_vector, values = pl.pallas_call(
        functools.partial(ring_kernel, blocks, cuts, entries),
        name="ring",
        in_specs=[smem, hbm, hbm, hbm, vmem, hbm],
        out_specs=[vmem, vmem],
        out_shape=[
            jax.ShapeDtypeStruct((rows, pairs, cols), f32),
            jax.ShapeDtypeStruct((8, 128), f32),
        ],
        scratch_shapes=[
            pltpu.VMEM((chips, pairs, 2 * rows, quarter), bf16),
            pltpu.VMEM((slots, 2 * rows, depth), bf16),
            pltpu.VMEM((chips, 2 * rows, slots * quarter), bf16),
            pltpu.VMEM((2 * pairs * rows, slots * quarter), bf16),
            pltpu.VMEM((slots * pairs * 8, slots * pairs * 8), f32),
            pltpu.VMEM((pairs, slots, rows // 2, quarter // 2), f32),
            pltpu.VMEM((chips + 2, 2, pairs, rows, rows), f32),
            pltpu.VMEM((chips, 2, pairs, rows, rows), f32),
            pltpu.VMEM((chips, pairs, rows, rows), f32),
            pltpu.VMEM((3, basis_count, rows, pairs, 128), f32),
            pltpu.VMEM((count, pairs, 128), f32),
            pltpu.VMEM((basis_count + 1, pairs, 128), f32),
            pltpu.VMEM((8, 128), f32),
            pltpu.VMEM((devices, 8, 128), f32),
            pltpu.VMEM((1, 128), f32),
            pltpu.VMEM((devices, 1, 128), f32),
            sem((devices,)),
            sem((devices,)),
            sem((devices,)),
            sem((devices,)),
            sem((2 + half_slots,)),
            sem((4 + 3 * half_slots,)),
            sem((4 + 3 * half_slots,)),
            sem((2, steps, 2)),
            sem((2, steps, 2)),
            sem((2, steps, 2)),
            sem((2, steps, 2)),
            sem((chips,)),
            sem((chips,)),
            sem((chips, 2)),
            sem((chips,)),
            sem((3,)),
        ],
        compiler_params=pltpu.CompilerParams(
            vmem_limit_bytes=65400 * 1024, collective_id=1, has_side_effects=True
        ),
    )(beta_prev.reshape(1), vec, left, right, square, basis)
    return next_vector, values[0, 0:1], values[0, 1:2]


def ring_fits(blocks, rows, basis_count):
    return blocks == 16 and rows == 128 and basis_count == 8


def gathered_image(cuts, table, left_env, right_env, current):
    row_count, pair_count, col_count = current.shape
    bond_width = table.shape[0]
    full_width = left_env.shape[2]
    me = lax.axis_index("cuts")
    swap = [(0, 1), (1, 0)]

    current = current.transpose(1, 0, 2)
    left_t = left_env.transpose(1, 0, 2)
    right_t = right_env.transpose(1, 0, 2)
    if cuts == 2:
        half = left_t.shape[0]
        theirs = lax.dynamic_slice_in_dim(right_t, (1 - me) * col_count, col_count, 2)
        mine = lax.dynamic_slice_in_dim(right_t, me * col_count, col_count, 2)
        right_k = jnp.concatenate([mine, lax.ppermute(theirs, "cuts", swap)], axis=0)
        left_k = jnp.concatenate([left_t, lax.ppermute(left_t, "cuts", swap)], axis=0)
        turned = jnp.roll(jnp.roll(table, -half, axis=0), -half, axis=1)
        table = jnp.where(me == 0, table, turned)
    else:
        left_k = lax.all_gather(left_t, "cuts", axis=0, tiled=True)
        right_k = lax.all_to_all(right_t, "cuts", split_axis=2, concat_axis=0, tiled=True)
    cur_full = lax.all_gather(current, "blk", axis=1, tiled=True)
    right_full = lax.all_gather(right_k, "blk", axis=1, tiled=True)

    mixed = mixed_left_of(table, left_k, cur_full)
    mixed = mixed.reshape(bond_width, pair_count * row_count, col_count)
    if cuts == 2:
        away = image_part(mixed, right_full, (1 - me) * col_count, col_count)
        away = lax.ppermute(away, "cuts", swap)
        here = image_part(mixed, right_full, me * col_count, col_count)
        image = here + away
    else:
        image = image_part(mixed, right_full, jnp.int32(0), full_width)
        image = lax.psum_scatter(image, "cuts", scatter_dimension=1, tiled=True)
    return image.reshape(pair_count, row_count, col_count).transpose(1, 0, 2)


def on_device(
    blocks, cuts, left_env, right_env, left_core, right_core, slot_bond, krylov_basis, beta_prev
):
    pair_count = left_core.shape[2] * left_core.shape[2]
    basis_count, row_count, _, _ = krylov_basis.shape
    full_width = left_env.shape[2]
    entries = float(full_width * pair_count * full_width)
    table = build_table(left_core, right_core, slot_bond)
    current = krylov_basis[basis_count - 1].astype(jnp.bfloat16)
    if cuts == 2 and ring_fits(blocks, row_count, basis_count):
        return ring_step(
            blocks, cuts, entries, table, left_env, right_env, current, krylov_basis, beta_prev
        )
    image = gathered_image(cuts, table, left_env, right_env, current)
    gram = gram_of(krylov_basis)

    sums = lax.psum(jnp.concatenate([gram, dots_of(krylov_basis, image)]), ("blk", "cuts"))
    sums = sums / entries
    count = basis_count * (basis_count + 1) // 2
    where = []
    for j in range(basis_count):
        for k in range(basis_count):
            low, high = min(j, k), max(j, k)
            where.append(low * basis_count - low * (low - 1) // 2 + high - low)
    gram_matrix = sums[jnp.array(where)].reshape(basis_count, basis_count)
    inner_prods = sums[count : count + basis_count]
    image_square = sums[count + basis_count]
    last, prior = basis_count - 1, basis_count - 2
    alpha_now = inner_prods[last]
    ortho_coeffs = (
        inner_prods - alpha_now * gram_matrix[:, last] - beta_prev * gram_matrix[:, prior]
    )
    first_square = (
        image_square
        - 2.0 * alpha_now * inner_prods[last]
        - 2.0 * beta_prev * inner_prods[prior]
        + alpha_now * alpha_now * gram_matrix[last, last]
        + 2.0 * alpha_now * beta_prev * gram_matrix[last, prior]
        + beta_prev * beta_prev * gram_matrix[prior, prior]
    )
    square_mean = (
        first_square
        - 2.0 * jnp.sum(ortho_coeffs * ortho_coeffs)
        + jnp.sum(ortho_coeffs[:, None] * gram_matrix * ortho_coeffs[None, :])
    )
    beta_new = jnp.sqrt(square_mean + 1e-06)
    index = jnp.arange(basis_count)
    coefs = (
        ortho_coeffs
        + jnp.where(index == last, alpha_now, 0.0)
        + jnp.where(index == prior, beta_prev, 0.0)
    )
    coefs = jnp.concatenate([coefs, (1.0 / beta_new)[None]])
    next_vector = final_of(coefs, krylov_basis, image)
    return (next_vector, alpha_now[None], beta_new[None])


def solution(mesh):
    in_specs = (
        P("blk", "cuts", None),
        P("blk", "cuts", None),
        P(),
        P(),
        P(),
        P(None, "blk", None, "cuts"),
        P(),
    )
    out_specs = (P("blk", None, "cuts"), P(), P())
    return jax.shard_map(
        functools.partial(on_device, mesh.shape["blk"], mesh.shape["cuts"]),
        mesh=mesh,
        in_specs=in_specs,
        out_specs=out_specs,
        check_vma=False,
    )
```

```python
import functools

import jax
import jax.numpy as jnp
from jax import lax
from jax.experimental import pallas as pl
from jax.experimental.pallas import tpu as pltpu
from jax.sharding import PartitionSpec as P

VMEM_BYTES = 60 * 1024 * 1024


def params():
    return pltpu.CompilerParams(vmem_limit_bytes=VMEM_BYTES)


def tile_of(size, most):
    return most if size % most == 0 else size


def build_table(left_core, right_core, slot_bond):
    bond_width = left_core.shape[0]
    phys_dim = left_core.shape[2]
    chosen = (slot_bond[:, None] == jnp.arange(bond_width, dtype=jnp.int32)[None, :]).astype(
        jnp.float32
    )
    picked = jnp.einsum("kw,wxac->kxac", chosen, left_core, precision=lax.Precision.HIGHEST)
    table = jnp.einsum("kxac,xybd->kyabcd", picked, right_core, precision=lax.Precision.HIGHEST)
    return table.reshape(bond_width, bond_width, phys_dim * phys_dim, phys_dim * phys_dim)


def mix_kernel(mix_ref, left_ref, cur_ref, out_ref, proj):
    slots, rows, depth = left_ref.shape
    pairs = cur_ref.shape[0]
    bonds = out_ref.shape[0]
    cols = cur_ref.shape[2]

    @pl.loop(0, pairs)
    def _(q):
        proj[q] = jnp.dot(
            left_ref[...].reshape(slots * rows, depth),
            cur_ref[q],
            preferred_element_type=jnp.float32,
        ).reshape(slots, rows, cols)

    @pl.loop(0, rows // 16)
    def _(g):
        mixed = []
        for h in range(2):
            at = pl.ds(pl.multiple_of(g * 16 + h * 8, 8), 8)
            stacked = jnp.concatenate(
                [proj[q, k, at, :] for k in range(slots) for q in range(pairs)], axis=0
            )
            mixed.append(
                jnp.dot(
                    mix_ref[...],
                    stacked,
                    precision=lax.Precision.HIGHEST,
                    preferred_element_type=jnp.float32,
                )
            )
        at = pl.ds(pl.multiple_of(g * 16, 16), 16)
        for y in range(bonds):
            for p in range(pairs):
                i = (y * pairs + p) * 8
                out_ref[y, p, at, :] = jnp.concatenate(
                    [m[i : i + 8] for m in mixed], axis=0
                ).astype(out_ref.dtype)


def mixed_left_of(table, left_k, cur_full):
    slots, rows, depth = left_k.shape
    pairs, _, cols = cur_full.shape
    bonds = table.shape[1]
    tb = tile_of(cols, 256)
    square = table.transpose(1, 2, 0, 3).reshape(bonds * pairs, slots * pairs)
    mix = jnp.kron(square, jnp.eye(8, dtype=jnp.float32))
    return pl.pallas_call(
        mix_kernel,
        grid=(cols // tb,),
        in_specs=[
            pl.BlockSpec(mix.shape, lambda i: (0, 0)),
            pl.BlockSpec((slots, rows, depth), lambda i: (0, 0, 0)),
            pl.BlockSpec((pairs, depth, tb), lambda i: (0, 0, i)),
        ],
        out_specs=pl.BlockSpec((bonds, pairs, rows, tb), lambda i: (0, 0, 0, i)),
        out_shape=jax.ShapeDtypeStruct((bonds, pairs, rows, cols), jnp.bfloat16),
        scratch_shapes=[pltpu.VMEM((pairs, slots, rows, tb), jnp.float32)],
        compiler_params=params(),
        cost_estimate=pl.CostEstimate(
            flops=2 * slots * rows * depth * pairs * cols,
            bytes_accessed=2 * (left_k.size + cur_full.size + bonds * pairs * rows * cols),
            transcendentals=0,
        ),
    )(mix, left_k, cur_full)


def image_kernel(start_ref, mixed_ref, right_ref, out_ref):
    bonds = mixed_ref.shape[0]
    out_ref[...] = jnp.zeros_like(out_ref)

    @pl.loop(0, bonds)
    def _(y):
        out_ref[...] += lax.dot_general(
            mixed_ref[y],
            right_ref[y],
            (((1,), (1,)), ((), ())),
            preferred_element_type=jnp.float32,
        )


def image_part(mixed, right_full, start, count):
    bonds, lines, cols = mixed.shape
    tb = tile_of(count, 256)
    return pl.pallas_call(
        image_kernel,
        grid_spec=pltpu.PrefetchScalarGridSpec(
            num_scalar_prefetch=1,
            grid=(count // tb,),
            in_specs=[
                pl.BlockSpec((bonds, lines, cols), lambda i, s: (0, 0, 0)),
                pl.BlockSpec((bonds, tb, cols), lambda i, s: (0, s[0] + i, 0)),
            ],
            out_specs=pl.BlockSpec((lines, tb), lambda i, s: (0, i)),
        ),
        out_shape=jax.ShapeDtypeStruct((lines, count), jnp.float32),
        compiler_params=params(),
        cost_estimate=pl.CostEstimate(
            flops=2 * bonds * lines * cols * count,
            bytes_accessed=2 * (mixed.size + bonds * count * cols),
            transcendentals=0,
        ),
    )((start // tb).reshape(1).astype(jnp.int32), mixed, right_full)


def gram_kernel(basis_ref, out_ref):
    basis_count, rows, pairs, cols = basis_ref.shape
    chunk = 4
    lanes = cols // 128

    @pl.when(pl.program_id(0) == 0)
    def _():
        out_ref[...] = jnp.zeros_like(out_ref)

    @pl.loop(0, rows // chunk)
    def _(r):
        for c in range(lanes):
            vecs = [
                basis_ref[j, pl.ds(r * chunk, chunk), :, c * 128 : (c + 1) * 128]
                for j in range(basis_count)
            ]
            i = 0
            for j in range(basis_count):
                for k in range(j, basis_count):
                    out_ref[i] += jnp.sum(vecs[j] * vecs[k], axis=0)
                    i += 1


def gram_of(basis):
    basis_count, rows, pairs, cols = basis.shape
    count = basis_count * (basis_count + 1) // 2
    ta = tile_of(rows, 16)
    sums = pl.pallas_call(
        gram_kernel,
        grid=(rows // ta,),
        in_specs=[pl.BlockSpec((basis_count, ta, pairs, cols), lambda i: (0, i, 0, 0))],
        out_specs=pl.BlockSpec((count, pairs, 128), lambda i: (0, 0, 0)),
        out_shape=jax.ShapeDtypeStruct((count, pairs, 128), jnp.float32),
        compiler_params=params(),
        cost_estimate=pl.CostEstimate(
            flops=2 * count * rows * pairs * cols,
            bytes_accessed=4 * basis.size,
            transcendentals=0,
        ),
    )(basis)
    return jnp.sum(sums, axis=(1, 2))


def dots_kernel(basis_ref, image_ref, out_ref):
    basis_count, rows, pairs, cols = basis_ref.shape

    @pl.when(pl.program_id(0) == 0)
    def _():
        out_ref[...] = jnp.zeros_like(out_ref)

    for c in range(cols // 128):
        at = slice(c * 128, (c + 1) * 128)
        image = image_ref[:, :, at]
        for j in range(basis_count):
            out_ref[j] += jnp.sum(basis_ref[j, :, :, at] * image, axis=0)
        out_ref[basis_count] += jnp.sum(image * image, axis=0)


def dots_of(basis, image):
    basis_count, rows, pairs, cols = basis.shape
    ta = tile_of(rows, 16)
    sums = pl.pallas_call(
        dots_kernel,
        grid=(rows // ta,),
        in_specs=[
            pl.BlockSpec((basis_count, ta, pairs, cols), lambda i: (0, i, 0, 0)),
            pl.BlockSpec((ta, pairs, cols), lambda i: (i, 0, 0)),
        ],
        out_specs=pl.BlockSpec((basis_count + 1, pairs, 128), lambda i: (0, 0, 0)),
        out_shape=jax.ShapeDtypeStruct((basis_count + 1, pairs, 128), jnp.float32),
        compiler_params=params(),
    )(basis, image)
    return jnp.sum(sums, axis=(1, 2))


def final_kernel(coef_ref, basis_ref, image_ref, out_ref):
    basis_count = basis_ref.shape[0]
    total = image_ref[...]
    for j in range(basis_count):
        total = total - coef_ref[j] * basis_ref[j]
    out_ref[...] = total * coef_ref[basis_count]


def final_of(coefs, basis, image):
    basis_count, rows, pairs, cols = basis.shape
    ta = tile_of(rows, 16)
    return pl.pallas_call(
        final_kernel,
        grid=(rows // ta,),
        in_specs=[
            pl.BlockSpec(memory_space=pltpu.SMEM),
            pl.BlockSpec((basis_count, ta, pairs, cols), lambda i: (0, i, 0, 0)),
            pl.BlockSpec((ta, pairs, cols), lambda i: (i, 0, 0)),
        ],
        out_specs=pl.BlockSpec((ta, pairs, cols), lambda i: (i, 0, 0)),
        out_shape=jax.ShapeDtypeStruct((rows, pairs, cols), jnp.float32),
        compiler_params=params(),
    )(coefs, basis, image)


MESH = pl.DeviceIdType.MESH


def ring_kernel(
    blocks, cuts, entries,
    beta_ref, left_ref, right_ref, square_ref, basis_ref,
    next_ref, values_ref,
    vec, left, right, mixed, mix_ref, proj, parts, pair_in, cut_in, stream, raw,
    gram_ref, dots_ref, gram_tile, gram_inbox, dots_tile, dots_inbox,
    gram_send, gram_recv, dots_send, dots_recv,
    own_sem, raw_sem, pre_send, pre_recv, vec_send, vec_recv, right_send, right_recv,
    pair_send, pair_recv, cut_send, cut_recv, stream_sem,
):
    chips, pairs, chip_rows, quarter = vec.shape
    slots, _, depth = left.shape
    rows, half_slots, _ = left_ref.shape
    span = half_slots * quarter
    last = chips - 1
    polls = 2 * last
    row_tile, col_tile = proj.shape[2], proj.shape[3]
    col_tiles = quarter // col_tile
    mix_units = (chip_rows // row_tile) * col_tiles
    basis_count = basis_ref.shape[0]
    lanes = stream.shape[4]
    pieces = basis_ref.shape[3] // lanes
    half = chips // 2

    blk = lax.axis_index("blk")
    cut = lax.axis_index("cuts")
    core = lax.rem(blk, 2)
    chip = blk // 2
    side = lax.rem(chip, 2)
    place = (1 - side) * (chip // 2) + side * (last - chip // 2)

    def chip_at(index):
        index = lax.rem(index + 2 * chips, chips)
        far = index // half
        return (1 - far) * 2 * index + far * (2 * (last - index) + 1)

    after = (2 * chip_at(place + 1) + core, cut)
    before = (2 * chip_at(place - 1) + core, cut)
    onward = (after, before)
    partner = (2 * chip + 1 - core, cut)
    across = (blk, 1 - cut)
    corner = (2 * chip + 1 - core, 1 - cut)

    def remote(src, dst, send, recv, device):
        return pltpu.make_async_remote_copy(
            src_ref=src, dst_ref=dst, send_sem=send, recv_sem=recv,
            device_id=device, device_id_type=MESH,
        )

    def from_place(way, step):
        return chip_at(place - 1 - step) if way == 0 else chip_at(place + 1 + step)

    def vec_copy(way, step, sub, at):
        view = vec.at[at, pl.ds(way * (pairs // 2), pairs // 2), pl.ds(sub * rows, rows), :]
        return remote(
            view, view, vec_send.at[way, step, sub], vec_recv.at[way, step, sub], onward[way]
        )

    def right_copy(way, step, sub, at):
        view = right.at[at, pl.ds(way * rows, rows), pl.ds(sub * span, span)]
        return remote(
            view, view, right_send.at[way, step, sub], right_recv.at[way, step, sub], onward[way]
        )

    def poll(copy_of, index):
        step, sub = index // 2, lax.rem(index + core, 2)
        for way in range(2):
            at = from_place(way, step)
            copy_of(way, step, sub, at).wait_recv()

            @pl.when(step < last - 1)
            def _():
                copy_of(way, step + 1, sub, at).start()

    def drain(copy_of):
        @pl.loop(0, polls)
        def _(index):
            for way in range(2):
                copy_of(way, index // 2, lax.rem(index, 2), chip).wait_send()

    mine = pl.ds(core * rows, rows)
    left_view = left.at[pl.ds(cut * half_slots, half_slots), mine, :]
    left_other = left.at[pl.ds((1 - cut) * half_slots, half_slots), mine, :]
    right_view = right.at[chip, mine, pl.ds(cut * span, span)]
    vec_load = pltpu.make_async_copy(basis_ref.at[basis_count - 1], next_ref, own_sem)
    vec_load.start()
    raw_rows = raw.shape[1]
    raw_units = rows // raw_rows

    def raw_copy(unit):
        source = right_ref if unit < raw_units else left_ref
        at = pl.ds((unit % raw_units) * raw_rows, raw_rows)
        return pltpu.make_async_copy(source.at[at], raw.at[unit % 2], raw_sem.at[unit % 2])

    raw_copy(0).start()
    raw_copy(1).start()

    def stream_copy(piece, slot):
        return pltpu.make_async_copy(
            basis_ref.at[:, :, :, pl.ds(pl.multiple_of(piece * lanes, lanes), lanes)],
            stream.at[slot],
            stream_sem.at[slot],
        )

    devices = blocks * cuts
    me = blk * cuts + cut

    def place_of(offset):
        device = lax.rem(me + offset, devices)
        return (device // cuts, lax.rem(device, cuts))

    barrier = pltpu.get_barrier_semaphore()
    for offset in range(1, devices):
        pl.semaphore_signal(barrier, inc=1, device_id=place_of(offset), device_id_type=MESH)

    vec_load.wait()
    for unit in range(rows // 16):
        at = slice(unit * 16, (unit + 1) * 16)
        to = pl.ds(pl.multiple_of(core * rows + unit * 16, 16), 16)
        for whose in range(2):
            owner = (core + whose) % 2
            cols = pl.ds(pl.multiple_of(owner * quarter, quarter), quarter)
            turned = jnp.swapaxes(next_ref[at, :, cols].astype(vec.dtype), 0, 1)
            if whose == 0:
                vec[chip, :, to, :] = turned
            else:
                for q in range(pairs):
                    mixed[at, q * quarter : (q + 1) * quarter] = turned[q]

    pl.semaphore_wait(barrier, devices - 1)

    vec_pre = [
        remote(
            mixed.at[pl.ds(0, rows), pl.ds(q * quarter, quarter)], vec.at[chip, q, mine, :],
            pre_send.at[6 + q], pre_recv.at[6 + q], partner,
        )
        for q in range(pairs)
    ]
    for copy in vec_pre:
        copy.start()
    for way in range(2):
        vec_copy(way, 0, core, chip).start()

    for unit in range(2 * raw_units):
        raw_copy(unit).wait()
        turned = jnp.swapaxes(raw[unit % 2], 0, 1)
        start = (unit % raw_units) * raw_rows
        to = pl.ds(pl.multiple_of(core * rows + start, raw_rows), raw_rows)
        if unit < raw_units:
            own = pl.ds(pl.multiple_of((2 * cut + core) * quarter, quarter), quarter)
            owned = jnp.swapaxes(raw[unit % 2, :, :, own], 0, 1)
            for slot in range(half_slots):
                cols = pl.ds(pl.multiple_of(cut * span + slot * quarter, quarter), quarter)
                right[chip, to, cols] = owned[slot]
                for e in range(4):
                    at = slice((1 + e) * rows + start, (1 + e) * rows + start + raw_rows)
                    mixed[at, slot * quarter : (slot + 1) * quarter] = turned[
                        slot, :, e * quarter : (e + 1) * quarter
                    ]
        else:
            left[pl.ds(cut * half_slots, half_slots), to, :] = turned
        if unit + 2 < 2 * raw_units:
            raw_copy(unit + 2).start()

    def right_part(to_cut, to_core):
        first_row = pl.multiple_of((1 + 2 * to_cut + to_core) * rows, rows)
        return mixed.at[pl.ds(first_row, rows), pl.ds(0, span)]

    for copy in vec_pre:
        copy.wait_recv()
    for way in range(2):
        vec_copy(way, 0, 1 - core, chip).start()

    right_pre = (
        remote(
            right_part(1 - cut, core), right_view, pre_send.at[2], pre_recv.at[2], across
        ),
        remote(
            right_part(1 - cut, 1 - core), right_view, pre_send.at[4], pre_recv.at[4], corner
        ),
        remote(
            right_part(cut, 1 - core), right_view, pre_send.at[5], pre_recv.at[5], partner
        ),
    )
    for copy in right_pre:
        copy.start()
    left_across = remote(left_view, left_view, pre_send.at[0], pre_recv.at[0], across)
    left_across.start()
    left_pair = remote(left_view, left_view, pre_send.at[1], pre_recv.at[1], partner)
    left_pair.start()
    stream_copy(0, 0).start()
    gram_ref[...] = jnp.zeros_like(gram_ref)
    dots_ref[...] = jnp.zeros_like(dots_ref)

    wide = lax.broadcasted_iota(jnp.int32, (mix_ref.shape[0], slots * pairs), 0)
    thin = lax.broadcasted_iota(jnp.int32, (mix_ref.shape[0], slots * pairs), 1)
    stretch = (wide // 8 == thin).astype(jnp.float32)
    tall = jnp.dot(
        stretch, square_ref[...],
        precision=lax.Precision.HIGHEST, preferred_element_type=jnp.float32,
    )
    full = lax.dot_general(
        tall, stretch, (((1,), (1,)), ((), ())),
        precision=lax.Precision.HIGHEST, preferred_element_type=jnp.float32,
    )
    row = lax.broadcasted_iota(jnp.int32, mix_ref.shape, 0)
    lane = lax.broadcasted_iota(jnp.int32, mix_ref.shape, 1)
    mix_ref[...] = jnp.where(lax.rem(row, 8) == lax.rem(lane, 8), full, 0.0)

    def gram_unit(unit):
        slot = lax.rem(unit, 2)
        stream_copy(unit, slot).wait()

        @pl.when(unit + 1 < pieces)
        def _():
            stream_copy(unit + 1, 1 - slot).start()

        chunk = 4

        @pl.loop(0, rows // chunk)
        def _(r):
            vecs = [stream[slot, j, pl.ds(r * chunk, chunk), :, :] for j in range(basis_count)]
            i = 0
            for j in range(basis_count):
                for k in range(j, basis_count):
                    gram_ref[i] += jnp.sum(vecs[j] * vecs[k], axis=0)
                    i += 1

    @pl.loop(0, polls - 2)
    def _(index):
        poll(vec_copy, index)

        @pl.when(index < pieces)
        def _():
            gram_unit(index)

    for copy in right_pre:
        copy.wait_recv()
    for sub in range(2):
        for way in range(2):
            right_copy(way, 0, lax.rem(sub + core, 2), chip).start()

    left_across.wait_recv()
    left_pass = remote(left_other, left_other, pre_send.at[3], pre_recv.at[3], partner)
    left_pass.start()

    def total_of(x):
        return jnp.sum(jnp.sum(x, axis=0, keepdims=True), axis=1, keepdims=True)

    row = lax.broadcasted_iota(jnp.int32, gram_tile.shape, 0)
    lane = lax.broadcasted_iota(jnp.int32, gram_tile.shape, 1)
    found = jnp.zeros(gram_tile.shape, jnp.float32)
    i = 0
    for j in range(basis_count):
        for k in range(j, basis_count):
            here = ((row == j) & (lane == k)) | ((row == k) & (lane == j))
            found = jnp.where(here, total_of(gram_ref[i]), found)
            i += 1
    gram_tile[...] = found
    gram_inbox[me] = found

    def gram_copy(offset):
        return remote(
            gram_tile, gram_inbox.at[me],
            gram_send.at[offset], gram_recv.at[offset], place_of(offset),
        )

    def dots_copy(offset):
        return remote(
            dots_tile, dots_inbox.at[me],
            dots_send.at[offset], dots_recv.at[offset], place_of(offset),
        )

    for offset in range(1, devices):
        gram_copy(offset).start()

    @pl.loop(polls - 2, polls)
    def _(index):
        poll(vec_copy, index)

    for copy in vec_pre:
        copy.wait_send()
    for copy in right_pre:
        copy.wait_send()
    left_pair.wait_recv()
    left_pass.wait_recv()

    def mix_unit(unit):
        row0 = pl.multiple_of((unit // col_tiles) * row_tile, row_tile)
        col0 = pl.multiple_of(lax.rem(unit, col_tiles) * col_tile, col_tile)

        @pl.loop(0, pairs)
        def _(q):
            proj[q] = jnp.dot(
                left[:, pl.ds(row0, row_tile), :].reshape(slots * row_tile, depth),
                vec[:, q, :, pl.ds(col0, col_tile)].reshape(depth, col_tile),
                preferred_element_type=jnp.float32,
            ).reshape(slots, row_tile, col_tile)

        owner = row0 // rows
        base = owner * (pairs * rows) + row0 - owner * rows

        @pl.loop(0, row_tile // 16)
        def _(g):
            lines = []
            for h in range(2):
                at = pl.ds(pl.multiple_of(g * 16 + h * 8, 8), 8)
                stacked = jnp.concatenate(
                    [proj[q, k, at, :] for k in range(slots) for q in range(pairs)], axis=0
                )
                lines.append(
                    jnp.dot(
                        mix_ref[...],
                        stacked,
                        precision=lax.Precision.HIGHEST,
                        preferred_element_type=jnp.float32,
                    )
                )
            for y in range(slots):
                cols = pl.ds(pl.multiple_of(y * quarter + col0, col_tile), col_tile)
                for p in range(pairs):
                    i = (y * pairs + p) * 8
                    at = pl.ds(pl.multiple_of(base + p * rows + g * 16, 16), 16)
                    mixed[at, cols] = jnp.concatenate(
                        [m[i : i + 8] for m in lines], axis=0
                    ).astype(mixed.dtype)

    lot = pairs * rows

    def pair_copy(unit):
        return remote(
            parts.at[chips + lax.rem(unit, 2)], pair_in.at[lax.rem(unit, 2)],
            pair_send.at[unit], pair_recv.at[unit], partner,
        )

    def block_of(unit, way):
        return chip_at(place - unit) if way == 0 else chip_at(place + unit)

    def home_of(unit, way):
        at = block_of(unit, way)
        return at // half, lax.rem(at, half) * 2 + way

    def cut_copy(unit, way):
        _, piece = home_of(unit, way)
        return remote(
            parts.at[unit, way], cut_in.at[piece],
            cut_send.at[unit, way], cut_recv.at[piece], across,
        )

    def image_half(unit, sub):
        @pl.when((unit >= 2) & (sub == 0))
        def _():
            pair_copy(unit - 2).wait_send()

        at = lax.rem(sub + core, 2)
        cols = pl.ds(pl.multiple_of(at * span, span), span)

        @pl.loop(0, 2)
        def _(k):
            owner = lax.rem(core + 1 + k, 2)
            to = (1 - k) * (chips + lax.rem(unit, 2)) + k * unit
            lines = jnp.concatenate(
                [
                    right[block_of(unit, way), way * rows : (way + 1) * rows, cols]
                    for way in range(2)
                ],
                axis=0,
            )
            out = lax.dot_general(
                mixed[pl.ds(pl.multiple_of(owner * lot, lot), lot), cols],
                lines,
                (((1,), (1,)), ((), ())),
                preferred_element_type=jnp.float32,
            )

            @pl.when(sub == 0)
            def _():
                for way in range(2):
                    piece = out[:, way * rows : (way + 1) * rows]
                    parts[to, way] = piece.reshape(pairs, rows, rows)

            @pl.when(sub == 1)
            def _():
                for way in range(2):
                    piece = out[:, way * rows : (way + 1) * rows]
                    parts[to, way] += piece.reshape(pairs, rows, rows)

            @pl.when((sub == 1) & (k == 0))
            def _():
                pair_copy(unit).start()

    def join_unit(unit):
        pair_copy(unit).wait_recv()
        for way in range(2):
            parts[unit, way] += pair_in[lax.rem(unit, 2), way]
            home, piece = home_of(unit, way)

            @pl.when(home != cut)
            def _():
                cut_copy(unit, way).start()

    def fetch_unit(unit):
        for way in range(2):
            home, piece = home_of(unit, way)

            @pl.when(home == cut)
            def _():
                stream_copy(piece, way).start()

    def settle_unit(unit):
        for way in range(2):
            home, piece = home_of(unit, way)

            @pl.when(home == cut)
            def _():
                cut_copy(unit, way).wait_recv()
                cols = pl.ds(pl.multiple_of(piece * rows, rows), rows)
                whole = parts[unit, way] + cut_in[piece]
                for p in range(pairs):
                    next_ref[:, p, cols] = whole[p]
                stream_copy(piece, way).wait()

                def add(step, sums):
                    sums = list(sums)
                    for line in range(16):
                        at = step * 16 + line
                        image = next_ref[at, :, cols]
                        for j in range(basis_count):
                            sums[j] += stream[way, j, at, :, :] * image
                        sums[basis_count] += image * image
                    return tuple(sums)

                sums = lax.fori_loop(
                    0, rows // 16, add, tuple(dots_ref[j] for j in range(basis_count + 1))
                )
                for j in range(basis_count + 1):
                    dots_ref[j] = sums[j]

    first = polls - chips

    @pl.loop(0, first)
    def _(index):
        poll(right_copy, index)

        @pl.loop((mix_units * index) // first, (mix_units * (index + 1)) // first)
        def _(unit):
            mix_unit(unit)

    def ready(index):
        return jnp.minimum(2 * (index - first) + 3, index + 3)

    @pl.loop(first, polls)
    def _(index):
        poll(right_copy, index)

        @pl.loop(jnp.where(index == first, 0, ready(index - 1)), ready(index))
        def _(piece):
            unit, sub = piece // 2, lax.rem(piece, 2)
            image_half(unit, sub)

            @pl.when(sub == 1)
            def _():
                join_unit(unit)

            @pl.when((sub == 1) & (unit == 1))
            def _():
                fetch_unit(0)

            @pl.when((sub == 1) & (unit > 1) & (unit < last))
            def _():
                settle_unit(unit - 2)
                fetch_unit(unit - 1)

    slots_held = stream.shape[0]
    stream_copy(0, slots_held - 1).start()
    settle_unit(last - 2)
    fetch_unit(last - 1)
    settle_unit(last - 1)
    fetch_unit(last)
    for offset in range(1, devices):
        gram_copy(offset).wait_recv()
    gram = gram_inbox[0]
    for d in range(1, devices):
        gram = gram + gram_inbox[d]
    gram = gram / entries
    settle_unit(last)
    for piece in range(1, slots_held):
        stream_copy(piece, piece - 1).start()

    spot = lax.broadcasted_iota(jnp.int32, dots_tile.shape, 1)
    found = jnp.zeros(dots_tile.shape, jnp.float32)
    for j in range(basis_count + 1):
        found = jnp.where(spot == j, total_of(dots_ref[j]), found)
    dots_tile[...] = found
    dots_inbox[me] = found
    for offset in range(1, devices):
        dots_copy(offset).start()
    for offset in range(1, devices):
        dots_copy(offset).wait_recv()
    along = dots_inbox[0]
    for d in range(1, devices):
        along = along + dots_inbox[d]
    along = along / entries

    n, end, prior = basis_count, basis_count - 1, basis_count - 2
    spread = jnp.broadcast_to(along, gram_tile.shape)
    down = jnp.sum(jnp.where(row == lane, spread, 0.0), axis=1, keepdims=True)[0:n]
    square = along[:, n : n + 1]
    along = along[:, 0:n]
    gram = gram[0:n, 0:n]
    alpha = down[end : end + 1]
    beta = jnp.full((1, 1), beta_ref[0], jnp.float32)
    ortho = down - alpha * gram[:, end : end + 1] - beta * gram[:, prior : prior + 1]
    ortho_row = along - alpha * gram[end : end + 1, :] - beta * gram[prior : prior + 1, :]
    first = (
        square
        - 2.0 * alpha * alpha
        - 2.0 * beta * down[prior : prior + 1]
        + alpha * alpha * gram[end : end + 1, end : end + 1]
        + 2.0 * alpha * beta * gram[end : end + 1, prior : prior + 1]
        + beta * beta * gram[prior : prior + 1, prior : prior + 1]
    )
    bent = jnp.sum(ortho * gram, axis=0, keepdims=True) * ortho_row
    mean = (
        first
        - 2.0 * jnp.sum(ortho * ortho, axis=0, keepdims=True)
        + jnp.sum(bent, axis=1, keepdims=True)
    )
    beta_new = jnp.sqrt(mean + 1e-06)
    values_ref[...] = jnp.where(
        (row == 0) & (lane == 0), alpha, jnp.where((row == 0) & (lane == 1), beta_new, 0.0)
    )
    index = lax.broadcasted_iota(jnp.int32, ortho.shape, 0)
    coefs = ortho + jnp.where(index == end, alpha, 0.0) + jnp.where(index == prior, beta, 0.0)
    coefs = [jnp.broadcast_to(coefs[j : j + 1], (pairs, lanes)) for j in range(n)]
    scale = jnp.broadcast_to(1.0 / beta_new, (pairs, lanes))

    @pl.loop(0, pieces)
    def _(piece):
        slot = lax.rem(piece + slots_held - 1, slots_held)
        stream_copy(piece, slot).wait()
        cols = pl.ds(pl.multiple_of(piece * lanes, lanes), lanes)

        @pl.loop(0, rows // 32)
        def _(step):
            for line in range(32):
                at = step * 32 + line
                value = next_ref[at, :, cols]
                for j in range(n):
                    value = value - coefs[j] * stream[slot, j, at, :, :]
                next_ref[at, :, cols] = value * scale

        @pl.when(piece + slots_held < pieces)
        def _():
            stream_copy(piece + slots_held, slot).start()

    @pl.loop(0, chips)
    def _(unit):
        for way in range(2):
            home, _ = home_of(unit, way)

            @pl.when(home != cut)
            def _():
                cut_copy(unit, way).wait_send()

    drain(vec_copy)
    drain(right_copy)
    for unit in (chips - 2, chips - 1):
        pair_copy(unit).wait_send()
    left_across.wait_send()
    left_pair.wait_send()
    left_pass.wait_send()
    for offset in range(1, devices):
        gram_copy(offset).wait_send()
        dots_copy(offset).wait_send()


def ring_step(blocks, cuts, entries, table, left_env, right_env, basis, beta_prev):
    rows, half_slots, depth = left_env.shape
    pairs, cols = basis.shape[2], basis.shape[3]
    slots, chips, quarter = 2 * half_slots, depth // (2 * rows), cols // 2
    basis_count = basis.shape[0]
    count = basis_count * (basis_count + 1) // 2
    square = table.transpose(1, 2, 0, 3).reshape(slots * pairs, slots * pairs)
    bf16, f32 = jnp.bfloat16, jnp.float32
    sem = pltpu.SemaphoreType.DMA
    steps = chips - 1
    hbm = pl.BlockSpec(memory_space=pltpu.HBM)
    vmem = pl.BlockSpec(memory_space=pltpu.VMEM)
    devices = blocks * cuts
    smem = pl.BlockSpec(memory_space=pltpu.SMEM)
    next_vector, values = pl.pallas_call(
        functools.partial(ring_kernel, blocks, cuts, entries),
        name="ring",
        in_specs=[smem, hbm, hbm, vmem, hbm],
        out_specs=[vmem, vmem],
        out_shape=[
            jax.ShapeDtypeStruct((rows, pairs, cols), f32),
            jax.ShapeDtypeStruct((8, 128), f32),
        ],
        scratch_shapes=[
            pltpu.VMEM((chips, pairs, 2 * rows, quarter), bf16),
            pltpu.VMEM((slots, 2 * rows, depth), bf16),
            pltpu.VMEM((chips, 2 * rows, slots * quarter), bf16),
            pltpu.VMEM((2 * pairs * rows, slots * quarter), bf16),
            pltpu.VMEM((slots * pairs * 8, slots * pairs * 8), f32),
            pltpu.VMEM((pairs, slots, rows // 2, quarter // 2), f32),
            pltpu.VMEM((chips + 2, 2, pairs, rows, rows), f32),
            pltpu.VMEM((2, 2, pairs, rows, rows), f32),
            pltpu.VMEM((chips, pairs, rows, rows), f32),
            pltpu.VMEM((3, basis_count, rows, pairs, 128), f32),
            pltpu.VMEM((2, 32, half_slots, depth), bf16),
            pltpu.VMEM((count, pairs, 128), f32),
            pltpu.VMEM((basis_count + 1, pairs, 128), f32),
            pltpu.VMEM((8, 128), f32),
            pltpu.VMEM((devices, 8, 128), f32),
            pltpu.VMEM((1, 128), f32),
            pltpu.VMEM((devices, 1, 128), f32),
            sem((devices,)),
            sem((devices,)),
            sem((devices,)),
            sem((devices,)),
            sem,
            sem((2,)),
            sem((6 + pairs,)),
            sem((6 + pairs,)),
            sem((2, steps, 2)),
            sem((2, steps, 2)),
            sem((2, steps, 2)),
            sem((2, steps, 2)),
            sem((chips,)),
            sem((chips,)),
            sem((chips, 2)),
            sem((chips,)),
            sem((3,)),
        ],
        compiler_params=pltpu.CompilerParams(
            vmem_limit_bytes=65400 * 1024, collective_id=1, has_side_effects=True
        ),
    )(beta_prev.reshape(1), left_env, right_env, square, basis)
    return next_vector, values[0, 0:1], values[0, 1:2]


def ring_fits(blocks, rows, basis_count):
    return blocks == 16 and rows == 128 and basis_count == 8


def gathered_image(cuts, table, left_env, right_env, current):
    row_count, pair_count, col_count = current.shape
    bond_width = table.shape[0]
    full_width = left_env.shape[2]
    me = lax.axis_index("cuts")
    swap = [(0, 1), (1, 0)]

    current = current.transpose(1, 0, 2)
    left_t = left_env.transpose(1, 0, 2)
    right_t = right_env.transpose(1, 0, 2)
    if cuts == 2:
        half = left_t.shape[0]
        theirs = lax.dynamic_slice_in_dim(right_t, (1 - me) * col_count, col_count, 2)
        mine = lax.dynamic_slice_in_dim(right_t, me * col_count, col_count, 2)
        right_k = jnp.concatenate([mine, lax.ppermute(theirs, "cuts", swap)], axis=0)
        left_k = jnp.concatenate([left_t, lax.ppermute(left_t, "cuts", swap)], axis=0)
        turned = jnp.roll(jnp.roll(table, -half, axis=0), -half, axis=1)
        table = jnp.where(me == 0, table, turned)
    else:
        left_k = lax.all_gather(left_t, "cuts", axis=0, tiled=True)
        right_k = lax.all_to_all(right_t, "cuts", split_axis=2, concat_axis=0, tiled=True)
    cur_full = lax.all_gather(current, "blk", axis=1, tiled=True)
    right_full = lax.all_gather(right_k, "blk", axis=1, tiled=True)

    mixed = mixed_left_of(table, left_k, cur_full)
    mixed = mixed.reshape(bond_width, pair_count * row_count, col_count)
    if cuts == 2:
        away = image_part(mixed, right_full, (1 - me) * col_count, col_count)
        away = lax.ppermute(away, "cuts", swap)
        here = image_part(mixed, right_full, me * col_count, col_count)
        image = here + away
    else:
        image = image_part(mixed, right_full, jnp.int32(0), full_width)
        image = lax.psum_scatter(image, "cuts", scatter_dimension=1, tiled=True)
    return image.reshape(pair_count, row_count, col_count).transpose(1, 0, 2)


def on_device(
    blocks, cuts, left_env, right_env, left_core, right_core, slot_bond, krylov_basis, beta_prev
):
    pair_count = left_core.shape[2] * left_core.shape[2]
    basis_count, row_count, _, _ = krylov_basis.shape
    full_width = left_env.shape[2]
    entries = float(full_width * pair_count * full_width)
    table = build_table(left_core, right_core, slot_bond)
    if cuts == 2 and ring_fits(blocks, row_count, basis_count):
        return ring_step(
            blocks, cuts, entries, table, left_env, right_env, krylov_basis, beta_prev
        )
    current = krylov_basis[basis_count - 1].astype(jnp.bfloat16)
    image = gathered_image(cuts, table, left_env, right_env, current)
    gram = gram_of(krylov_basis)

    sums = lax.psum(jnp.concatenate([gram, dots_of(krylov_basis, image)]), ("blk", "cuts"))
    sums = sums / entries
    count = basis_count * (basis_count + 1) // 2
    where = []
    for j in range(basis_count):
        for k in range(basis_count):
            low, high = min(j, k), max(j, k)
            where.append(low * basis_count - low * (low - 1) // 2 + high - low)
    gram_matrix = sums[jnp.array(where)].reshape(basis_count, basis_count)
    inner_prods = sums[count : count + basis_count]
    image_square = sums[count + basis_count]
    last, prior = basis_count - 1, basis_count - 2
    alpha_now = inner_prods[last]
    ortho_coeffs = (
        inner_prods - alpha_now * gram_matrix[:, last] - beta_prev * gram_matrix[:, prior]
    )
    first_square = (
        image_square
        - 2.0 * alpha_now * inner_prods[last]
        - 2.0 * beta_prev * inner_prods[prior]
        + alpha_now * alpha_now * gram_matrix[last, last]
        + 2.0 * alpha_now * beta_prev * gram_matrix[last, prior]
        + beta_prev * beta_prev * gram_matrix[prior, prior]
    )
    square_mean = (
        first_square
        - 2.0 * jnp.sum(ortho_coeffs * ortho_coeffs)
        + jnp.sum(ortho_coeffs[:, None] * gram_matrix * ortho_coeffs[None, :])
    )
    beta_new = jnp.sqrt(square_mean + 1e-06)
    index = jnp.arange(basis_count)
    coefs = (
        ortho_coeffs
        + jnp.where(index == last, alpha_now, 0.0)
        + jnp.where(index == prior, beta_prev, 0.0)
    )
    coefs = jnp.concatenate([coefs, (1.0 / beta_new)[None]])
    next_vector = final_of(coefs, krylov_basis, image)
    return (next_vector, alpha_now[None], beta_new[None])


def solution(mesh):
    in_specs = (
        P("blk", "cuts", None),
        P("blk", "cuts", None),
        P(),
        P(),
        P(),
        P(None, "blk", None, "cuts"),
        P(),
    )
    out_specs = (P("blk", None, "cuts"), P(), P())
    return jax.shard_map(
        functools.partial(on_device, mesh.shape["blk"], mesh.shape["cuts"]),
        mesh=mesh,
        in_specs=in_specs,
        out_specs=out_specs,
        check_vma=False,
    )
```

```python
import functools

import jax
import jax.numpy as jnp
from jax import lax
from jax.experimental import pallas as pl
from jax.experimental.pallas import tpu as pltpu
from jax.sharding import PartitionSpec as P

VMEM_BYTES = 60 * 1024 * 1024


def params():
    return pltpu.CompilerParams(vmem_limit_bytes=VMEM_BYTES)


def tile_of(size, most):
    return most if size % most == 0 else size


def build_table(left_core, right_core, slot_bond):
    bond_width = left_core.shape[0]
    phys_dim = left_core.shape[2]
    chosen = (slot_bond[:, None] == jnp.arange(bond_width, dtype=jnp.int32)[None, :]).astype(
        jnp.float32
    )
    picked = jnp.einsum("kw,wxac->kxac", chosen, left_core, precision=lax.Precision.HIGHEST)
    table = jnp.einsum("kxac,xybd->kyabcd", picked, right_core, precision=lax.Precision.HIGHEST)
    return table.reshape(bond_width, bond_width, phys_dim * phys_dim, phys_dim * phys_dim)


def mix_kernel(mix_ref, left_ref, cur_ref, out_ref, proj):
    slots, rows, depth = left_ref.shape
    pairs = cur_ref.shape[0]
    bonds = out_ref.shape[0]
    cols = cur_ref.shape[2]

    @pl.loop(0, pairs)
    def _(q):
        proj[q] = jnp.dot(
            left_ref[...].reshape(slots * rows, depth),
            cur_ref[q],
            preferred_element_type=jnp.float32,
        ).reshape(slots, rows, cols)

    @pl.loop(0, rows // 16)
    def _(g):
        mixed = []
        for h in range(2):
            at = pl.ds(pl.multiple_of(g * 16 + h * 8, 8), 8)
            stacked = jnp.concatenate(
                [proj[q, k, at, :] for k in range(slots) for q in range(pairs)], axis=0
            )
            mixed.append(
                jnp.dot(
                    mix_ref[...],
                    stacked,
                    precision=lax.Precision.HIGHEST,
                    preferred_element_type=jnp.float32,
                )
            )
        at = pl.ds(pl.multiple_of(g * 16, 16), 16)
        for y in range(bonds):
            for p in range(pairs):
                i = (y * pairs + p) * 8
                out_ref[y, p, at, :] = jnp.concatenate(
                    [m[i : i + 8] for m in mixed], axis=0
                ).astype(out_ref.dtype)


def mixed_left_of(table, left_k, cur_full):
    slots, rows, depth = left_k.shape
    pairs, _, cols = cur_full.shape
    bonds = table.shape[1]
    tb = tile_of(cols, 256)
    square = table.transpose(1, 2, 0, 3).reshape(bonds * pairs, slots * pairs)
    mix = jnp.kron(square, jnp.eye(8, dtype=jnp.float32))
    return pl.pallas_call(
        mix_kernel,
        grid=(cols // tb,),
        in_specs=[
            pl.BlockSpec(mix.shape, lambda i: (0, 0)),
            pl.BlockSpec((slots, rows, depth), lambda i: (0, 0, 0)),
            pl.BlockSpec((pairs, depth, tb), lambda i: (0, 0, i)),
        ],
        out_specs=pl.BlockSpec((bonds, pairs, rows, tb), lambda i: (0, 0, 0, i)),
        out_shape=jax.ShapeDtypeStruct((bonds, pairs, rows, cols), jnp.bfloat16),
        scratch_shapes=[pltpu.VMEM((pairs, slots, rows, tb), jnp.float32)],
        compiler_params=params(),
        cost_estimate=pl.CostEstimate(
            flops=2 * slots * rows * depth * pairs * cols,
            bytes_accessed=2 * (left_k.size + cur_full.size + bonds * pairs * rows * cols),
            transcendentals=0,
        ),
    )(mix, left_k, cur_full)


def image_kernel(start_ref, mixed_ref, right_ref, out_ref):
    bonds = mixed_ref.shape[0]
    out_ref[...] = jnp.zeros_like(out_ref)

    @pl.loop(0, bonds)
    def _(y):
        out_ref[...] += lax.dot_general(
            mixed_ref[y],
            right_ref[y],
            (((1,), (1,)), ((), ())),
            preferred_element_type=jnp.float32,
        )


def image_part(mixed, right_full, start, count):
    bonds, lines, cols = mixed.shape
    tb = tile_of(count, 256)
    return pl.pallas_call(
        image_kernel,
        grid_spec=pltpu.PrefetchScalarGridSpec(
            num_scalar_prefetch=1,
            grid=(count // tb,),
            in_specs=[
                pl.BlockSpec((bonds, lines, cols), lambda i, s: (0, 0, 0)),
                pl.BlockSpec((bonds, tb, cols), lambda i, s: (0, s[0] + i, 0)),
            ],
            out_specs=pl.BlockSpec((lines, tb), lambda i, s: (0, i)),
        ),
        out_shape=jax.ShapeDtypeStruct((lines, count), jnp.float32),
        compiler_params=params(),
        cost_estimate=pl.CostEstimate(
            flops=2 * bonds * lines * cols * count,
            bytes_accessed=2 * (mixed.size + bonds * count * cols),
            transcendentals=0,
        ),
    )((start // tb).reshape(1).astype(jnp.int32), mixed, right_full)


def gram_kernel(basis_ref, out_ref):
    basis_count, rows, pairs, cols = basis_ref.shape
    chunk = 4
    lanes = cols // 128

    @pl.when(pl.program_id(0) == 0)
    def _():
        out_ref[...] = jnp.zeros_like(out_ref)

    @pl.loop(0, rows // chunk)
    def _(r):
        for c in range(lanes):
            vecs = [
                basis_ref[j, pl.ds(r * chunk, chunk), :, c * 128 : (c + 1) * 128]
                for j in range(basis_count)
            ]
            i = 0
            for j in range(basis_count):
                for k in range(j, basis_count):
                    out_ref[i] += jnp.sum(vecs[j] * vecs[k], axis=0)
                    i += 1


def gram_of(basis):
    basis_count, rows, pairs, cols = basis.shape
    count = basis_count * (basis_count + 1) // 2
    ta = tile_of(rows, 16)
    sums = pl.pallas_call(
        gram_kernel,
        grid=(rows // ta,),
        in_specs=[pl.BlockSpec((basis_count, ta, pairs, cols), lambda i: (0, i, 0, 0))],
        out_specs=pl.BlockSpec((count, pairs, 128), lambda i: (0, 0, 0)),
        out_shape=jax.ShapeDtypeStruct((count, pairs, 128), jnp.float32),
        compiler_params=params(),
        cost_estimate=pl.CostEstimate(
            flops=2 * count * rows * pairs * cols,
            bytes_accessed=4 * basis.size,
            transcendentals=0,
        ),
    )(basis)
    return jnp.sum(sums, axis=(1, 2))


def dots_kernel(basis_ref, image_ref, out_ref):
    basis_count, rows, pairs, cols = basis_ref.shape

    @pl.when(pl.program_id(0) == 0)
    def _():
        out_ref[...] = jnp.zeros_like(out_ref)

    for c in range(cols // 128):
        at = slice(c * 128, (c + 1) * 128)
        image = image_ref[:, :, at]
        for j in range(basis_count):
            out_ref[j] += jnp.sum(basis_ref[j, :, :, at] * image, axis=0)
        out_ref[basis_count] += jnp.sum(image * image, axis=0)


def dots_of(basis, image):
    basis_count, rows, pairs, cols = basis.shape
    ta = tile_of(rows, 16)
    sums = pl.pallas_call(
        dots_kernel,
        grid=(rows // ta,),
        in_specs=[
            pl.BlockSpec((basis_count, ta, pairs, cols), lambda i: (0, i, 0, 0)),
            pl.BlockSpec((ta, pairs, cols), lambda i: (i, 0, 0)),
        ],
        out_specs=pl.BlockSpec((basis_count + 1, pairs, 128), lambda i: (0, 0, 0)),
        out_shape=jax.ShapeDtypeStruct((basis_count + 1, pairs, 128), jnp.float32),
        compiler_params=params(),
    )(basis, image)
    return jnp.sum(sums, axis=(1, 2))


def final_kernel(coef_ref, basis_ref, image_ref, out_ref):
    basis_count = basis_ref.shape[0]
    total = image_ref[...]
    for j in range(basis_count):
        total = total - coef_ref[j] * basis_ref[j]
    out_ref[...] = total * coef_ref[basis_count]


def final_of(coefs, basis, image):
    basis_count, rows, pairs, cols = basis.shape
    ta = tile_of(rows, 16)
    return pl.pallas_call(
        final_kernel,
        grid=(rows // ta,),
        in_specs=[
            pl.BlockSpec(memory_space=pltpu.SMEM),
            pl.BlockSpec((basis_count, ta, pairs, cols), lambda i: (0, i, 0, 0)),
            pl.BlockSpec((ta, pairs, cols), lambda i: (i, 0, 0)),
        ],
        out_specs=pl.BlockSpec((ta, pairs, cols), lambda i: (i, 0, 0)),
        out_shape=jax.ShapeDtypeStruct((rows, pairs, cols), jnp.float32),
        compiler_params=params(),
    )(coefs, basis, image)


MESH = pl.DeviceIdType.MESH


def ring_kernel(
    blocks, cuts, entries,
    beta_ref, left_ref, right_ref, square_ref, basis_ref,
    next_ref, values_ref,
    vec, left, right, mixed, mix_ref, proj, parts, pair_in, cut_in, stream, raw,
    gram_ref, dots_ref, gram_tile, gram_inbox, dots_tile, dots_inbox,
    gram_send, gram_recv, dots_send, dots_recv,
    own_sem, raw_sem, pre_send, pre_recv, vec_send, vec_recv, right_send, right_recv,
    pair_send, pair_recv, cut_send, cut_recv, stream_sem,
):
    chips, pairs, chip_rows, quarter = vec.shape
    slots, _, depth = left.shape
    rows, half_slots, _ = left_ref.shape
    span = half_slots * quarter
    last = chips - 1
    polls = 2 * last
    row_tile, col_tile = proj.shape[2], proj.shape[3]
    col_tiles = quarter // col_tile
    mix_units = (chip_rows // row_tile) * col_tiles
    basis_count = basis_ref.shape[0]
    lanes = stream.shape[4]
    pieces = basis_ref.shape[3] // lanes
    half = chips // 2

    blk = lax.axis_index("blk")
    cut = lax.axis_index("cuts")
    core = lax.rem(blk, 2)
    chip = blk // 2
    side = lax.rem(chip, 2)
    place = (1 - side) * (chip // 2) + side * (last - chip // 2)

    def chip_at(index):
        index = lax.rem(index + 2 * chips, chips)
        far = index // half
        return (1 - far) * 2 * index + far * (2 * (last - index) + 1)

    after = (2 * chip_at(place + 1) + core, cut)
    before = (2 * chip_at(place - 1) + core, cut)
    onward = (after, before)
    partner = (2 * chip + 1 - core, cut)
    across = (blk, 1 - cut)
    corner = (2 * chip + 1 - core, 1 - cut)

    def remote(src, dst, send, recv, device):
        return pltpu.make_async_remote_copy(
            src_ref=src, dst_ref=dst, send_sem=send, recv_sem=recv,
            device_id=device, device_id_type=MESH,
        )

    turn = last - 2

    def off_place(way, off):
        return chip_at(place - off) if way == 0 else chip_at(place + off)

    def side_of(way, late):
        return late + way * (1 - 2 * late)

    def vec_copy(way, step, sub, at):
        view = vec.at[at, pl.ds(way * (pairs // 2), pairs // 2), pl.ds(sub * rows, rows), :]
        return remote(
            view, view, vec_send.at[way, step, sub], vec_recv.at[way, step, sub], onward[way]
        )

    def right_copy(way, step, sub, at):
        lines = pl.ds(pl.multiple_of(side_of(way, step // turn) * rows, rows), rows)
        view = right.at[at, lines, pl.ds(sub * span, span)]
        return remote(
            view, view, right_send.at[way, step, sub], right_recv.at[way, step, sub], onward[way]
        )

    def poll(copy_of, index, bend):
        step, sub = index // 2, lax.rem(index + core, 2)
        for way in range(2):
            at = off_place(way, step + 1 - bend * (step // bend))
            copy_of(way, step, sub, at).wait_recv()
            bent = (step + 1) // bend - step // bend

            @pl.when(step < last - 1)
            def _():
                copy_of(way, step + 1, sub, at + bent * (chip - at)).start()

    def drain(copy_of):
        @pl.loop(0, polls)
        def _(index):
            for way in range(2):
                copy_of(way, index // 2, lax.rem(index, 2), chip).wait_send()

    mine = pl.ds(core * rows, rows)
    left_view = left.at[pl.ds(cut * half_slots, half_slots), mine, :]
    left_other = left.at[pl.ds((1 - cut) * half_slots, half_slots), mine, :]
    right_view = right.at[chip, mine, pl.ds(cut * span, span)]
    vec_load = pltpu.make_async_copy(basis_ref.at[basis_count - 1], next_ref, own_sem)
    vec_load.start()
    raw_rows = raw.shape[1]
    raw_units = rows // raw_rows

    def raw_copy(unit):
        source = right_ref if unit < raw_units else left_ref
        at = pl.ds((unit % raw_units) * raw_rows, raw_rows)
        return pltpu.make_async_copy(source.at[at], raw.at[unit % 2], raw_sem.at[unit % 2])

    raw_copy(0).start()
    raw_copy(1).start()

    def stream_copy(piece, slot):
        return pltpu.make_async_copy(
            basis_ref.at[:, :, :, pl.ds(pl.multiple_of(piece * lanes, lanes), lanes)],
            stream.at[slot],
            stream_sem.at[slot],
        )

    devices = blocks * cuts
    me = blk * cuts + cut

    def place_of(offset):
        device = lax.rem(me + offset, devices)
        return (device // cuts, lax.rem(device, cuts))

    barrier = pltpu.get_barrier_semaphore()
    for offset in range(1, devices):
        pl.semaphore_signal(barrier, inc=1, device_id=place_of(offset), device_id_type=MESH)

    vec_load.wait()
    for unit in range(rows // 16):
        at = slice(unit * 16, (unit + 1) * 16)
        to = pl.ds(pl.multiple_of(core * rows + unit * 16, 16), 16)
        for whose in range(2):
            owner = (core + whose) % 2
            cols = pl.ds(pl.multiple_of(owner * quarter, quarter), quarter)
            turned = jnp.swapaxes(next_ref[at, :, cols].astype(vec.dtype), 0, 1)
            if whose == 0:
                vec[chip, :, to, :] = turned
            else:
                for q in range(pairs):
                    mixed[at, q * quarter : (q + 1) * quarter] = turned[q]

    pl.semaphore_wait(barrier, devices - 1)

    vec_pre = [
        remote(
            mixed.at[pl.ds(0, rows), pl.ds(q * quarter, quarter)], vec.at[chip, q, mine, :],
            pre_send.at[6 + q], pre_recv.at[6 + q], partner,
        )
        for q in range(pairs)
    ]
    for copy in vec_pre:
        copy.start()
    for way in range(2):
        vec_copy(way, 0, core, chip).start()

    for unit in range(2 * raw_units):
        raw_copy(unit).wait()
        turned = jnp.swapaxes(raw[unit % 2], 0, 1)
        start = (unit % raw_units) * raw_rows
        to = pl.ds(pl.multiple_of(core * rows + start, raw_rows), raw_rows)
        if unit < raw_units:
            own = pl.ds(pl.multiple_of((2 * cut + core) * quarter, quarter), quarter)
            owned = jnp.swapaxes(raw[unit % 2, :, :, own], 0, 1)
            for slot in range(half_slots):
                cols = pl.ds(pl.multiple_of(cut * span + slot * quarter, quarter), quarter)
                right[chip, to, cols] = owned[slot]
                for e in range(4):
                    at = slice((1 + e) * rows + start, (1 + e) * rows + start + raw_rows)
                    mixed[at, slot * quarter : (slot + 1) * quarter] = turned[
                        slot, :, e * quarter : (e + 1) * quarter
                    ]
        else:
            left[pl.ds(cut * half_slots, half_slots), to, :] = turned
        if unit + 2 < 2 * raw_units:
            raw_copy(unit + 2).start()

    def right_part(to_cut, to_core):
        first_row = pl.multiple_of((1 + 2 * to_cut + to_core) * rows, rows)
        return mixed.at[pl.ds(first_row, rows), pl.ds(0, span)]

    for copy in vec_pre:
        copy.wait_recv()
    for way in range(2):
        vec_copy(way, 0, 1 - core, chip).start()

    right_pre = (
        remote(
            right_part(1 - cut, core), right_view, pre_send.at[2], pre_recv.at[2], across
        ),
        remote(
            right_part(1 - cut, 1 - core), right_view, pre_send.at[4], pre_recv.at[4], corner
        ),
        remote(
            right_part(cut, 1 - core), right_view, pre_send.at[5], pre_recv.at[5], partner
        ),
    )
    for copy in right_pre:
        copy.start()
    left_across = remote(left_view, left_view, pre_send.at[0], pre_recv.at[0], across)
    left_across.start()
    left_pair = remote(left_view, left_view, pre_send.at[1], pre_recv.at[1], partner)
    left_pair.start()
    stream_copy(0, 0).start()
    gram_ref[...] = jnp.zeros_like(gram_ref)
    dots_ref[...] = jnp.zeros_like(dots_ref)

    wide = lax.broadcasted_iota(jnp.int32, (mix_ref.shape[0], slots * pairs), 0)
    thin = lax.broadcasted_iota(jnp.int32, (mix_ref.shape[0], slots * pairs), 1)
    stretch = (wide // 8 == thin).astype(jnp.float32)
    tall = jnp.dot(
        stretch, square_ref[...],
        precision=lax.Precision.HIGHEST, preferred_element_type=jnp.float32,
    )
    full = lax.dot_general(
        tall, stretch, (((1,), (1,)), ((), ())),
        precision=lax.Precision.HIGHEST, preferred_element_type=jnp.float32,
    )
    row = lax.broadcasted_iota(jnp.int32, mix_ref.shape, 0)
    lane = lax.broadcasted_iota(jnp.int32, mix_ref.shape, 1)
    mix_ref[...] = jnp.where(lax.rem(row, 8) == lax.rem(lane, 8), full, 0.0)

    def gram_unit(unit):
        slot = lax.rem(unit, 2)
        stream_copy(unit, slot).wait()

        @pl.when(unit + 1 < pieces)
        def _():
            stream_copy(unit + 1, 1 - slot).start()

        chunk = 4

        @pl.loop(0, rows // chunk)
        def _(r):
            vecs = [stream[slot, j, pl.ds(r * chunk, chunk), :, :] for j in range(basis_count)]
            i = 0
            for j in range(basis_count):
                for k in range(j, basis_count):
                    gram_ref[i] += jnp.sum(vecs[j] * vecs[k], axis=0)
                    i += 1

    @pl.loop(0, polls - 2)
    def _(index):
        poll(vec_copy, index, last)

        @pl.when(index < pieces)
        def _():
            gram_unit(index)

    for copy in right_pre:
        copy.wait_recv()
    for sub in range(2):
        for way in range(2):
            right_copy(way, 0, lax.rem(sub + core, 2), chip).start()

    left_across.wait_recv()
    left_pass = remote(left_other, left_other, pre_send.at[3], pre_recv.at[3], partner)
    left_pass.start()

    def total_of(x):
        return jnp.sum(jnp.sum(x, axis=0, keepdims=True), axis=1, keepdims=True)

    row = lax.broadcasted_iota(jnp.int32, gram_tile.shape, 0)
    lane = lax.broadcasted_iota(jnp.int32, gram_tile.shape, 1)
    found = jnp.zeros(gram_tile.shape, jnp.float32)
    i = 0
    for j in range(basis_count):
        for k in range(j, basis_count):
            here = ((row == j) & (lane == k)) | ((row == k) & (lane == j))
            found = jnp.where(here, total_of(gram_ref[i]), found)
            i += 1
    gram_tile[...] = found
    gram_inbox[me] = found

    def gram_copy(offset):
        return remote(
            gram_tile, gram_inbox.at[me],
            gram_send.at[offset], gram_recv.at[offset], place_of(offset),
        )

    def dots_copy(offset):
        return remote(
            dots_tile, dots_inbox.at[me],
            dots_send.at[offset], dots_recv.at[offset], place_of(offset),
        )

    for offset in range(1, devices):
        gram_copy(offset).start()

    @pl.loop(polls - 2, polls)
    def _(index):
        poll(vec_copy, index, last)

    for copy in vec_pre:
        copy.wait_send()
    for copy in right_pre:
        copy.wait_send()
    left_pair.wait_recv()
    left_pass.wait_recv()

    def mix_unit(unit):
        row0 = pl.multiple_of((unit // col_tiles) * row_tile, row_tile)
        col0 = pl.multiple_of(lax.rem(unit, col_tiles) * col_tile, col_tile)

        @pl.loop(0, pairs)
        def _(q):
            proj[q] = jnp.dot(
                left[:, pl.ds(row0, row_tile), :].reshape(slots * row_tile, depth),
                vec[:, q, :, pl.ds(col0, col_tile)].reshape(depth, col_tile),
                preferred_element_type=jnp.float32,
            ).reshape(slots, row_tile, col_tile)

        owner = row0 // rows
        base = owner * (pairs * rows) + row0 - owner * rows

        @pl.loop(0, row_tile // 16)
        def _(g):
            lines = []
            for h in range(2):
                at = pl.ds(pl.multiple_of(g * 16 + h * 8, 8), 8)
                stacked = jnp.concatenate(
                    [proj[q, k, at, :] for k in range(slots) for q in range(pairs)], axis=0
                )
                lines.append(
                    jnp.dot(
                        mix_ref[...],
                        stacked,
                        precision=lax.Precision.HIGHEST,
                        preferred_element_type=jnp.float32,
                    )
                )
            for y in range(slots):
                cols = pl.ds(pl.multiple_of(y * quarter + col0, col_tile), col_tile)
                for p in range(pairs):
                    i = (y * pairs + p) * 8
                    at = pl.ds(pl.multiple_of(base + p * rows + g * 16, 16), 16)
                    mixed[at, cols] = jnp.concatenate(
                        [m[i : i + 8] for m in lines], axis=0
                    ).astype(mixed.dtype)

    lot = pairs * rows

    def pair_copy(unit):
        return remote(
            parts.at[chips + lax.rem(unit, 2)], pair_in.at[lax.rem(unit, 2)],
            pair_send.at[unit], pair_recv.at[unit], partner,
        )

    def late_of(unit):
        return unit // (turn + 1)

    def block_of(unit, way):
        return off_place(way, unit - turn * late_of(unit))

    def home_of(unit, way):
        at = block_of(unit, way)
        return at // half, lax.rem(at, half) * 2 + side_of(way, late_of(unit))

    def cut_copy(unit, way):
        _, piece = home_of(unit, way)
        return remote(
            parts.at[unit, way], cut_in.at[piece],
            cut_send.at[unit, way], cut_recv.at[piece], across,
        )

    def lines_of(unit, way):
        return pl.ds(pl.multiple_of(side_of(way, late_of(unit)) * rows, rows), rows)

    def image_half(unit, sub):
        @pl.when((unit >= 2) & (sub == 0))
        def _():
            pair_copy(unit - 2).wait_send()

        at = lax.rem(sub + core, 2)
        cols = pl.ds(pl.multiple_of(at * span, span), span)

        @pl.loop(0, 2)
        def _(k):
            owner = lax.rem(core + 1 + k, 2)
            to = (1 - k) * (chips + lax.rem(unit, 2)) + k * unit
            lines = jnp.concatenate(
                [
                    right[block_of(unit, way), lines_of(unit, way), cols]
                    for way in range(2)
                ],
                axis=0,
            )
            out = lax.dot_general(
                mixed[pl.ds(pl.multiple_of(owner * lot, lot), lot), cols],
                lines,
                (((1,), (1,)), ((), ())),
                preferred_element_type=jnp.float32,
            )

            @pl.when(sub == 0)
            def _():
                for way in range(2):
                    piece = out[:, way * rows : (way + 1) * rows]
                    parts[to, way] = piece.reshape(pairs, rows, rows)

            @pl.when(sub == 1)
            def _():
                for way in range(2):
                    piece = out[:, way * rows : (way + 1) * rows]
                    parts[to, way] += piece.reshape(pairs, rows, rows)

            @pl.when((sub == 1) & (k == 0))
            def _():
                pair_copy(unit).start()

    def join_unit(unit):
        pair_copy(unit).wait_recv()
        for way in range(2):
            parts[unit, way] += pair_in[lax.rem(unit, 2), way]
            home, piece = home_of(unit, way)

            @pl.when(home != cut)
            def _():
                cut_copy(unit, way).start()

    def fetch_unit(unit):
        for way in range(2):
            home, piece = home_of(unit, way)

            @pl.when(home == cut)
            def _():
                stream_copy(piece, way).start()

    def settle_unit(unit):
        for way in range(2):
            home, piece = home_of(unit, way)

            @pl.when(home == cut)
            def _():
                cut_copy(unit, way).wait_recv()
                cols = pl.ds(pl.multiple_of(piece * rows, rows), rows)
                whole = parts[unit, way] + cut_in[piece]
                for p in range(pairs):
                    next_ref[:, p, cols] = whole[p]
                stream_copy(piece, way).wait()

                def add(step, sums):
                    sums = list(sums)
                    for line in range(16):
                        at = step * 16 + line
                        image = next_ref[at, :, cols]
                        for j in range(basis_count):
                            sums[j] += stream[way, j, at, :, :] * image
                        sums[basis_count] += image * image
                    return tuple(sums)

                sums = lax.fori_loop(
                    0, rows // 16, add, tuple(dots_ref[j] for j in range(basis_count + 1))
                )
                for j in range(basis_count + 1):
                    dots_ref[j] = sums[j]

    first = polls - chips

    @pl.loop(0, first)
    def _(index):
        poll(right_copy, index, turn)

        @pl.loop((mix_units * index) // first, (mix_units * (index + 1)) // first)
        def _(unit):
            mix_unit(unit)

    def ready(index):
        return jnp.minimum(2 * (index - first) + 3, index + 3)

    @pl.loop(first, polls)
    def _(index):
        poll(right_copy, index, turn)

        @pl.loop(jnp.where(index == first, 0, ready(index - 1)), ready(index))
        def _(piece):
            unit, sub = piece // 2, lax.rem(piece, 2)
            image_half(unit, sub)

            @pl.when(sub == 1)
            def _():
                join_unit(unit)

            @pl.when((sub == 1) & (unit == 1))
            def _():
                fetch_unit(0)

            @pl.when((sub == 1) & (unit > 1) & (unit < last))
            def _():
                settle_unit(unit - 2)
                fetch_unit(unit - 1)

    slots_held = stream.shape[0]
    for piece in range(slots_held - 2):
        stream_copy(piece, 2 + piece).start()
    settle_unit(last - 2)
    fetch_unit(last - 1)
    settle_unit(last - 1)
    fetch_unit(last)
    for offset in range(1, devices):
        gram_copy(offset).wait_recv()
    gram = gram_inbox[0]
    for d in range(1, devices):
        gram = gram + gram_inbox[d]
    gram = gram / entries
    settle_unit(last)
    for slot in range(2):
        stream_copy(slots_held - 2 + slot, slot).start()

    spot = lax.broadcasted_iota(jnp.int32, dots_tile.shape, 1)
    found = jnp.zeros(dots_tile.shape, jnp.float32)
    for j in range(basis_count + 1):
        found = jnp.where(spot == j, total_of(dots_ref[j]), found)
    dots_tile[...] = found
    dots_inbox[me] = found
    for offset in range(1, devices):
        dots_copy(offset).start()
    for offset in range(1, devices):
        dots_copy(offset).wait_recv()
    along = dots_inbox[0]
    for d in range(1, devices):
        along = along + dots_inbox[d]
    along = along / entries

    n, end, prior = basis_count, basis_count - 1, basis_count - 2
    spread = jnp.broadcast_to(along, gram_tile.shape)
    down = jnp.sum(jnp.where(row == lane, spread, 0.0), axis=1, keepdims=True)[0:n]
    square = along[:, n : n + 1]
    along = along[:, 0:n]
    gram = gram[0:n, 0:n]
    alpha = down[end : end + 1]
    beta = jnp.full((1, 1), beta_ref[0], jnp.float32)
    ortho = down - alpha * gram[:, end : end + 1] - beta * gram[:, prior : prior + 1]
    ortho_row = along - alpha * gram[end : end + 1, :] - beta * gram[prior : prior + 1, :]
    first = (
        square
        - 2.0 * alpha * alpha
        - 2.0 * beta * down[prior : prior + 1]
        + alpha * alpha * gram[end : end + 1, end : end + 1]
        + 2.0 * alpha * beta * gram[end : end + 1, prior : prior + 1]
        + beta * beta * gram[prior : prior + 1, prior : prior + 1]
    )
    bent = jnp.sum(ortho * gram, axis=0, keepdims=True) * ortho_row
    mean = (
        first
        - 2.0 * jnp.sum(ortho * ortho, axis=0, keepdims=True)
        + jnp.sum(bent, axis=1, keepdims=True)
    )
    beta_new = jnp.sqrt(mean + 1e-06)
    values_ref[...] = jnp.where(
        (row == 0) & (lane == 0), alpha, jnp.where((row == 0) & (lane == 1), beta_new, 0.0)
    )
    index = lax.broadcasted_iota(jnp.int32, ortho.shape, 0)
    coefs = ortho + jnp.where(index == end, alpha, 0.0) + jnp.where(index == prior, beta, 0.0)
    coefs = [jnp.broadcast_to(coefs[j : j + 1], (pairs, lanes)) for j in range(n)]
    scale = jnp.broadcast_to(1.0 / beta_new, (pairs, lanes))

    @pl.loop(0, pieces)
    def _(piece):
        slot = lax.rem(piece + 2, slots_held)
        stream_copy(piece, slot).wait()
        cols = pl.ds(pl.multiple_of(piece * lanes, lanes), lanes)

        @pl.loop(0, rows // 32)
        def _(step):
            for line in range(32):
                at = step * 32 + line
                value = next_ref[at, :, cols]
                for j in range(n):
                    value = value - coefs[j] * stream[slot, j, at, :, :]
                next_ref[at, :, cols] = value * scale

        @pl.when(piece + slots_held < pieces)
        def _():
            stream_copy(piece + slots_held, slot).start()

    @pl.loop(0, chips)
    def _(unit):
        for way in range(2):
            home, _ = home_of(unit, way)

            @pl.when(home != cut)
            def _():
                cut_copy(unit, way).wait_send()

    drain(vec_copy)
    drain(right_copy)
    for unit in (chips - 2, chips - 1):
        pair_copy(unit).wait_send()
    left_across.wait_send()
    left_pair.wait_send()
    left_pass.wait_send()
    for offset in range(1, devices):
        gram_copy(offset).wait_send()
        dots_copy(offset).wait_send()


def ring_step(blocks, cuts, entries, table, left_env, right_env, basis, beta_prev):
    rows, half_slots, depth = left_env.shape
    pairs, cols = basis.shape[2], basis.shape[3]
    slots, chips, quarter = 2 * half_slots, depth // (2 * rows), cols // 2
    basis_count = basis.shape[0]
    count = basis_count * (basis_count + 1) // 2
    square = table.transpose(1, 2, 0, 3).reshape(slots * pairs, slots * pairs)
    bf16, f32 = jnp.bfloat16, jnp.float32
    sem = pltpu.SemaphoreType.DMA
    steps = chips - 1
    hbm = pl.BlockSpec(memory_space=pltpu.HBM)
    vmem = pl.BlockSpec(memory_space=pltpu.VMEM)
    devices = blocks * cuts
    smem = pl.BlockSpec(memory_space=pltpu.SMEM)
    next_vector, values = pl.pallas_call(
        functools.partial(ring_kernel, blocks, cuts, entries),
        name="ring",
        in_specs=[smem, hbm, hbm, vmem, hbm],
        out_specs=[vmem, vmem],
        out_shape=[
            jax.ShapeDtypeStruct((rows, pairs, cols), f32),
            jax.ShapeDtypeStruct((8, 128), f32),
        ],
        scratch_shapes=[
            pltpu.VMEM((chips, pairs, 2 * rows, quarter), bf16),
            pltpu.VMEM((slots, 2 * rows, depth), bf16),
            pltpu.VMEM((chips, 2 * rows, slots * quarter), bf16),
            pltpu.VMEM((2 * pairs * rows, slots * quarter), bf16),
            pltpu.VMEM((slots * pairs * 8, slots * pairs * 8), f32),
            pltpu.VMEM((pairs, slots, rows // 2, quarter // 2), f32),
            pltpu.VMEM((chips + 2, 2, pairs, rows, rows), f32),
            pltpu.VMEM((2, 2, pairs, rows, rows), f32),
            pltpu.VMEM((chips, pairs, rows, rows), f32),
            pltpu.VMEM((4, basis_count, rows, pairs, 128), f32),
            pltpu.VMEM((2, 32, half_slots, depth), bf16),
            pltpu.VMEM((count, pairs, 128), f32),
            pltpu.VMEM((basis_count + 1, pairs, 128), f32),
            pltpu.VMEM((8, 128), f32),
            pltpu.VMEM((devices, 8, 128), f32),
            pltpu.VMEM((1, 128), f32),
            pltpu.VMEM((devices, 1, 128), f32),
            sem((devices,)),
            sem((devices,)),
            sem((devices,)),
            sem((devices,)),
            sem,
            sem((2,)),
            sem((6 + pairs,)),
            sem((6 + pairs,)),
            sem((2, steps, 2)),
            sem((2, steps, 2)),
            sem((2, steps, 2)),
            sem((2, steps, 2)),
            sem((chips,)),
            sem((chips,)),
            sem((chips, 2)),
            sem((chips,)),
            sem((4,)),
        ],
        compiler_params=pltpu.CompilerParams(
            vmem_limit_bytes=65400 * 1024, collective_id=1, has_side_effects=True
        ),
    )(beta_prev.reshape(1), left_env, right_env, square, basis)
    return next_vector, values[0, 0:1], values[0, 1:2]


def ring_fits(blocks, rows, basis_count):
    return blocks == 16 and rows == 128 and basis_count == 8


def gathered_image(cuts, table, left_env, right_env, current):
    row_count, pair_count, col_count = current.shape
    bond_width = table.shape[0]
    full_width = left_env.shape[2]
    me = lax.axis_index("cuts")
    swap = [(0, 1), (1, 0)]

    current = current.transpose(1, 0, 2)
    left_t = left_env.transpose(1, 0, 2)
    right_t = right_env.transpose(1, 0, 2)
    if cuts == 2:
        half = left_t.shape[0]
        theirs = lax.dynamic_slice_in_dim(right_t, (1 - me) * col_count, col_count, 2)
        mine = lax.dynamic_slice_in_dim(right_t, me * col_count, col_count, 2)
        right_k = jnp.concatenate([mine, lax.ppermute(theirs, "cuts", swap)], axis=0)
        left_k = jnp.concatenate([left_t, lax.ppermute(left_t, "cuts", swap)], axis=0)
        turned = jnp.roll(jnp.roll(table, -half, axis=0), -half, axis=1)
        table = jnp.where(me == 0, table, turned)
    else:
        left_k = lax.all_gather(left_t, "cuts", axis=0, tiled=True)
        right_k = lax.all_to_all(right_t, "cuts", split_axis=2, concat_axis=0, tiled=True)
    cur_full = lax.all_gather(current, "blk", axis=1, tiled=True)
    right_full = lax.all_gather(right_k, "blk", axis=1, tiled=True)

    mixed = mixed_left_of(table, left_k, cur_full)
    mixed = mixed.reshape(bond_width, pair_count * row_count, col_count)
    if cuts == 2:
        away = image_part(mixed, right_full, (1 - me) * col_count, col_count)
        away = lax.ppermute(away, "cuts", swap)
        here = image_part(mixed, right_full, me * col_count, col_count)
        image = here + away
    else:
        image = image_part(mixed, right_full, jnp.int32(0), full_width)
        image = lax.psum_scatter(image, "cuts", scatter_dimension=1, tiled=True)
    return image.reshape(pair_count, row_count, col_count).transpose(1, 0, 2)


def on_device(
    blocks, cuts, left_env, right_env, left_core, right_core, slot_bond, krylov_basis, beta_prev
):
    pair_count = left_core.shape[2] * left_core.shape[2]
    basis_count, row_count, _, _ = krylov_basis.shape
    full_width = left_env.shape[2]
    entries = float(full_width * pair_count * full_width)
    table = build_table(left_core, right_core, slot_bond)
    if cuts == 2 and ring_fits(blocks, row_count, basis_count):
        return ring_step(
            blocks, cuts, entries, table, left_env, right_env, krylov_basis, beta_prev
        )
    current = krylov_basis[basis_count - 1].astype(jnp.bfloat16)
    image = gathered_image(cuts, table, left_env, right_env, current)
    gram = gram_of(krylov_basis)

    sums = lax.psum(jnp.concatenate([gram, dots_of(krylov_basis, image)]), ("blk", "cuts"))
    sums = sums / entries
    count = basis_count * (basis_count + 1) // 2
    where = []
    for j in range(basis_count):
        for k in range(basis_count):
            low, high = min(j, k), max(j, k)
            where.append(low * basis_count - low * (low - 1) // 2 + high - low)
    gram_matrix = sums[jnp.array(where)].reshape(basis_count, basis_count)
    inner_prods = sums[count : count + basis_count]
    image_square = sums[count + basis_count]
    last, prior = basis_count - 1, basis_count - 2
    alpha_now = inner_prods[last]
    ortho_coeffs = (
        inner_prods - alpha_now * gram_matrix[:, last] - beta_prev * gram_matrix[:, prior]
    )
    first_square = (
        image_square
        - 2.0 * alpha_now * inner_prods[last]
        - 2.0 * beta_prev * inner_prods[prior]
        + alpha_now * alpha_now * gram_matrix[last, last]
        + 2.0 * alpha_now * beta_prev * gram_matrix[last, prior]
        + beta_prev * beta_prev * gram_matrix[prior, prior]
    )
    square_mean = (
        first_square
        - 2.0 * jnp.sum(ortho_coeffs * ortho_coeffs)
        + jnp.sum(ortho_coeffs[:, None] * gram_matrix * ortho_coeffs[None, :])
    )
    beta_new = jnp.sqrt(square_mean + 1e-06)
    index = jnp.arange(basis_count)
    coefs = (
        ortho_coeffs
        + jnp.where(index == last, alpha_now, 0.0)
        + jnp.where(index == prior, beta_prev, 0.0)
    )
    coefs = jnp.concatenate([coefs, (1.0 / beta_new)[None]])
    next_vector = final_of(coefs, krylov_basis, image)
    return (next_vector, alpha_now[None], beta_new[None])


def solution(mesh):
    in_specs = (
        P("blk", "cuts", None),
        P("blk", "cuts", None),
        P(),
        P(),
        P(),
        P(None, "blk", None, "cuts"),
        P(),
    )
    out_specs = (P("blk", None, "cuts"), P(), P())
    return jax.shard_map(
        functools.partial(on_device, mesh.shape["blk"], mesh.shape["cuts"]),
        mesh=mesh,
        in_specs=in_specs,
        out_specs=out_specs,
        check_vma=False,
    )
```

```python
import functools

import jax
import jax.numpy as jnp
from jax import lax
from jax.experimental import pallas as pl
from jax.experimental.pallas import tpu as pltpu
from jax.sharding import PartitionSpec as P

VMEM_BYTES = 60 * 1024 * 1024


def params():
    return pltpu.CompilerParams(vmem_limit_bytes=VMEM_BYTES)


def tile_of(size, most):
    return most if size % most == 0 else size


def build_table(left_core, right_core, slot_bond):
    bond_width = left_core.shape[0]
    phys_dim = left_core.shape[2]
    chosen = (slot_bond[:, None] == jnp.arange(bond_width, dtype=jnp.int32)[None, :]).astype(
        jnp.float32
    )
    picked = jnp.einsum("kw,wxac->kxac", chosen, left_core, precision=lax.Precision.HIGHEST)
    table = jnp.einsum("kxac,xybd->kyabcd", picked, right_core, precision=lax.Precision.HIGHEST)
    return table.reshape(bond_width, bond_width, phys_dim * phys_dim, phys_dim * phys_dim)


def mix_kernel(mix_ref, left_ref, cur_ref, out_ref, proj):
    slots, rows, depth = left_ref.shape
    pairs = cur_ref.shape[0]
    bonds = out_ref.shape[0]
    cols = cur_ref.shape[2]

    @pl.loop(0, pairs)
    def _(q):
        proj[q] = jnp.dot(
            left_ref[...].reshape(slots * rows, depth),
            cur_ref[q],
            preferred_element_type=jnp.float32,
        ).reshape(slots, rows, cols)

    @pl.loop(0, rows // 16)
    def _(g):
        mixed = []
        for h in range(2):
            at = pl.ds(pl.multiple_of(g * 16 + h * 8, 8), 8)
            stacked = jnp.concatenate(
                [proj[q, k, at, :] for k in range(slots) for q in range(pairs)], axis=0
            )
            mixed.append(
                jnp.dot(
                    mix_ref[...],
                    stacked,
                    precision=lax.Precision.HIGHEST,
                    preferred_element_type=jnp.float32,
                )
            )
        at = pl.ds(pl.multiple_of(g * 16, 16), 16)
        for y in range(bonds):
            for p in range(pairs):
                i = (y * pairs + p) * 8
                out_ref[y, p, at, :] = jnp.concatenate(
                    [m[i : i + 8] for m in mixed], axis=0
                ).astype(out_ref.dtype)


def mixed_left_of(table, left_k, cur_full):
    slots, rows, depth = left_k.shape
    pairs, _, cols = cur_full.shape
    bonds = table.shape[1]
    tb = tile_of(cols, 256)
    square = table.transpose(1, 2, 0, 3).reshape(bonds * pairs, slots * pairs)
    mix = jnp.kron(square, jnp.eye(8, dtype=jnp.float32))
    return pl.pallas_call(
        mix_kernel,
        grid=(cols // tb,),
        in_specs=[
            pl.BlockSpec(mix.shape, lambda i: (0, 0)),
            pl.BlockSpec((slots, rows, depth), lambda i: (0, 0, 0)),
            pl.BlockSpec((pairs, depth, tb), lambda i: (0, 0, i)),
        ],
        out_specs=pl.BlockSpec((bonds, pairs, rows, tb), lambda i: (0, 0, 0, i)),
        out_shape=jax.ShapeDtypeStruct((bonds, pairs, rows, cols), jnp.bfloat16),
        scratch_shapes=[pltpu.VMEM((pairs, slots, rows, tb), jnp.float32)],
        compiler_params=params(),
        cost_estimate=pl.CostEstimate(
            flops=2 * slots * rows * depth * pairs * cols,
            bytes_accessed=2 * (left_k.size + cur_full.size + bonds * pairs * rows * cols),
            transcendentals=0,
        ),
    )(mix, left_k, cur_full)


def image_kernel(start_ref, mixed_ref, right_ref, out_ref):
    bonds = mixed_ref.shape[0]
    out_ref[...] = jnp.zeros_like(out_ref)

    @pl.loop(0, bonds)
    def _(y):
        out_ref[...] += lax.dot_general(
            mixed_ref[y],
            right_ref[y],
            (((1,), (1,)), ((), ())),
            preferred_element_type=jnp.float32,
        )


def image_part(mixed, right_full, start, count):
    bonds, lines, cols = mixed.shape
    tb = tile_of(count, 256)
    return pl.pallas_call(
        image_kernel,
        grid_spec=pltpu.PrefetchScalarGridSpec(
            num_scalar_prefetch=1,
            grid=(count // tb,),
            in_specs=[
                pl.BlockSpec((bonds, lines, cols), lambda i, s: (0, 0, 0)),
                pl.BlockSpec((bonds, tb, cols), lambda i, s: (0, s[0] + i, 0)),
            ],
            out_specs=pl.BlockSpec((lines, tb), lambda i, s: (0, i)),
        ),
        out_shape=jax.ShapeDtypeStruct((lines, count), jnp.float32),
        compiler_params=params(),
        cost_estimate=pl.CostEstimate(
            flops=2 * bonds * lines * cols * count,
            bytes_accessed=2 * (mixed.size + bonds * count * cols),
            transcendentals=0,
        ),
    )((start // tb).reshape(1).astype(jnp.int32), mixed, right_full)


def gram_kernel(basis_ref, out_ref):
    basis_count, rows, pairs, cols = basis_ref.shape
    chunk = 4
    lanes = cols // 128

    @pl.when(pl.program_id(0) == 0)
    def _():
        out_ref[...] = jnp.zeros_like(out_ref)

    @pl.loop(0, rows // chunk)
    def _(r):
        for c in range(lanes):
            vecs = [
                basis_ref[j, pl.ds(r * chunk, chunk), :, c * 128 : (c + 1) * 128]
                for j in range(basis_count)
            ]
            i = 0
            for j in range(basis_count):
                for k in range(j, basis_count):
                    out_ref[i] += jnp.sum(vecs[j] * vecs[k], axis=0)
                    i += 1


def gram_of(basis):
    basis_count, rows, pairs, cols = basis.shape
    count = basis_count * (basis_count + 1) // 2
    ta = tile_of(rows, 16)
    sums = pl.pallas_call(
        gram_kernel,
        grid=(rows // ta,),
        in_specs=[pl.BlockSpec((basis_count, ta, pairs, cols), lambda i: (0, i, 0, 0))],
        out_specs=pl.BlockSpec((count, pairs, 128), lambda i: (0, 0, 0)),
        out_shape=jax.ShapeDtypeStruct((count, pairs, 128), jnp.float32),
        compiler_params=params(),
        cost_estimate=pl.CostEstimate(
            flops=2 * count * rows * pairs * cols,
            bytes_accessed=4 * basis.size,
            transcendentals=0,
        ),
    )(basis)
    return jnp.sum(sums, axis=(1, 2))


def dots_kernel(basis_ref, image_ref, out_ref):
    basis_count, rows, pairs, cols = basis_ref.shape

    @pl.when(pl.program_id(0) == 0)
    def _():
        out_ref[...] = jnp.zeros_like(out_ref)

    for c in range(cols // 128):
        at = slice(c * 128, (c + 1) * 128)
        image = image_ref[:, :, at]
        for j in range(basis_count):
            out_ref[j] += jnp.sum(basis_ref[j, :, :, at] * image, axis=0)
        out_ref[basis_count] += jnp.sum(image * image, axis=0)


def dots_of(basis, image):
    basis_count, rows, pairs, cols = basis.shape
    ta = tile_of(rows, 16)
    sums = pl.pallas_call(
        dots_kernel,
        grid=(rows // ta,),
        in_specs=[
            pl.BlockSpec((basis_count, ta, pairs, cols), lambda i: (0, i, 0, 0)),
            pl.BlockSpec((ta, pairs, cols), lambda i: (i, 0, 0)),
        ],
        out_specs=pl.BlockSpec((basis_count + 1, pairs, 128), lambda i: (0, 0, 0)),
        out_shape=jax.ShapeDtypeStruct((basis_count + 1, pairs, 128), jnp.float32),
        compiler_params=params(),
    )(basis, image)
    return jnp.sum(sums, axis=(1, 2))


def final_kernel(coef_ref, basis_ref, image_ref, out_ref):
    basis_count = basis_ref.shape[0]
    total = image_ref[...]
    for j in range(basis_count):
        total = total - coef_ref[j] * basis_ref[j]
    out_ref[...] = total * coef_ref[basis_count]


def final_of(coefs, basis, image):
    basis_count, rows, pairs, cols = basis.shape
    ta = tile_of(rows, 16)
    return pl.pallas_call(
        final_kernel,
        grid=(rows // ta,),
        in_specs=[
            pl.BlockSpec(memory_space=pltpu.SMEM),
            pl.BlockSpec((basis_count, ta, pairs, cols), lambda i: (0, i, 0, 0)),
            pl.BlockSpec((ta, pairs, cols), lambda i: (i, 0, 0)),
        ],
        out_specs=pl.BlockSpec((ta, pairs, cols), lambda i: (i, 0, 0)),
        out_shape=jax.ShapeDtypeStruct((rows, pairs, cols), jnp.float32),
        compiler_params=params(),
    )(coefs, basis, image)


MESH = pl.DeviceIdType.MESH


def ring_kernel(
    blocks, cuts, entries,
    beta_ref, left_ref, right_ref, square_ref, basis_ref,
    next_ref, values_ref,
    vec, left, right, mixed, mix_ref, proj, parts, pair_in, cut_in, stream, raw,
    gram_ref, dots_ref, gram_tile, gram_inbox, dots_tile, dots_inbox,
    gram_send, gram_recv, dots_send, dots_recv,
    own_sem, raw_sem, pre_send, pre_recv, vec_send, vec_recv, right_send, right_recv,
    pair_send, pair_recv, cut_send, cut_recv, stream_sem,
):
    chips, pairs, chip_rows, quarter = vec.shape
    slots, _, depth = left.shape
    rows, half_slots, _ = left_ref.shape
    span = half_slots * quarter
    last = chips - 1
    polls = 2 * last
    row_tile, col_tile = proj.shape[2], proj.shape[3]
    col_tiles = quarter // col_tile
    mix_units = (chip_rows // row_tile) * col_tiles
    basis_count = basis_ref.shape[0]
    lanes = stream.shape[4]
    pieces = basis_ref.shape[3] // lanes
    half = chips // 2

    blk = lax.axis_index("blk")
    cut = lax.axis_index("cuts")
    core = lax.rem(blk, 2)
    chip = blk // 2
    side = lax.rem(chip, 2)
    place = (1 - side) * (chip // 2) + side * (last - chip // 2)

    def chip_at(index):
        index = lax.rem(index + 2 * chips, chips)
        far = index // half
        return (1 - far) * 2 * index + far * (2 * (last - index) + 1)

    after = (2 * chip_at(place + 1) + core, cut)
    before = (2 * chip_at(place - 1) + core, cut)
    onward = (after, before)
    partner = (2 * chip + 1 - core, cut)
    across = (blk, 1 - cut)
    corner = (2 * chip + 1 - core, 1 - cut)

    def remote(src, dst, send, recv, device):
        return pltpu.make_async_remote_copy(
            src_ref=src, dst_ref=dst, send_sem=send, recv_sem=recv,
            device_id=device, device_id_type=MESH,
        )

    turn = last - 2

    def off_place(way, off):
        return chip_at(place - off) if way == 0 else chip_at(place + off)

    def side_of(way, late):
        return late + way * (1 - 2 * late)

    def vec_copy(way, step, sub, at):
        view = vec.at[at, pl.ds(way * (pairs // 2), pairs // 2), pl.ds(sub * rows, rows), :]
        return remote(
            view, view, vec_send.at[way, step, sub], vec_recv.at[way, step, sub], onward[way]
        )

    def right_copy(way, step, sub, at):
        lines = pl.ds(pl.multiple_of(side_of(way, step // turn) * rows, rows), rows)
        view = right.at[at, lines, pl.ds(sub * span, span)]
        return remote(
            view, view, right_send.at[way, step, sub], right_recv.at[way, step, sub], onward[way]
        )

    def poll(copy_of, index, bend):
        step, sub = index // 2, lax.rem(index + core, 2)
        for way in range(2):
            at = off_place(way, step + 1 - bend * (step // bend))
            copy_of(way, step, sub, at).wait_recv()
            bent = (step + 1) // bend - step // bend

            @pl.when(step < last - 1)
            def _():
                copy_of(way, step + 1, sub, at + bent * (chip - at)).start()

    def drain(copy_of):
        @pl.loop(0, polls)
        def _(index):
            for way in range(2):
                copy_of(way, index // 2, lax.rem(index, 2), chip).wait_send()

    mine = pl.ds(core * rows, rows)
    left_view = left.at[pl.ds(cut * half_slots, half_slots), mine, :]
    left_other = left.at[pl.ds((1 - cut) * half_slots, half_slots), mine, :]
    right_view = right.at[chip, mine, pl.ds(cut * span, span)]
    vec_load = []
    for part in range(2):
        at = pl.ds(part * (rows // 2), rows // 2)
        vec_load.append(
            pltpu.make_async_copy(
                basis_ref.at[basis_count - 1, at], next_ref.at[at], own_sem.at[part]
            )
        )
        vec_load[part].start()
    raw_rows = raw.shape[1]
    raw_units = rows // raw_rows

    def raw_copy(unit):
        source = right_ref if unit < raw_units else left_ref
        at = pl.ds((unit % raw_units) * raw_rows, raw_rows)
        return pltpu.make_async_copy(source.at[at], raw.at[unit % 2], raw_sem.at[unit % 2])

    raw_copy(0).start()
    raw_copy(1).start()

    def stream_copy(piece, slot):
        return pltpu.make_async_copy(
            basis_ref.at[:, :, :, pl.ds(pl.multiple_of(piece * lanes, lanes), lanes)],
            stream.at[slot],
            stream_sem.at[slot],
        )

    devices = blocks * cuts
    me = blk * cuts + cut

    def place_of(offset):
        device = lax.rem(me + offset, devices)
        return (device // cuts, lax.rem(device, cuts))

    barrier = pltpu.get_barrier_semaphore()
    friends = (after, before, partner, across, corner)
    for friend in friends:
        pl.semaphore_signal(barrier, inc=1, device_id=friend, device_id_type=MESH)

    def turned_vec(unit, owner):
        at = slice(unit * 16, (unit + 1) * 16)
        cols = pl.ds(pl.multiple_of(owner * quarter, quarter), quarter)
        return jnp.swapaxes(next_ref[at, :, cols].astype(vec.dtype), 0, 1)

    for unit in range(rows // 16):
        if unit % (rows // 32) == 0:
            vec_load[unit // (rows // 32)].wait()
        to = pl.ds(pl.multiple_of(core * rows + unit * 16, 16), 16)
        vec[chip, :, to, :] = turned_vec(unit, core)

    pl.semaphore_wait(barrier, len(friends))
    for way in range(2):
        vec_copy(way, 0, core, chip).start()

    for unit in range(rows // 16):
        turned = turned_vec(unit, 1 - core)
        for q in range(pairs):
            mixed[unit * 16 : (unit + 1) * 16, q * quarter : (q + 1) * quarter] = turned[q]

    vec_pre = [
        remote(
            mixed.at[pl.ds(0, rows), pl.ds(q * quarter, quarter)], vec.at[chip, q, mine, :],
            pre_send.at[6 + q], pre_recv.at[6 + q], partner,
        )
        for q in range(pairs)
    ]
    for copy in vec_pre:
        copy.start()

    for unit in range(2 * raw_units):
        raw_copy(unit).wait()
        turned = jnp.swapaxes(raw[unit % 2], 0, 1)
        start = (unit % raw_units) * raw_rows
        to = pl.ds(pl.multiple_of(core * rows + start, raw_rows), raw_rows)
        if unit < raw_units:
            own = pl.ds(pl.multiple_of((2 * cut + core) * quarter, quarter), quarter)
            owned = jnp.swapaxes(raw[unit % 2, :, :, own], 0, 1)
            for slot in range(half_slots):
                cols = pl.ds(pl.multiple_of(cut * span + slot * quarter, quarter), quarter)
                right[chip, to, cols] = owned[slot]
                for e in range(4):
                    at = slice((1 + e) * rows + start, (1 + e) * rows + start + raw_rows)
                    mixed[at, slot * quarter : (slot + 1) * quarter] = turned[
                        slot, :, e * quarter : (e + 1) * quarter
                    ]
        else:
            left[pl.ds(cut * half_slots, half_slots), to, :] = turned
        if unit + 2 < 2 * raw_units:
            raw_copy(unit + 2).start()

    def right_part(to_cut, to_core):
        first_row = pl.multiple_of((1 + 2 * to_cut + to_core) * rows, rows)
        return mixed.at[pl.ds(first_row, rows), pl.ds(0, span)]

    for copy in vec_pre:
        copy.wait_recv()
    for way in range(2):
        vec_copy(way, 0, 1 - core, chip).start()

    right_pre = (
        remote(
            right_part(1 - cut, core), right_view, pre_send.at[2], pre_recv.at[2], across
        ),
        remote(
            right_part(1 - cut, 1 - core), right_view, pre_send.at[4], pre_recv.at[4], corner
        ),
        remote(
            right_part(cut, 1 - core), right_view, pre_send.at[5], pre_recv.at[5], partner
        ),
    )
    for copy in right_pre:
        copy.start()
    left_across = remote(left_view, left_view, pre_send.at[0], pre_recv.at[0], across)
    left_across.start()
    left_pair = remote(left_view, left_view, pre_send.at[1], pre_recv.at[1], partner)
    left_pair.start()
    stream_copy(0, 0).start()
    gram_ref[...] = jnp.zeros_like(gram_ref)
    dots_ref[...] = jnp.zeros_like(dots_ref)

    wide = lax.broadcasted_iota(jnp.int32, (mix_ref.shape[0], slots * pairs), 0)
    thin = lax.broadcasted_iota(jnp.int32, (mix_ref.shape[0], slots * pairs), 1)
    stretch = (wide // 8 == thin).astype(jnp.float32)
    tall = jnp.dot(
        stretch, square_ref[...],
        precision=lax.Precision.HIGHEST, preferred_element_type=jnp.float32,
    )
    full = lax.dot_general(
        tall, stretch, (((1,), (1,)), ((), ())),
        precision=lax.Precision.HIGHEST, preferred_element_type=jnp.float32,
    )
    row = lax.broadcasted_iota(jnp.int32, mix_ref.shape, 0)
    lane = lax.broadcasted_iota(jnp.int32, mix_ref.shape, 1)
    mix_ref[...] = jnp.where(lax.rem(row, 8) == lax.rem(lane, 8), full, 0.0)

    def gram_unit(unit):
        slot = lax.rem(unit, 2)
        stream_copy(unit, slot).wait()

        @pl.when(unit + 1 < pieces)
        def _():
            stream_copy(unit + 1, 1 - slot).start()

        chunk = 4

        @pl.loop(0, rows // chunk)
        def _(r):
            vecs = [stream[slot, j, pl.ds(r * chunk, chunk), :, :] for j in range(basis_count)]
            i = 0
            for j in range(basis_count):
                for k in range(j, basis_count):
                    gram_ref[i] += jnp.sum(vecs[j] * vecs[k], axis=0)
                    i += 1

    @pl.loop(0, polls - 2)
    def _(index):
        poll(vec_copy, index, last)

        @pl.when(index < pieces)
        def _():
            gram_unit(index)

    for copy in right_pre:
        copy.wait_recv()
    for sub in range(2):
        for way in range(2):
            right_copy(way, 0, lax.rem(sub + core, 2), chip).start()

    left_across.wait_recv()
    left_pass = remote(left_other, left_other, pre_send.at[3], pre_recv.at[3], partner)
    left_pass.start()

    def total_of(x):
        return jnp.sum(jnp.sum(x, axis=0, keepdims=True), axis=1, keepdims=True)

    row = lax.broadcasted_iota(jnp.int32, gram_tile.shape, 0)
    lane = lax.broadcasted_iota(jnp.int32, gram_tile.shape, 1)
    found = jnp.zeros(gram_tile.shape, jnp.float32)
    i = 0
    for j in range(basis_count):
        for k in range(j, basis_count):
            here = ((row == j) & (lane == k)) | ((row == k) & (lane == j))
            found = jnp.where(here, total_of(gram_ref[i]), found)
            i += 1
    gram_tile[...] = found
    gram_inbox[me] = found

    def gram_copy(offset):
        return remote(
            gram_tile, gram_inbox.at[me],
            gram_send.at[offset], gram_recv.at[offset], place_of(offset),
        )

    def dots_copy(offset):
        return remote(
            dots_tile, dots_inbox.at[me],
            dots_send.at[offset], dots_recv.at[offset], place_of(offset),
        )

    @pl.loop(polls - 2, polls)
    def _(index):
        poll(vec_copy, index, last)

    for offset in range(1, devices):
        gram_copy(offset).start()

    for copy in vec_pre:
        copy.wait_send()
    for copy in right_pre:
        copy.wait_send()
    left_pair.wait_recv()
    left_pass.wait_recv()

    def mix_unit(unit):
        row0 = pl.multiple_of((unit // col_tiles) * row_tile, row_tile)
        col0 = pl.multiple_of(lax.rem(unit, col_tiles) * col_tile, col_tile)

        @pl.loop(0, pairs)
        def _(q):
            proj[q] = jnp.dot(
                left[:, pl.ds(row0, row_tile), :].reshape(slots * row_tile, depth),
                vec[:, q, :, pl.ds(col0, col_tile)].reshape(depth, col_tile),
                preferred_element_type=jnp.float32,
            ).reshape(slots, row_tile, col_tile)

        owner = row0 // rows
        base = owner * (pairs * rows) + row0 - owner * rows

        @pl.loop(0, row_tile // 16)
        def _(g):
            lines = []
            for h in range(2):
                at = pl.ds(pl.multiple_of(g * 16 + h * 8, 8), 8)
                stacked = jnp.concatenate(
                    [proj[q, k, at, :] for k in range(slots) for q in range(pairs)], axis=0
                )
                lines.append(
                    jnp.dot(
                        mix_ref[...],
                        stacked,
                        precision=lax.Precision.HIGHEST,
                        preferred_element_type=jnp.float32,
                    )
                )
            for y in range(slots):
                cols = pl.ds(pl.multiple_of(y * quarter + col0, col_tile), col_tile)
                for p in range(pairs):
                    i = (y * pairs + p) * 8
                    at = pl.ds(pl.multiple_of(base + p * rows + g * 16, 16), 16)
                    mixed[at, cols] = jnp.concatenate(
                        [m[i : i + 8] for m in lines], axis=0
                    ).astype(mixed.dtype)

    lot = pairs * rows

    def pair_copy(unit):
        return remote(
            parts.at[chips + lax.rem(unit, 2)], pair_in.at[lax.rem(unit, 2)],
            pair_send.at[unit], pair_recv.at[unit], partner,
        )

    def late_of(unit):
        return unit // (turn + 1)

    def block_of(unit, way):
        return off_place(way, unit - turn * late_of(unit))

    def home_of(unit, way):
        at = block_of(unit, way)
        return at // half, lax.rem(at, half) * 2 + side_of(way, late_of(unit))

    def cut_copy(unit, way):
        _, piece = home_of(unit, way)
        return remote(
            parts.at[unit, way], cut_in.at[piece],
            cut_send.at[unit, way], cut_recv.at[piece], across,
        )

    def lines_of(unit, way):
        return pl.ds(pl.multiple_of(side_of(way, late_of(unit)) * rows, rows), rows)

    def image_half(unit, sub):
        @pl.when((unit >= 2) & (sub == 0))
        def _():
            pair_copy(unit - 2).wait_send()

        at = lax.rem(sub + core, 2)
        cols = pl.ds(pl.multiple_of(at * span, span), span)

        @pl.loop(0, 2)
        def _(k):
            owner = lax.rem(core + 1 + k, 2)
            to = (1 - k) * (chips + lax.rem(unit, 2)) + k * unit
            lines = jnp.concatenate(
                [
                    right[block_of(unit, way), lines_of(unit, way), cols]
                    for way in range(2)
                ],
                axis=0,
            )
            out = lax.dot_general(
                mixed[pl.ds(pl.multiple_of(owner * lot, lot), lot), cols],
                lines,
                (((1,), (1,)), ((), ())),
                preferred_element_type=jnp.float32,
            )

            @pl.when(sub == 0)
            def _():
                for way in range(2):
                    piece = out[:, way * rows : (way + 1) * rows]
                    parts[to, way] = piece.reshape(pairs, rows, rows)

            @pl.when(sub == 1)
            def _():
                for way in range(2):
                    piece = out[:, way * rows : (way + 1) * rows]
                    parts[to, way] += piece.reshape(pairs, rows, rows)

            @pl.when((sub == 1) & (k == 0))
            def _():
                pair_copy(unit).start()

    def join_unit(unit):
        pair_copy(unit).wait_recv()
        for way in range(2):
            parts[unit, way] += pair_in[lax.rem(unit, 2), way]
            home, piece = home_of(unit, way)

            @pl.when(home != cut)
            def _():
                cut_copy(unit, way).start()

    def fetch_unit(unit):
        for way in range(2):
            home, piece = home_of(unit, way)

            @pl.when(home == cut)
            def _():
                stream_copy(piece, way).start()

    def settle_unit(unit):
        for way in range(2):
            home, piece = home_of(unit, way)

            @pl.when(home == cut)
            def _():
                cut_copy(unit, way).wait_recv()
                cols = pl.ds(pl.multiple_of(piece * rows, rows), rows)
                whole = parts[unit, way] + cut_in[piece]
                for p in range(pairs):
                    next_ref[:, p, cols] = whole[p]
                stream_copy(piece, way).wait()

                def add(step, sums):
                    sums = list(sums)
                    for line in range(16):
                        at = step * 16 + line
                        image = next_ref[at, :, cols]
                        for j in range(basis_count):
                            sums[j] += stream[way, j, at, :, :] * image
                        sums[basis_count] += image * image
                    return tuple(sums)

                sums = lax.fori_loop(
                    0, rows // 16, add, tuple(dots_ref[j] for j in range(basis_count + 1))
                )
                for j in range(basis_count + 1):
                    dots_ref[j] = sums[j]

    first = polls - chips

    @pl.loop(0, first)
    def _(index):
        poll(right_copy, index, turn)

        @pl.loop((mix_units * index) // first, (mix_units * (index + 1)) // first)
        def _(unit):
            mix_unit(unit)

    def ready(index):
        return jnp.minimum(2 * (index - first) + 3, index + 3)

    @pl.loop(first, polls)
    def _(index):
        poll(right_copy, index, turn)

        @pl.loop(jnp.where(index == first, 0, ready(index - 1)), ready(index))
        def _(piece):
            unit, sub = piece // 2, lax.rem(piece, 2)
            image_half(unit, sub)

            @pl.when(sub == 1)
            def _():
                join_unit(unit)

            @pl.when((sub == 1) & (unit == 1))
            def _():
                fetch_unit(0)

            @pl.when((sub == 1) & (unit > 1) & (unit < last))
            def _():
                settle_unit(unit - 2)
                fetch_unit(unit - 1)

    slots_held = stream.shape[0]
    for piece in range(slots_held - 2):
        stream_copy(piece, 2 + piece).start()
    settle_unit(last - 2)
    fetch_unit(last - 1)
    settle_unit(last - 1)
    fetch_unit(last)
    for offset in range(1, devices):
        gram_copy(offset).wait_recv()
    gram = gram_inbox[0]
    for d in range(1, devices):
        gram = gram + gram_inbox[d]
    gram = gram / entries
    settle_unit(last)
    for slot in range(2):
        stream_copy(slots_held - 2 + slot, slot).start()

    spot = lax.broadcasted_iota(jnp.int32, dots_tile.shape, 1)
    found = jnp.zeros(dots_tile.shape, jnp.float32)
    for j in range(basis_count + 1):
        found = jnp.where(spot == j, total_of(dots_ref[j]), found)
    dots_tile[...] = found
    dots_inbox[me] = found
    for offset in range(1, devices):
        dots_copy(offset).start()
    for offset in range(1, devices):
        dots_copy(offset).wait_recv()
    along = dots_inbox[0]
    for d in range(1, devices):
        along = along + dots_inbox[d]
    along = along / entries

    n, end, prior = basis_count, basis_count - 1, basis_count - 2
    spread = jnp.broadcast_to(along, gram_tile.shape)
    down = jnp.sum(jnp.where(row == lane, spread, 0.0), axis=1, keepdims=True)[0:n]
    square = along[:, n : n + 1]
    along = along[:, 0:n]
    gram = gram[0:n, 0:n]
    alpha = down[end : end + 1]
    beta = jnp.full((1, 1), beta_ref[0], jnp.float32)
    ortho = down - alpha * gram[:, end : end + 1] - beta * gram[:, prior : prior + 1]
    ortho_row = along - alpha * gram[end : end + 1, :] - beta * gram[prior : prior + 1, :]
    first = (
        square
        - 2.0 * alpha * alpha
        - 2.0 * beta * down[prior : prior + 1]
        + alpha * alpha * gram[end : end + 1, end : end + 1]
        + 2.0 * alpha * beta * gram[end : end + 1, prior : prior + 1]
        + beta * beta * gram[prior : prior + 1, prior : prior + 1]
    )
    bent = jnp.sum(ortho * gram, axis=0, keepdims=True) * ortho_row
    mean = (
        first
        - 2.0 * jnp.sum(ortho * ortho, axis=0, keepdims=True)
        + jnp.sum(bent, axis=1, keepdims=True)
    )
    beta_new = jnp.sqrt(mean + 1e-06)
    values_ref[...] = jnp.where(
        (row == 0) & (lane == 0), alpha, jnp.where((row == 0) & (lane == 1), beta_new, 0.0)
    )
    index = lax.broadcasted_iota(jnp.int32, ortho.shape, 0)
    coefs = ortho + jnp.where(index == end, alpha, 0.0) + jnp.where(index == prior, beta, 0.0)
    coefs = [jnp.broadcast_to(coefs[j : j + 1], (pairs, lanes)) for j in range(n)]
    scale = jnp.broadcast_to(1.0 / beta_new, (pairs, lanes))

    @pl.loop(0, pieces)
    def _(piece):
        slot = lax.rem(piece + 2, slots_held)
        stream_copy(piece, slot).wait()
        cols = pl.ds(pl.multiple_of(piece * lanes, lanes), lanes)

        @pl.loop(0, rows // 32)
        def _(step):
            for line in range(32):
                at = step * 32 + line
                value = next_ref[at, :, cols]
                for j in range(n):
                    value = value - coefs[j] * stream[slot, j, at, :, :]
                next_ref[at, :, cols] = value * scale

        @pl.when(piece + slots_held < pieces)
        def _():
            stream_copy(piece + slots_held, slot).start()

    @pl.loop(0, chips)
    def _(unit):
        for way in range(2):
            home, _ = home_of(unit, way)

            @pl.when(home != cut)
            def _():
                cut_copy(unit, way).wait_send()

    drain(vec_copy)
    drain(right_copy)
    for unit in (chips - 2, chips - 1):
        pair_copy(unit).wait_send()
    left_across.wait_send()
    left_pair.wait_send()
    left_pass.wait_send()
    for offset in range(1, devices):
        gram_copy(offset).wait_send()
        dots_copy(offset).wait_send()


def ring_step(blocks, cuts, entries, table, left_env, right_env, basis, beta_prev):
    rows, half_slots, depth = left_env.shape
    pairs, cols = basis.shape[2], basis.shape[3]
    slots, chips, quarter = 2 * half_slots, depth // (2 * rows), cols // 2
    basis_count = basis.shape[0]
    count = basis_count * (basis_count + 1) // 2
    square = table.transpose(1, 2, 0, 3).reshape(slots * pairs, slots * pairs)
    bf16, f32 = jnp.bfloat16, jnp.float32
    sem = pltpu.SemaphoreType.DMA
    steps = chips - 1
    hbm = pl.BlockSpec(memory_space=pltpu.HBM)
    vmem = pl.BlockSpec(memory_space=pltpu.VMEM)
    devices = blocks * cuts
    smem = pl.BlockSpec(memory_space=pltpu.SMEM)
    next_vector, values = pl.pallas_call(
        functools.partial(ring_kernel, blocks, cuts, entries),
        name="ring",
        in_specs=[smem, hbm, hbm, vmem, hbm],
        out_specs=[vmem, vmem],
        out_shape=[
            jax.ShapeDtypeStruct((rows, pairs, cols), f32),
            jax.ShapeDtypeStruct((8, 128), f32),
        ],
        scratch_shapes=[
            pltpu.VMEM((chips, pairs, 2 * rows, quarter), bf16),
            pltpu.VMEM((slots, 2 * rows, depth), bf16),
            pltpu.VMEM((chips, 2 * rows, slots * quarter), bf16),
            pltpu.VMEM((2 * pairs * rows, slots * quarter), bf16),
            pltpu.VMEM((slots * pairs * 8, slots * pairs * 8), f32),
            pltpu.VMEM((pairs, slots, rows // 2, quarter // 2), f32),
            pltpu.VMEM((chips + 2, 2, pairs, rows, rows), f32),
            pltpu.VMEM((2, 2, pairs, rows, rows), f32),
            pltpu.VMEM((chips, pairs, rows, rows), f32),
            pltpu.VMEM((4, basis_count, rows, pairs, 128), f32),
            pltpu.VMEM((2, 32, half_slots, depth), bf16),
            pltpu.VMEM((count, pairs, 128), f32),
            pltpu.VMEM((basis_count + 1, pairs, 128), f32),
            pltpu.VMEM((8, 128), f32),
            pltpu.VMEM((devices, 8, 128), f32),
            pltpu.VMEM((1, 128), f32),
            pltpu.VMEM((devices, 1, 128), f32),
            sem((devices,)),
            sem((devices,)),
            sem((devices,)),
            sem((devices,)),
            sem((2,)),
            sem((2,)),
            sem((6 + pairs,)),
            sem((6 + pairs,)),
            sem((2, steps, 2)),
            sem((2, steps, 2)),
            sem((2, steps, 2)),
            sem((2, steps, 2)),
            sem((chips,)),
            sem((chips,)),
            sem((chips, 2)),
            sem((chips,)),
            sem((4,)),
        ],
        compiler_params=pltpu.CompilerParams(
            vmem_limit_bytes=65400 * 1024, collective_id=1, has_side_effects=True
        ),
    )(beta_prev.reshape(1), left_env, right_env, square, basis)
    return next_vector, values[0, 0:1], values[0, 1:2]


def ring_fits(blocks, rows, basis_count):
    return blocks == 16 and rows == 128 and basis_count == 8


def gathered_image(cuts, table, left_env, right_env, current):
    row_count, pair_count, col_count = current.shape
    bond_width = table.shape[0]
    full_width = left_env.shape[2]
    me = lax.axis_index("cuts")
    swap = [(0, 1), (1, 0)]

    current = current.transpose(1, 0, 2)
    left_t = left_env.transpose(1, 0, 2)
    right_t = right_env.transpose(1, 0, 2)
    if cuts == 2:
        half = left_t.shape[0]
        theirs = lax.dynamic_slice_in_dim(right_t, (1 - me) * col_count, col_count, 2)
        mine = lax.dynamic_slice_in_dim(right_t, me * col_count, col_count, 2)
        right_k = jnp.concatenate([mine, lax.ppermute(theirs, "cuts", swap)], axis=0)
        left_k = jnp.concatenate([left_t, lax.ppermute(left_t, "cuts", swap)], axis=0)
        turned = jnp.roll(jnp.roll(table, -half, axis=0), -half, axis=1)
        table = jnp.where(me == 0, table, turned)
    else:
        left_k = lax.all_gather(left_t, "cuts", axis=0, tiled=True)
        right_k = lax.all_to_all(right_t, "cuts", split_axis=2, concat_axis=0, tiled=True)
    cur_full = lax.all_gather(current, "blk", axis=1, tiled=True)
    right_full = lax.all_gather(right_k, "blk", axis=1, tiled=True)

    mixed = mixed_left_of(table, left_k, cur_full)
    mixed = mixed.reshape(bond_width, pair_count * row_count, col_count)
    if cuts == 2:
        away = image_part(mixed, right_full, (1 - me) * col_count, col_count)
        away = lax.ppermute(away, "cuts", swap)
        here = image_part(mixed, right_full, me * col_count, col_count)
        image = here + away
    else:
        image = image_part(mixed, right_full, jnp.int32(0), full_width)
        image = lax.psum_scatter(image, "cuts", scatter_dimension=1, tiled=True)
    return image.reshape(pair_count, row_count, col_count).transpose(1, 0, 2)


def on_device(
    blocks, cuts, left_env, right_env, left_core, right_core, slot_bond, krylov_basis, beta_prev
):
    pair_count = left_core.shape[2] * left_core.shape[2]
    basis_count, row_count, _, _ = krylov_basis.shape
    full_width = left_env.shape[2]
    entries = float(full_width * pair_count * full_width)
    table = build_table(left_core, right_core, slot_bond)
    if cuts == 2 and ring_fits(blocks, row_count, basis_count):
        return ring_step(
            blocks, cuts, entries, table, left_env, right_env, krylov_basis, beta_prev
        )
    current = krylov_basis[basis_count - 1].astype(jnp.bfloat16)
    image = gathered_image(cuts, table, left_env, right_env, current)
    gram = gram_of(krylov_basis)

    sums = lax.psum(jnp.concatenate([gram, dots_of(krylov_basis, image)]), ("blk", "cuts"))
    sums = sums / entries
    count = basis_count * (basis_count + 1) // 2
    where = []
    for j in range(basis_count):
        for k in range(basis_count):
            low, high = min(j, k), max(j, k)
            where.append(low * basis_count - low * (low - 1) // 2 + high - low)
    gram_matrix = sums[jnp.array(where)].reshape(basis_count, basis_count)
    inner_prods = sums[count : count + basis_count]
    image_square = sums[count + basis_count]
    last, prior = basis_count - 1, basis_count - 2
    alpha_now = inner_prods[last]
    ortho_coeffs = (
        inner_prods - alpha_now * gram_matrix[:, last] - beta_prev * gram_matrix[:, prior]
    )
    first_square = (
        image_square
        - 2.0 * alpha_now * inner_prods[last]
        - 2.0 * beta_prev * inner_prods[prior]
        + alpha_now * alpha_now * gram_matrix[last, last]
        + 2.0 * alpha_now * beta_prev * gram_matrix[last, prior]
        + beta_prev * beta_prev * gram_matrix[prior, prior]
    )
    square_mean = (
        first_square
        - 2.0 * jnp.sum(ortho_coeffs * ortho_coeffs)
        + jnp.sum(ortho_coeffs[:, None] * gram_matrix * ortho_coeffs[None, :])
    )
    beta_new = jnp.sqrt(square_mean + 1e-06)
    index = jnp.arange(basis_count)
    coefs = (
        ortho_coeffs
        + jnp.where(index == last, alpha_now, 0.0)
        + jnp.where(index == prior, beta_prev, 0.0)
    )
    coefs = jnp.concatenate([coefs, (1.0 / beta_new)[None]])
    next_vector = final_of(coefs, krylov_basis, image)
    return (next_vector, alpha_now[None], beta_new[None])


def solution(mesh):
    in_specs = (
        P("blk", "cuts", None),
        P("blk", "cuts", None),
        P(),
        P(),
        P(),
        P(None, "blk", None, "cuts"),
        P(),
    )
    out_specs = (P("blk", None, "cuts"), P(), P())
    return jax.shard_map(
        functools.partial(on_device, mesh.shape["blk"], mesh.shape["cuts"]),
        mesh=mesh,
        in_specs=in_specs,
        out_specs=out_specs,
        check_vma=False,
    )
```

```python
import functools

import jax
import jax.numpy as jnp
from jax import lax
from jax.experimental import pallas as pl
from jax.experimental.pallas import tpu as pltpu
from jax.sharding import PartitionSpec as P

VMEM_BYTES = 60 * 1024 * 1024


def params():
    return pltpu.CompilerParams(vmem_limit_bytes=VMEM_BYTES)


def tile_of(size, most):
    return most if size % most == 0 else size


def build_table(left_core, right_core, slot_bond):
    bond_width = left_core.shape[0]
    phys_dim = left_core.shape[2]
    chosen = (slot_bond[:, None] == jnp.arange(bond_width, dtype=jnp.int32)[None, :]).astype(
        jnp.float32
    )
    picked = jnp.einsum("kw,wxac->kxac", chosen, left_core, precision=lax.Precision.HIGHEST)
    table = jnp.einsum("kxac,xybd->kyabcd", picked, right_core, precision=lax.Precision.HIGHEST)
    return table.reshape(bond_width, bond_width, phys_dim * phys_dim, phys_dim * phys_dim)


def mix_kernel(mix_ref, left_ref, cur_ref, out_ref, proj):
    slots, rows, depth = left_ref.shape
    pairs = cur_ref.shape[0]
    bonds = out_ref.shape[0]
    cols = cur_ref.shape[2]

    @pl.loop(0, pairs)
    def _(q):
        proj[q] = jnp.dot(
            left_ref[...].reshape(slots * rows, depth),
            cur_ref[q],
            preferred_element_type=jnp.float32,
        ).reshape(slots, rows, cols)

    @pl.loop(0, rows // 16)
    def _(g):
        mixed = []
        for h in range(2):
            at = pl.ds(pl.multiple_of(g * 16 + h * 8, 8), 8)
            stacked = jnp.concatenate(
                [proj[q, k, at, :] for k in range(slots) for q in range(pairs)], axis=0
            )
            mixed.append(
                jnp.dot(
                    mix_ref[...],
                    stacked,
                    precision=lax.Precision.HIGHEST,
                    preferred_element_type=jnp.float32,
                )
            )
        at = pl.ds(pl.multiple_of(g * 16, 16), 16)
        for y in range(bonds):
            for p in range(pairs):
                i = (y * pairs + p) * 8
                out_ref[y, p, at, :] = jnp.concatenate(
                    [m[i : i + 8] for m in mixed], axis=0
                ).astype(out_ref.dtype)


def mixed_left_of(table, left_k, cur_full):
    slots, rows, depth = left_k.shape
    pairs, _, cols = cur_full.shape
    bonds = table.shape[1]
    tb = tile_of(cols, 256)
    square = table.transpose(1, 2, 0, 3).reshape(bonds * pairs, slots * pairs)
    mix = jnp.kron(square, jnp.eye(8, dtype=jnp.float32))
    return pl.pallas_call(
        mix_kernel,
        grid=(cols // tb,),
        in_specs=[
            pl.BlockSpec(mix.shape, lambda i: (0, 0)),
            pl.BlockSpec((slots, rows, depth), lambda i: (0, 0, 0)),
            pl.BlockSpec((pairs, depth, tb), lambda i: (0, 0, i)),
        ],
        out_specs=pl.BlockSpec((bonds, pairs, rows, tb), lambda i: (0, 0, 0, i)),
        out_shape=jax.ShapeDtypeStruct((bonds, pairs, rows, cols), jnp.bfloat16),
        scratch_shapes=[pltpu.VMEM((pairs, slots, rows, tb), jnp.float32)],
        compiler_params=params(),
        cost_estimate=pl.CostEstimate(
            flops=2 * slots * rows * depth * pairs * cols,
            bytes_accessed=2 * (left_k.size + cur_full.size + bonds * pairs * rows * cols),
            transcendentals=0,
        ),
    )(mix, left_k, cur_full)


def image_kernel(start_ref, mixed_ref, right_ref, out_ref):
    bonds = mixed_ref.shape[0]
    out_ref[...] = jnp.zeros_like(out_ref)

    @pl.loop(0, bonds)
    def _(y):
        out_ref[...] += lax.dot_general(
            mixed_ref[y],
            right_ref[y],
            (((1,), (1,)), ((), ())),
            preferred_element_type=jnp.float32,
        )


def image_part(mixed, right_full, start, count):
    bonds, lines, cols = mixed.shape
    tb = tile_of(count, 256)
    return pl.pallas_call(
        image_kernel,
        grid_spec=pltpu.PrefetchScalarGridSpec(
            num_scalar_prefetch=1,
            grid=(count // tb,),
            in_specs=[
                pl.BlockSpec((bonds, lines, cols), lambda i, s: (0, 0, 0)),
                pl.BlockSpec((bonds, tb, cols), lambda i, s: (0, s[0] + i, 0)),
            ],
            out_specs=pl.BlockSpec((lines, tb), lambda i, s: (0, i)),
        ),
        out_shape=jax.ShapeDtypeStruct((lines, count), jnp.float32),
        compiler_params=params(),
        cost_estimate=pl.CostEstimate(
            flops=2 * bonds * lines * cols * count,
            bytes_accessed=2 * (mixed.size + bonds * count * cols),
            transcendentals=0,
        ),
    )((start // tb).reshape(1).astype(jnp.int32), mixed, right_full)


def gram_kernel(basis_ref, out_ref):
    basis_count, rows, pairs, cols = basis_ref.shape
    chunk = 4
    lanes = cols // 128

    @pl.when(pl.program_id(0) == 0)
    def _():
        out_ref[...] = jnp.zeros_like(out_ref)

    @pl.loop(0, rows // chunk)
    def _(r):
        for c in range(lanes):
            vecs = [
                basis_ref[j, pl.ds(r * chunk, chunk), :, c * 128 : (c + 1) * 128]
                for j in range(basis_count)
            ]
            i = 0
            for j in range(basis_count):
                for k in range(j, basis_count):
                    out_ref[i] += jnp.sum(vecs[j] * vecs[k], axis=0)
                    i += 1


def gram_of(basis):
    basis_count, rows, pairs, cols = basis.shape
    count = basis_count * (basis_count + 1) // 2
    ta = tile_of(rows, 16)
    sums = pl.pallas_call(
        gram_kernel,
        grid=(rows // ta,),
        in_specs=[pl.BlockSpec((basis_count, ta, pairs, cols), lambda i: (0, i, 0, 0))],
        out_specs=pl.BlockSpec((count, pairs, 128), lambda i: (0, 0, 0)),
        out_shape=jax.ShapeDtypeStruct((count, pairs, 128), jnp.float32),
        compiler_params=params(),
        cost_estimate=pl.CostEstimate(
            flops=2 * count * rows * pairs * cols,
            bytes_accessed=4 * basis.size,
            transcendentals=0,
        ),
    )(basis)
    return jnp.sum(sums, axis=(1, 2))


def dots_kernel(basis_ref, image_ref, out_ref):
    basis_count, rows, pairs, cols = basis_ref.shape

    @pl.when(pl.program_id(0) == 0)
    def _():
        out_ref[...] = jnp.zeros_like(out_ref)

    for c in range(cols // 128):
        at = slice(c * 128, (c + 1) * 128)
        image = image_ref[:, :, at]
        for j in range(basis_count):
            out_ref[j] += jnp.sum(basis_ref[j, :, :, at] * image, axis=0)
        out_ref[basis_count] += jnp.sum(image * image, axis=0)


def dots_of(basis, image):
    basis_count, rows, pairs, cols = basis.shape
    ta = tile_of(rows, 16)
    sums = pl.pallas_call(
        dots_kernel,
        grid=(rows // ta,),
        in_specs=[
            pl.BlockSpec((basis_count, ta, pairs, cols), lambda i: (0, i, 0, 0)),
            pl.BlockSpec((ta, pairs, cols), lambda i: (i, 0, 0)),
        ],
        out_specs=pl.BlockSpec((basis_count + 1, pairs, 128), lambda i: (0, 0, 0)),
        out_shape=jax.ShapeDtypeStruct((basis_count + 1, pairs, 128), jnp.float32),
        compiler_params=params(),
    )(basis, image)
    return jnp.sum(sums, axis=(1, 2))


def final_kernel(coef_ref, basis_ref, image_ref, out_ref):
    basis_count = basis_ref.shape[0]
    total = image_ref[...]
    for j in range(basis_count):
        total = total - coef_ref[j] * basis_ref[j]
    out_ref[...] = total * coef_ref[basis_count]


def final_of(coefs, basis, image):
    basis_count, rows, pairs, cols = basis.shape
    ta = tile_of(rows, 16)
    return pl.pallas_call(
        final_kernel,
        grid=(rows // ta,),
        in_specs=[
            pl.BlockSpec(memory_space=pltpu.SMEM),
            pl.BlockSpec((basis_count, ta, pairs, cols), lambda i: (0, i, 0, 0)),
            pl.BlockSpec((ta, pairs, cols), lambda i: (i, 0, 0)),
        ],
        out_specs=pl.BlockSpec((ta, pairs, cols), lambda i: (i, 0, 0)),
        out_shape=jax.ShapeDtypeStruct((rows, pairs, cols), jnp.float32),
        compiler_params=params(),
    )(coefs, basis, image)


MESH = pl.DeviceIdType.MESH


def ring_kernel(
    blocks, cuts, entries,
    beta_ref, left_ref, right_ref, square_ref, basis_ref,
    next_ref, values_ref,
    vec, left, right, mixed, mix_ref, proj, parts, pair_in, cut_in, stream, raw,
    gram_ref, dots_ref, gram_tile, gram_inbox, dots_tile, dots_inbox,
    gram_send, gram_recv, dots_send, dots_recv,
    own_sem, raw_sem, pre_send, pre_recv, vec_send, vec_recv, right_send, right_recv,
    pair_send, pair_recv, cut_send, cut_recv, stream_sem,
):
    chips, pairs, chip_rows, quarter = vec.shape
    slots, _, depth = left.shape
    rows, half_slots, _ = left_ref.shape
    span = half_slots * quarter
    last = chips - 1
    polls = 2 * last
    row_tile, col_tile = proj.shape[2], proj.shape[3]
    col_tiles = quarter // col_tile
    mix_units = (chip_rows // row_tile) * col_tiles
    basis_count = basis_ref.shape[0]
    lanes = stream.shape[4]
    pieces = basis_ref.shape[3] // lanes
    half = chips // 2

    blk = lax.axis_index("blk")
    cut = lax.axis_index("cuts")
    core = lax.rem(blk, 2)
    chip = blk // 2
    side = lax.rem(chip, 2)
    place = (1 - side) * (chip // 2) + side * (last - chip // 2)

    def chip_at(index):
        index = lax.rem(index + 2 * chips, chips)
        far = index // half
        return (1 - far) * 2 * index + far * (2 * (last - index) + 1)

    after = (2 * chip_at(place + 1) + core, cut)
    before = (2 * chip_at(place - 1) + core, cut)
    onward = (after, before)
    partner = (2 * chip + 1 - core, cut)
    across = (blk, 1 - cut)
    corner = (2 * chip + 1 - core, 1 - cut)

    def remote(src, dst, send, recv, device):
        return pltpu.make_async_remote_copy(
            src_ref=src, dst_ref=dst, send_sem=send, recv_sem=recv,
            device_id=device, device_id_type=MESH,
        )

    turn = last - 2

    def off_place(way, off):
        return chip_at(place - off) if way == 0 else chip_at(place + off)

    def side_of(way, late):
        return late + way * (1 - 2 * late)

    def vec_copy(way, step, sub, at):
        view = vec.at[at, pl.ds(way * (pairs // 2), pairs // 2), pl.ds(sub * rows, rows), :]
        return remote(
            view, view, vec_send.at[way, step, sub], vec_recv.at[way, step, sub], onward[way]
        )

    def right_copy(way, step, sub, at):
        lines = pl.ds(pl.multiple_of(side_of(way, step // turn) * rows, rows), rows)
        view = right.at[at, lines, pl.ds(sub * span, span)]
        return remote(
            view, view, right_send.at[way, step, sub], right_recv.at[way, step, sub], onward[way]
        )

    def poll(copy_of, index, bend):
        step, sub = index // 2, lax.rem(index + core, 2)
        for way in range(2):
            at = off_place(way, step + 1 - bend * (step // bend))
            copy_of(way, step, sub, at).wait_recv()
            bent = (step + 1) // bend - step // bend

            @pl.when(step < last - 1)
            def _():
                copy_of(way, step + 1, sub, at + bent * (chip - at)).start()

    def drain(copy_of):
        @pl.loop(0, polls)
        def _(index):
            for way in range(2):
                copy_of(way, index // 2, lax.rem(index, 2), chip).wait_send()

    mine = pl.ds(core * rows, rows)
    left_view = left.at[pl.ds(cut * half_slots, half_slots), mine, :]
    left_other = left.at[pl.ds((1 - cut) * half_slots, half_slots), mine, :]
    right_view = right.at[chip, mine, pl.ds(cut * span, span)]
    vec_load = []
    for part in range(2):
        at = pl.ds(part * (rows // 2), rows // 2)
        vec_load.append(
            pltpu.make_async_copy(
                basis_ref.at[basis_count - 1, at], next_ref.at[at], own_sem.at[part]
            )
        )
        vec_load[part].start()
    raw_rows = raw.shape[1]
    raw_units = rows // raw_rows

    def raw_copy(unit):
        source = right_ref if unit < raw_units else left_ref
        at = pl.ds((unit % raw_units) * raw_rows, raw_rows)
        return pltpu.make_async_copy(source.at[at], raw.at[unit % 2], raw_sem.at[unit % 2])

    raw_copy(0).start()
    raw_copy(1).start()

    def stream_copy(piece, slot):
        return pltpu.make_async_copy(
            basis_ref.at[:, :, :, pl.ds(pl.multiple_of(piece * lanes, lanes), lanes)],
            stream.at[slot],
            stream_sem.at[slot],
        )

    devices = blocks * cuts
    me = blk * cuts + cut

    def place_of(offset):
        device = lax.rem(me + offset, devices)
        return (device // cuts, lax.rem(device, cuts))

    barrier = pltpu.get_barrier_semaphore()
    friends = (after, before, partner, across, corner)
    for friend in friends:
        pl.semaphore_signal(barrier, inc=1, device_id=friend, device_id_type=MESH)

    def turned_vec(unit, owner):
        at = slice(unit * 16, (unit + 1) * 16)
        cols = pl.ds(pl.multiple_of(owner * quarter, quarter), quarter)
        return jnp.swapaxes(next_ref[at, :, cols].astype(vec.dtype), 0, 1)

    for unit in range(rows // 16):
        if unit % (rows // 32) == 0:
            vec_load[unit // (rows // 32)].wait()
        to = pl.ds(pl.multiple_of(core * rows + unit * 16, 16), 16)
        vec[chip, :, to, :] = turned_vec(unit, core)

    pl.semaphore_wait(barrier, len(friends))
    for way in range(2):
        vec_copy(way, 0, core, chip).start()

    for unit in range(rows // 16):
        turned = turned_vec(unit, 1 - core)
        for q in range(pairs):
            mixed[unit * 16 : (unit + 1) * 16, q * quarter : (q + 1) * quarter] = turned[q]

    vec_pre = [
        remote(
            mixed.at[pl.ds(0, rows), pl.ds(q * quarter, quarter)], vec.at[chip, q, mine, :],
            pre_send.at[6 + q], pre_recv.at[6 + q], partner,
        )
        for q in range(pairs)
    ]
    for copy in vec_pre:
        copy.start()

    for unit in range(2 * raw_units):
        raw_copy(unit).wait()
        turned = jnp.swapaxes(raw[unit % 2], 0, 1)
        start = (unit % raw_units) * raw_rows
        to = pl.ds(pl.multiple_of(core * rows + start, raw_rows), raw_rows)
        if unit < raw_units:
            own = pl.ds(pl.multiple_of((2 * cut + core) * quarter, quarter), quarter)
            owned = jnp.swapaxes(raw[unit % 2, :, :, own], 0, 1)
            for slot in range(half_slots):
                cols = pl.ds(pl.multiple_of(cut * span + slot * quarter, quarter), quarter)
                right[chip, to, cols] = owned[slot]
                for e in range(4):
                    at = slice((1 + e) * rows + start, (1 + e) * rows + start + raw_rows)
                    mixed[at, slot * quarter : (slot + 1) * quarter] = turned[
                        slot, :, e * quarter : (e + 1) * quarter
                    ]
        else:
            left[pl.ds(cut * half_slots, half_slots), to, :] = turned
        if unit + 2 < 2 * raw_units:
            raw_copy(unit + 2).start()

    def right_part(to_cut, to_core):
        first_row = pl.multiple_of((1 + 2 * to_cut + to_core) * rows, rows)
        return mixed.at[pl.ds(first_row, rows), pl.ds(0, span)]

    for copy in vec_pre:
        copy.wait_recv()
    for way in range(2):
        vec_copy(way, 0, 1 - core, chip).start()

    right_pre = (
        remote(
            right_part(1 - cut, core), right_view, pre_send.at[2], pre_recv.at[2], across
        ),
        remote(
            right_part(1 - cut, 1 - core), right_view, pre_send.at[4], pre_recv.at[4], corner
        ),
        remote(
            right_part(cut, 1 - core), right_view, pre_send.at[5], pre_recv.at[5], partner
        ),
    )
    for copy in right_pre:
        copy.start()
    left_across = remote(left_view, left_view, pre_send.at[0], pre_recv.at[0], across)
    left_across.start()
    left_pair = remote(left_view, left_view, pre_send.at[1], pre_recv.at[1], partner)
    left_pair.start()
    stream_copy(0, 0).start()
    gram_ref[...] = jnp.zeros_like(gram_ref)
    dots_ref[...] = jnp.zeros_like(dots_ref)

    wide = lax.broadcasted_iota(jnp.int32, (mix_ref.shape[0], slots * pairs), 0)
    thin = lax.broadcasted_iota(jnp.int32, (mix_ref.shape[0], slots * pairs), 1)
    stretch = (wide // 8 == thin).astype(jnp.float32)
    tall = jnp.dot(
        stretch, square_ref[...],
        precision=lax.Precision.HIGHEST, preferred_element_type=jnp.float32,
    )
    full = lax.dot_general(
        tall, stretch, (((1,), (1,)), ((), ())),
        precision=lax.Precision.HIGHEST, preferred_element_type=jnp.float32,
    )
    row = lax.broadcasted_iota(jnp.int32, mix_ref.shape, 0)
    lane = lax.broadcasted_iota(jnp.int32, mix_ref.shape, 1)
    mix_ref[...] = jnp.where(lax.rem(row, 8) == lax.rem(lane, 8), full, 0.0)

    def gram_unit(unit):
        slot = lax.rem(unit, 2)
        stream_copy(unit, slot).wait()

        @pl.when(unit + 1 < pieces)
        def _():
            stream_copy(unit + 1, 1 - slot).start()

        chunk = 4

        @pl.loop(0, rows // chunk)
        def _(r):
            vecs = [stream[slot, j, pl.ds(r * chunk, chunk), :, :] for j in range(basis_count)]
            i = 0
            for j in range(basis_count):
                for k in range(j, basis_count):
                    gram_ref[i] += jnp.sum(vecs[j] * vecs[k], axis=0)
                    i += 1

    @pl.loop(0, polls - 2)
    def _(index):
        poll(vec_copy, index, last)

        @pl.when(index < pieces)
        def _():
            gram_unit(index)

    for copy in right_pre:
        copy.wait_recv()
    for sub in range(2):
        for way in range(2):
            right_copy(way, 0, lax.rem(sub + core, 2), chip).start()

    left_across.wait_recv()
    left_pass = remote(left_other, left_other, pre_send.at[3], pre_recv.at[3], partner)
    left_pass.start()

    def total_of(x):
        return jnp.sum(jnp.sum(x, axis=0, keepdims=True), axis=1, keepdims=True)

    row = lax.broadcasted_iota(jnp.int32, gram_tile.shape, 0)
    lane = lax.broadcasted_iota(jnp.int32, gram_tile.shape, 1)
    found = jnp.zeros(gram_tile.shape, jnp.float32)
    i = 0
    for j in range(basis_count):
        for k in range(j, basis_count):
            here = ((row == j) & (lane == k)) | ((row == k) & (lane == j))
            found = jnp.where(here, total_of(gram_ref[i]), found)
            i += 1
    gram_tile[...] = found
    gram_inbox[me] = found

    def gram_copy(offset):
        return remote(
            gram_tile, gram_inbox.at[me],
            gram_send.at[offset], gram_recv.at[offset], place_of(offset),
        )

    def dots_copy(offset):
        return remote(
            dots_tile, dots_inbox.at[me],
            dots_send.at[offset], dots_recv.at[offset], place_of(offset),
        )

    @pl.loop(polls - 2, polls)
    def _(index):
        poll(vec_copy, index, last)

    for offset in range(1, devices):
        gram_copy(offset).start()

    for copy in vec_pre:
        copy.wait_send()
    for copy in right_pre:
        copy.wait_send()
    left_pair.wait_recv()
    left_pass.wait_recv()

    def mix_unit(unit):
        row0 = pl.multiple_of((unit // col_tiles) * row_tile, row_tile)
        col0 = pl.multiple_of(lax.rem(unit, col_tiles) * col_tile, col_tile)

        @pl.loop(0, pairs)
        def _(q):
            proj[q] = jnp.dot(
                left[:, pl.ds(row0, row_tile), :].reshape(slots * row_tile, depth),
                vec[:, q, :, pl.ds(col0, col_tile)].reshape(depth, col_tile),
                preferred_element_type=jnp.float32,
            ).reshape(slots, row_tile, col_tile)

        owner = row0 // rows
        base = owner * (pairs * rows) + row0 - owner * rows

        @pl.loop(0, row_tile // 16)
        def _(g):
            lines = []
            for h in range(2):
                at = pl.ds(pl.multiple_of(g * 16 + h * 8, 8), 8)
                stacked = jnp.concatenate(
                    [proj[q, k, at, :] for k in range(slots) for q in range(pairs)], axis=0
                )
                lines.append(
                    jnp.dot(
                        mix_ref[...],
                        stacked,
                        precision=lax.Precision.HIGHEST,
                        preferred_element_type=jnp.float32,
                    )
                )
            for y in range(slots):
                cols = pl.ds(pl.multiple_of(y * quarter + col0, col_tile), col_tile)
                for p in range(pairs):
                    i = (y * pairs + p) * 8
                    at = pl.ds(pl.multiple_of(base + p * rows + g * 16, 16), 16)
                    mixed[at, cols] = jnp.concatenate(
                        [m[i : i + 8] for m in lines], axis=0
                    ).astype(mixed.dtype)

    lot = pairs * rows

    def pair_copy(unit):
        return remote(
            parts.at[chips + lax.rem(unit, 2)], pair_in.at[lax.rem(unit, 2)],
            pair_send.at[unit], pair_recv.at[unit], partner,
        )

    def late_of(unit):
        return unit // (turn + 1)

    def block_of(unit, way):
        return off_place(way, unit - turn * late_of(unit))

    def home_of(unit, way):
        at = block_of(unit, way)
        return at // half, lax.rem(at, half) * 2 + side_of(way, late_of(unit))

    def cut_copy(unit, way):
        _, piece = home_of(unit, way)
        return remote(
            parts.at[unit, way], cut_in.at[piece],
            cut_send.at[unit, way], cut_recv.at[piece], across,
        )

    def lines_of(unit, way):
        return pl.ds(pl.multiple_of(side_of(way, late_of(unit)) * rows, rows), rows)

    def image_half(unit, sub):
        @pl.when((unit >= 2) & (sub == 0))
        def _():
            pair_copy(unit - 2).wait_send()

        at = lax.rem(sub + core, 2)
        cols = pl.ds(pl.multiple_of(at * span, span), span)

        @pl.loop(0, 2)
        def _(k):
            owner = lax.rem(core + 1 + k, 2)
            to = (1 - k) * (chips + lax.rem(unit, 2)) + k * unit
            lines = jnp.concatenate(
                [
                    right[block_of(unit, way), lines_of(unit, way), cols]
                    for way in range(2)
                ],
                axis=0,
            )
            out = lax.dot_general(
                mixed[pl.ds(pl.multiple_of(owner * lot, lot), lot), cols],
                lines,
                (((1,), (1,)), ((), ())),
                preferred_element_type=jnp.float32,
            )

            @pl.when(sub == 0)
            def _():
                for way in range(2):
                    piece = out[:, way * rows : (way + 1) * rows]
                    parts[to, way] = piece.reshape(pairs, rows, rows)

            @pl.when(sub == 1)
            def _():
                for way in range(2):
                    piece = out[:, way * rows : (way + 1) * rows]
                    parts[to, way] += piece.reshape(pairs, rows, rows)

            @pl.when((sub == 1) & (k == 0))
            def _():
                pair_copy(unit).start()

    def join_unit(unit):
        pair_copy(unit).wait_recv()
        for way in range(2):
            parts[unit, way] += pair_in[lax.rem(unit, 2), way]
            home, piece = home_of(unit, way)

            @pl.when(home != cut)
            def _():
                cut_copy(unit, way).start()

    def fetch_unit(unit):
        for way in range(2):
            home, piece = home_of(unit, way)

            @pl.when(home == cut)
            def _():
                stream_copy(piece, way).start()

    def settle_unit(unit):
        for way in range(2):
            home, piece = home_of(unit, way)

            @pl.when(home == cut)
            def _():
                cut_copy(unit, way).wait_recv()
                cols = pl.ds(pl.multiple_of(piece * rows, rows), rows)
                whole = parts[unit, way] + cut_in[piece]
                for p in range(pairs):
                    next_ref[:, p, cols] = whole[p]
                stream_copy(piece, way).wait()

                def add(step, sums):
                    sums = list(sums)
                    for line in range(16):
                        at = step * 16 + line
                        image = next_ref[at, :, cols]
                        for j in range(basis_count):
                            sums[j] += stream[way, j, at, :, :] * image
                        sums[basis_count] += image * image
                    return tuple(sums)

                sums = lax.fori_loop(
                    0, rows // 16, add, tuple(dots_ref[j] for j in range(basis_count + 1))
                )
                for j in range(basis_count + 1):
                    dots_ref[j] = sums[j]

    first = polls - chips

    @pl.loop(0, first)
    def _(index):
        poll(right_copy, index, turn)

        @pl.loop((mix_units * index) // first, (mix_units * (index + 1)) // first)
        def _(unit):
            mix_unit(unit)

    def ready(index):
        return jnp.minimum(2 * (index - first) + 3, index + 3)

    @pl.loop(first, polls)
    def _(index):
        poll(right_copy, index, turn)

        @pl.loop(jnp.where(index == first, 0, ready(index - 1)), ready(index))
        def _(piece):
            unit, sub = piece // 2, lax.rem(piece, 2)
            image_half(unit, sub)

            @pl.when(sub == 1)
            def _():
                join_unit(unit)

            @pl.when((sub == 1) & (unit == 1))
            def _():
                fetch_unit(0)

            @pl.when((sub == 1) & (unit > 1) & (unit < last))
            def _():
                settle_unit(unit - 2)
                fetch_unit(unit - 1)

    slots_held = stream.shape[0]
    for piece in range(slots_held - 2):
        stream_copy(piece, 2 + piece).start()
    settle_unit(last - 2)
    fetch_unit(last - 1)
    settle_unit(last - 1)
    fetch_unit(last)
    for offset in range(1, devices):
        gram_copy(offset).wait_recv()
    gram = gram_inbox[0]
    for d in range(1, devices):
        gram = gram + gram_inbox[d]
    gram = gram / entries
    settle_unit(last)
    for slot in range(2):
        stream_copy(slots_held - 2 + slot, slot).start()

    spot = lax.broadcasted_iota(jnp.int32, dots_tile.shape, 1)
    found = jnp.zeros(dots_tile.shape, jnp.float32)
    for j in range(basis_count + 1):
        found = jnp.where(spot == j, total_of(dots_ref[j]), found)
    dots_tile[...] = found
    dots_inbox[me] = found
    for offset in range(1, devices):
        dots_copy(offset).start()

    @pl.loop(0, chips)
    def _(unit):
        for way in range(2):
            home, _ = home_of(unit, way)

            @pl.when(home != cut)
            def _():
                cut_copy(unit, way).wait_send()

    drain(vec_copy)
    drain(right_copy)
    for unit in (chips - 2, chips - 1):
        pair_copy(unit).wait_send()
    left_across.wait_send()
    left_pair.wait_send()
    left_pass.wait_send()
    for offset in range(1, devices):
        gram_copy(offset).wait_send()

    for offset in range(1, devices):
        dots_copy(offset).wait_recv()
    along = dots_inbox[0]
    for d in range(1, devices):
        along = along + dots_inbox[d]
    along = along / entries

    n, end, prior = basis_count, basis_count - 1, basis_count - 2
    spread = jnp.broadcast_to(along, gram_tile.shape)
    down = jnp.sum(jnp.where(row == lane, spread, 0.0), axis=1, keepdims=True)[0:n]
    square = along[:, n : n + 1]
    along = along[:, 0:n]
    gram = gram[0:n, 0:n]
    alpha = down[end : end + 1]
    beta = jnp.full((1, 1), beta_ref[0], jnp.float32)
    ortho = down - alpha * gram[:, end : end + 1] - beta * gram[:, prior : prior + 1]
    ortho_row = along - alpha * gram[end : end + 1, :] - beta * gram[prior : prior + 1, :]
    first = (
        square
        - 2.0 * alpha * alpha
        - 2.0 * beta * down[prior : prior + 1]
        + alpha * alpha * gram[end : end + 1, end : end + 1]
        + 2.0 * alpha * beta * gram[end : end + 1, prior : prior + 1]
        + beta * beta * gram[prior : prior + 1, prior : prior + 1]
    )
    bent = jnp.sum(ortho * gram, axis=0, keepdims=True) * ortho_row
    mean = (
        first
        - 2.0 * jnp.sum(ortho * ortho, axis=0, keepdims=True)
        + jnp.sum(bent, axis=1, keepdims=True)
    )
    beta_new = jnp.sqrt(mean + 1e-06)
    values_ref[...] = jnp.where(
        (row == 0) & (lane == 0), alpha, jnp.where((row == 0) & (lane == 1), beta_new, 0.0)
    )
    index = lax.broadcasted_iota(jnp.int32, ortho.shape, 0)
    coefs = ortho + jnp.where(index == end, alpha, 0.0) + jnp.where(index == prior, beta, 0.0)
    coefs = [jnp.broadcast_to(coefs[j : j + 1], (pairs, lanes)) for j in range(n)]
    scale = jnp.broadcast_to(1.0 / beta_new, (pairs, lanes))

    @pl.loop(0, pieces)
    def _(piece):
        slot = lax.rem(piece + 2, slots_held)
        stream_copy(piece, slot).wait()
        cols = pl.ds(pl.multiple_of(piece * lanes, lanes), lanes)

        @pl.loop(0, rows // 32)
        def _(step):
            for line in range(32):
                at = step * 32 + line
                value = next_ref[at, :, cols]
                for j in range(n):
                    value = value - coefs[j] * stream[slot, j, at, :, :]
                next_ref[at, :, cols] = value * scale

        @pl.when(piece + slots_held < pieces)
        def _():
            stream_copy(piece + slots_held, slot).start()

    for offset in range(1, devices):
        dots_copy(offset).wait_send()


def ring_step(blocks, cuts, entries, table, left_env, right_env, basis, beta_prev):
    rows, half_slots, depth = left_env.shape
    pairs, cols = basis.shape[2], basis.shape[3]
    slots, chips, quarter = 2 * half_slots, depth // (2 * rows), cols // 2
    basis_count = basis.shape[0]
    count = basis_count * (basis_count + 1) // 2
    square = table.transpose(1, 2, 0, 3).reshape(slots * pairs, slots * pairs)
    bf16, f32 = jnp.bfloat16, jnp.float32
    sem = pltpu.SemaphoreType.DMA
    steps = chips - 1
    hbm = pl.BlockSpec(memory_space=pltpu.HBM)
    vmem = pl.BlockSpec(memory_space=pltpu.VMEM)
    devices = blocks * cuts
    smem = pl.BlockSpec(memory_space=pltpu.SMEM)
    next_vector, values = pl.pallas_call(
        functools.partial(ring_kernel, blocks, cuts, entries),
        name="ring",
        in_specs=[smem, hbm, hbm, vmem, hbm],
        out_specs=[vmem, vmem],
        out_shape=[
            jax.ShapeDtypeStruct((rows, pairs, cols), f32),
            jax.ShapeDtypeStruct((8, 128), f32),
        ],
        scratch_shapes=[
            pltpu.VMEM((chips, pairs, 2 * rows, quarter), bf16),
            pltpu.VMEM((slots, 2 * rows, depth), bf16),
            pltpu.VMEM((chips, 2 * rows, slots * quarter), bf16),
            pltpu.VMEM((2 * pairs * rows, slots * quarter), bf16),
            pltpu.VMEM((slots * pairs * 8, slots * pairs * 8), f32),
            pltpu.VMEM((pairs, slots, rows // 2, quarter // 2), f32),
            pltpu.VMEM((chips + 2, 2, pairs, rows, rows), f32),
            pltpu.VMEM((2, 2, pairs, rows, rows), f32),
            pltpu.VMEM((chips, pairs, rows, rows), f32),
            pltpu.VMEM((4, basis_count, rows, pairs, 128), f32),
            pltpu.VMEM((2, 32, half_slots, depth), bf16),
            pltpu.VMEM((count, pairs, 128), f32),
            pltpu.VMEM((basis_count + 1, pairs, 128), f32),
            pltpu.VMEM((8, 128), f32),
            pltpu.VMEM((devices, 8, 128), f32),
            pltpu.VMEM((1, 128), f32),
            pltpu.VMEM((devices, 1, 128), f32),
            sem((devices,)),
            sem((devices,)),
            sem((devices,)),
            sem((devices,)),
            sem((2,)),
            sem((2,)),
            sem((6 + pairs,)),
            sem((6 + pairs,)),
            sem((2, steps, 2)),
            sem((2, steps, 2)),
            sem((2, steps, 2)),
            sem((2, steps, 2)),
            sem((chips,)),
            sem((chips,)),
            sem((chips, 2)),
            sem((chips,)),
            sem((4,)),
        ],
        compiler_params=pltpu.CompilerParams(
            vmem_limit_bytes=65400 * 1024, collective_id=1, has_side_effects=True
        ),
    )(beta_prev.reshape(1), left_env, right_env, square, basis)
    return next_vector, values[0, 0:1], values[0, 1:2]


def ring_fits(blocks, rows, basis_count):
    return blocks == 16 and rows == 128 and basis_count == 8


def gathered_image(cuts, table, left_env, right_env, current):
    row_count, pair_count, col_count = current.shape
    bond_width = table.shape[0]
    full_width = left_env.shape[2]
    me = lax.axis_index("cuts")
    swap = [(0, 1), (1, 0)]

    current = current.transpose(1, 0, 2)
    left_t = left_env.transpose(1, 0, 2)
    right_t = right_env.transpose(1, 0, 2)
    if cuts == 2:
        half = left_t.shape[0]
        theirs = lax.dynamic_slice_in_dim(right_t, (1 - me) * col_count, col_count, 2)
        mine = lax.dynamic_slice_in_dim(right_t, me * col_count, col_count, 2)
        right_k = jnp.concatenate([mine, lax.ppermute(theirs, "cuts", swap)], axis=0)
        left_k = jnp.concatenate([left_t, lax.ppermute(left_t, "cuts", swap)], axis=0)
        turned = jnp.roll(jnp.roll(table, -half, axis=0), -half, axis=1)
        table = jnp.where(me == 0, table, turned)
    else:
        left_k = lax.all_gather(left_t, "cuts", axis=0, tiled=True)
        right_k = lax.all_to_all(right_t, "cuts", split_axis=2, concat_axis=0, tiled=True)
    cur_full = lax.all_gather(current, "blk", axis=1, tiled=True)
    right_full = lax.all_gather(right_k, "blk", axis=1, tiled=True)

    mixed = mixed_left_of(table, left_k, cur_full)
    mixed = mixed.reshape(bond_width, pair_count * row_count, col_count)
    if cuts == 2:
        away = image_part(mixed, right_full, (1 - me) * col_count, col_count)
        away = lax.ppermute(away, "cuts", swap)
        here = image_part(mixed, right_full, me * col_count, col_count)
        image = here + away
    else:
        image = image_part(mixed, right_full, jnp.int32(0), full_width)
        image = lax.psum_scatter(image, "cuts", scatter_dimension=1, tiled=True)
    return image.reshape(pair_count, row_count, col_count).transpose(1, 0, 2)


def on_device(
    blocks, cuts, left_env, right_env, left_core, right_core, slot_bond, krylov_basis, beta_prev
):
    pair_count = left_core.shape[2] * left_core.shape[2]
    basis_count, row_count, _, _ = krylov_basis.shape
    full_width = left_env.shape[2]
    entries = float(full_width * pair_count * full_width)
    table = build_table(left_core, right_core, slot_bond)
    if cuts == 2 and ring_fits(blocks, row_count, basis_count):
        return ring_step(
            blocks, cuts, entries, table, left_env, right_env, krylov_basis, beta_prev
        )
    current = krylov_basis[basis_count - 1].astype(jnp.bfloat16)
    image = gathered_image(cuts, table, left_env, right_env, current)
    gram = gram_of(krylov_basis)

    sums = lax.psum(jnp.concatenate([gram, dots_of(krylov_basis, image)]), ("blk", "cuts"))
    sums = sums / entries
    count = basis_count * (basis_count + 1) // 2
    where = []
    for j in range(basis_count):
        for k in range(basis_count):
            low, high = min(j, k), max(j, k)
            where.append(low * basis_count - low * (low - 1) // 2 + high - low)
    gram_matrix = sums[jnp.array(where)].reshape(basis_count, basis_count)
    inner_prods = sums[count : count + basis_count]
    image_square = sums[count + basis_count]
    last, prior = basis_count - 1, basis_count - 2
    alpha_now = inner_prods[last]
    ortho_coeffs = (
        inner_prods - alpha_now * gram_matrix[:, last] - beta_prev * gram_matrix[:, prior]
    )
    first_square = (
        image_square
        - 2.0 * alpha_now * inner_prods[last]
        - 2.0 * beta_prev * inner_prods[prior]
        + alpha_now * alpha_now * gram_matrix[last, last]
        + 2.0 * alpha_now * beta_prev * gram_matrix[last, prior]
        + beta_prev * beta_prev * gram_matrix[prior, prior]
    )
    square_mean = (
        first_square
        - 2.0 * jnp.sum(ortho_coeffs * ortho_coeffs)
        + jnp.sum(ortho_coeffs[:, None] * gram_matrix * ortho_coeffs[None, :])
    )
    beta_new = jnp.sqrt(square_mean + 1e-06)
    index = jnp.arange(basis_count)
    coefs = (
        ortho_coeffs
        + jnp.where(index == last, alpha_now, 0.0)
        + jnp.where(index == prior, beta_prev, 0.0)
    )
    coefs = jnp.concatenate([coefs, (1.0 / beta_new)[None]])
    next_vector = final_of(coefs, krylov_basis, image)
    return (next_vector, alpha_now[None], beta_new[None])


def solution(mesh):
    in_specs = (
        P("blk", "cuts", None),
        P("blk", "cuts", None),
        P(),
        P(),
        P(),
        P(None, "blk", None, "cuts"),
        P(),
    )
    out_specs = (P("blk", None, "cuts"), P(), P())
    return jax.shard_map(
        functools.partial(on_device, mesh.shape["blk"], mesh.shape["cuts"]),
        mesh=mesh,
        in_specs=in_specs,
        out_specs=out_specs,
        check_vma=False,
    )
```
